32 devices in a mesh: dp: 2 (over x), tp: 4 (over z), pp: 4 (over y, core).
Axes of the slice: x: 2, y: 2, z: 4, core: 2. Of those that a mesh axis runs over, the one named last changes fastest.
Arguments:
- x_in: bfloat16 [2, 2, 2048, 512], P(None, 'dp'), parts along dimension 1
- dy_out: bfloat16 [2, 2, 2048, 512], P(None, 'dp'), parts along dimension 1
- w_qkv: bfloat16 [4, 3, 512, 8, 64], P('pp', None, None, 'tp')
- b_qkv: bfloat16 [4, 3, 8, 64], P('pp', None, 'tp')
- w_out: bfloat16 [4, 8, 64, 512], P('pp', 'tp')
- b_out: bfloat16 [4, 512], P('pp')
- ln_par: bfloat16 [4, 4, 512], P('pp')
- w_fc1: bfloat16 [4, 512, 2048], P('pp', None, 'tp')
- b_fc1: bfloat16 [4, 2048], P('pp', 'tp')
- w_fc2: bfloat16 [4, 2048, 512], P('pp', 'tp')
- b_fc2: bfloat16 [4, 512], P('pp')
Outputs:
- output 1: bfloat16 [4, 2, 2, 2048, 512], P('pp', None, 'dp'), parts along dimension 2
- output 2: bfloat16 [4, 2, 2, 2048, 512], P('pp', None, 'dp'), parts along dimension 2
- output 3: float32 [8, 3, 512, 8, 64], P(('dp', 'pp'), None, None, 'tp'), parts along dimension 0
- output 4: float32 [8, 3, 8, 64], P(('dp', 'pp'), None, 'tp'), parts along dimension 0
- output 5: float32 [8, 8, 64, 512], P(('dp', 'pp'), 'tp'), parts along dimension 0
- output 6: float32 [8, 512], P(('dp', 'pp')), parts along dimension 0
- output 7: float32 [8, 4, 512], P(('dp', 'pp')), parts along dimension 0
- output 8: float32 [8, 512, 2048], P(('dp', 'pp'), None, 'tp'), parts along dimension 0
- output 9: float32 [8, 2048], P(('dp', 'pp'), 'tp'), parts along dimension 0
- output 10: float32 [8, 2048, 512], P(('dp', 'pp'), 'tp'), parts along dimension 0
- output 11: float32 [8, 512], P(('dp', 'pp')), parts along dimension 0
There are 2 independent parts. The reference program is written for one: setup_inputs(seed, part) draws one part's arguments, and reference() takes and returns one part's arrays. A program takes and returns all parts, laid end to end along the dimension named above; an argument that names none is the same for every part.
All inputs are finite; a program needn't handle non-finite values.
Results may differ from the reference program's by a relative error of at most 0.02.
Values are sent between devices in bfloat16 or wider.
A program may use at most 1 GiB of HBM per device.

```python
import jax
import jax.numpy as jnp
from jax import lax

NUM_STAGES = 4
NUM_MICRO = 2
MICRO_ROWS = 1
SEQ_LEN = 2048
D_MODEL = 512
NUM_HEADS = 8
D_FF = 2048

HEAD_DIM = D_MODEL // NUM_HEADS
LN_EPS = 1e-5


def setup_inputs(seed: int = 0, part: int = 0) -> dict:
    base_key = jax.random.key(seed)
    data_keys = jax.random.split(jax.random.fold_in(base_key, part), 2)
    param_keys = jax.random.split(base_key, 9)
    act_shape = (NUM_MICRO, MICRO_ROWS, SEQ_LEN, D_MODEL)
    in_scale = D_MODEL ** -0.5
    ff_scale = D_FF ** -0.5
    ln_offset = jnp.array([1.0, 0.0, 1.0, 0.0], jnp.float32)[None, :, None]

    def normal_draw(key_item, shape_tuple, draw_scale):
        return jax.random.normal(key_item, shape_tuple, jnp.float32) * draw_scale

    return {
        "x_in": normal_draw(data_keys[0], act_shape, 1.0).astype(jnp.bfloat16),
        "dy_out": normal_draw(data_keys[1], act_shape, 1.0).astype(jnp.bfloat16),
        "w_qkv": normal_draw(param_keys[0], (NUM_STAGES, 3, D_MODEL, NUM_HEADS, HEAD_DIM), in_scale).astype(jnp.bfloat16),
        "b_qkv": normal_draw(param_keys[1], (NUM_STAGES, 3, NUM_HEADS, HEAD_DIM), 0.5).astype(jnp.bfloat16),
        "w_out": normal_draw(param_keys[2], (NUM_STAGES, NUM_HEADS, HEAD_DIM, D_MODEL), in_scale).astype(jnp.bfloat16),
        "b_out": normal_draw(param_keys[3], (NUM_STAGES, D_MODEL), 0.3).astype(jnp.bfloat16),
        "ln_par": (normal_draw(param_keys[4], (NUM_STAGES, 4, D_MODEL), 0.3) + ln_offset).astype(jnp.bfloat16),
        "w_fc1": normal_draw(param_keys[5], (NUM_STAGES, D_MODEL, D_FF), in_scale).astype(jnp.bfloat16),
        "b_fc1": normal_draw(param_keys[6], (NUM_STAGES, D_FF), 0.5).astype(jnp.bfloat16),
        "w_fc2": normal_draw(param_keys[7], (NUM_STAGES, D_FF, D_MODEL), ff_scale).astype(jnp.bfloat16),
        "b_fc2": normal_draw(param_keys[8], (NUM_STAGES, D_MODEL), 0.3).astype(jnp.bfloat16),
    }


def layer_norm(x_act, ln_gain, ln_shift):
    x_wide = x_act.astype(jnp.float32)
    row_mean = jnp.mean(x_wide, axis=-1, keepdims=True)
    centered = x_wide - row_mean
    row_var = jnp.mean(centered * centered, axis=-1, keepdims=True)
    normed = centered * lax.rsqrt(row_var + LN_EPS)
    return (normed * ln_gain.astype(jnp.float32) + ln_shift.astype(jnp.float32)).astype(jnp.bfloat16)


def causal_attention(q_heads, k_heads, v_heads):
    scores = jnp.einsum("bqhe,bkhe->bhqk", q_heads.astype(jnp.float32), k_heads.astype(jnp.float32)) * (HEAD_DIM ** -0.5)
    positions = jnp.arange(SEQ_LEN)
    causal = positions[:, None] >= positions[None, :]
    scores = jnp.where(causal, scores, -1e30)
    attn_probs = jax.nn.softmax(scores, axis=-1).astype(jnp.bfloat16)
    attn_mix = jnp.einsum("bhqk,bkhe->bqhe", attn_probs.astype(jnp.float32), v_heads.astype(jnp.float32))
    return attn_mix.astype(jnp.bfloat16)


def gpt_layer(x_act, w_qkv, b_qkv, w_out, b_out, ln_par, w_fc1, b_fc1, w_fc2, b_fc2):
    h_one = layer_norm(x_act, ln_par[0], ln_par[1])
    qkv_pre = jnp.einsum("bsd,cdhe->bsche", h_one.astype(jnp.float32), w_qkv.astype(jnp.float32)) + b_qkv.astype(jnp.float32)
    qkv_all = qkv_pre.astype(jnp.bfloat16)
    attn_mix = causal_attention(qkv_all[:, :, 0], qkv_all[:, :, 1], qkv_all[:, :, 2])
    attn_sum = jnp.einsum("bshe,hed->bsd", attn_mix.astype(jnp.float32), w_out.astype(jnp.float32))
    x_mid = (x_act.astype(jnp.float32) + attn_sum + b_out.astype(jnp.float32)).astype(jnp.bfloat16)
    h_two = layer_norm(x_mid, ln_par[2], ln_par[3])
    pre_act = jnp.einsum("bsd,df->bsf", h_two.astype(jnp.float32), w_fc1.astype(jnp.float32)) + b_fc1.astype(jnp.float32)
    gelu_out = jax.nn.gelu(pre_act, approximate=True).astype(jnp.bfloat16)
    mlp_sum = jnp.einsum("bsf,fd->bsd", gelu_out.astype(jnp.float32), w_fc2.astype(jnp.float32))
    return (x_mid.astype(jnp.float32) + mlp_sum + b_fc2.astype(jnp.float32)).astype(jnp.bfloat16)


def reference(x_in, dy_out, w_qkv, b_qkv, w_out, b_out, ln_par, w_fc1, b_fc1, w_fc2, b_fc2):
    weights = (w_qkv, b_qkv, w_out, b_out, ln_par, w_fc1, b_fc1, w_fc2, b_fc2)

    def forward_step(x_act, layer_w):
        y_act = gpt_layer(x_act, *layer_w)
        return y_act, (x_act, y_act)

    def backward_step(grad_act, layer_pack):
        layer_in, layer_w = layer_pack
        wide_w = tuple(w_item.astype(jnp.float32) for w_item in layer_w)
        _, pullback = jax.vjp(gpt_layer, layer_in, *wide_w)
        grad_list = pullback(grad_act)
        return grad_list[0], (grad_list[0], grad_list[1:])

    def one_micro(grad_acc, micro_pack):
        x_micro, dy_micro = micro_pack
        _, (stage_in, stage_out) = lax.scan(forward_step, x_micro, weights)
        _, (stage_grad, weight_grad) = lax.scan(backward_step, dy_micro, (stage_in, weights), reverse=True)
        grad_acc = tuple(acc_item + new_item for acc_item, new_item in zip(grad_acc, weight_grad))
        return grad_acc, (stage_out, stage_grad)

    grad_init = tuple(jnp.zeros(w_item.shape, jnp.float32) for w_item in weights)
    grad_sum, (all_out, all_grad) = lax.scan(one_micro, grad_init, (x_in, dy_out))
    h_out = jnp.swapaxes(all_out, 0, 1)
    g_in = jnp.swapaxes(all_grad, 0, 1)
    return (h_out, g_in, grad_sum[0], grad_sum[1], grad_sum[2], grad_sum[3], grad_sum[4], grad_sum[5], grad_sum[6], grad_sum[7], grad_sum[8])
```

```python
import functools

import jax
import jax.numpy as jnp
from jax import lax
from jax.experimental import pallas as pl
from jax.experimental.pallas import tpu as pltpu
from jax.sharding import PartitionSpec as P

LN_EPS = 1e-5
BF = jnp.bfloat16
F32 = jnp.float32
MESH = pl.DeviceIdType.MESH

LAYERS = 4
SEQ = 2048
D = 512
CH = 128
NJ = 8
ROWS = CH * NJ
SLOTS = 2 * NJ
GELU_C = 0.7978845608028654
GELU_A = 0.044715
W = 128
KB = 256
NO = None


def nn(a, b):
    return lax.dot_general(a, b, (((1,), (0,)), ((), ())), preferred_element_type=F32)


def nt(a, b):
    return lax.dot_general(a, b, (((1,), (1,)), ((), ())), preferred_element_type=F32)


def tn(a, b):
    return lax.dot_general(a, b, (((0,), (0,)), ((), ())), preferred_element_type=F32)


def ln_stats(x_wide):
    mean = jnp.mean(x_wide, axis=-1, keepdims=True)
    cent = x_wide - mean
    var = jnp.mean(cent * cent, axis=-1, keepdims=True)
    rstd = lax.rsqrt(var + LN_EPS)
    return cent * rstd, rstd


def ln_back(dy, xhat, rstd, gain):
    dxhat = dy * gain
    m1 = jnp.mean(dxhat, axis=-1, keepdims=True)
    m2 = jnp.mean(dxhat * xhat, axis=-1, keepdims=True)
    return rstd * (dxhat - m1 - xhat * m2)


def colsum(v):
    return jnp.sum(v, axis=0, keepdims=True)


def when(cond):
    return pl.when(cond)


def wait_dma(ref, sem):
    pltpu.make_async_copy(ref, ref, sem).wait()


class Place:
    def __init__(self):
        self.z = lax.axis_index("tp")
        self.p = lax.axis_index("pp")
        self.y = self.p // 2
        self.c = self.p % 2
        self.hub = (self.z == 1) | (self.z == 2)
        self.leaf = jnp.logical_not(self.hub)
        self.my_hub = jnp.where(self.z == 0, 1, 2)
        self.my_leaf = jnp.where(self.z == 1, 0, 3)
        self.other_hub = 3 - self.z
        self.mate = self.p + 1 - 2 * self.c
        self.across = 2 * (1 - self.y) + self.c

    def tile(self, j):
        return 2 * j + (self.c + j) % 2

    def tile_rows(self, j):
        return pl.ds(pl.multiple_of(self.tile(j) * CH, CH), CH)

    def mate_rows(self, j):
        return pl.ds(pl.multiple_of((2 * j + (self.c + j + 1) % 2) * CH, CH), CH)

    def enter(self):
        bar = pltpu.get_barrier_semaphore()
        for k in range(1, 4):
            pl.semaphore_signal(bar, inc=1, device_id={"pp": (self.p + k) % 4}, device_id_type=MESH)

        @when(self.z > 0)
        def _():
            pl.semaphore_signal(bar, inc=1, device_id={"tp": self.z - 1}, device_id_type=MESH)

        @when(self.z < 3)
        def _():
            pl.semaphore_signal(bar, inc=1, device_id={"tp": self.z + 1}, device_id_type=MESH)

        @when(self.hub)
        def _():
            pl.semaphore_wait(bar, 5)

        @when(self.leaf)
        def _():
            pl.semaphore_wait(bar, 4)


def chunk_rows(j):
    return pl.ds(pl.multiple_of(j * CH, CH), CH)


def send(src, dst, ssem, rsem, dev):
    pltpu.make_async_remote_copy(src, dst, ssem, rsem, device_id=dev, device_id_type=MESH).start()


class LineSum:
    def __init__(self, at, part, lbuf, hbuf, sbuf, fin, s1, s2, r_l, r_h, r_f):
        self.at, self.part, self.lbuf, self.hbuf, self.sbuf, self.fin = at, part, lbuf, hbuf, sbuf, fin
        self.s1, self.s2, self.r_l, self.r_h, self.r_f = s1, s2, r_l, r_h, r_f

    def emit(self, e, value):
        slot = e % SLOTS
        at = self.at

        @when(at.leaf & (e >= SLOTS))
        def _():
            wait_dma(self.part.at[slot], self.s1.at[slot])

        self.part[slot] = value.astype(BF)

        @when(at.leaf)
        def _():
            send(self.part.at[slot], self.lbuf.at[slot], self.s1.at[slot], self.r_l.at[slot], {"tp": at.my_hub})

        self.serve_first(e - 2)
        self.serve_second(e - 4)

    def serve_first(self, e):
        slot = (e + SLOTS) % SLOTS
        at = self.at

        @when(at.hub & (e >= 0))
        def _():
            wait_dma(self.lbuf.at[slot], self.r_l.at[slot])

            @when(e >= SLOTS)
            def _():
                wait_dma(self.sbuf.at[slot], self.s1.at[slot])

            self.sbuf[slot] = (self.part[slot].astype(F32) + self.lbuf[slot].astype(F32)).astype(BF)
            send(self.sbuf.at[slot], self.hbuf.at[slot], self.s1.at[slot], self.r_h.at[slot], {"tp": at.other_hub})

    def serve_second(self, e):
        slot = (e + SLOTS) % SLOTS
        at = self.at

        @when(at.hub & (e >= 0))
        def _():
            wait_dma(self.hbuf.at[slot], self.r_h.at[slot])

            @when(e >= SLOTS)
            def _():
                wait_dma(self.fin.at[slot], self.s2.at[slot])

            self.fin[slot] = (self.sbuf[slot].astype(F32) + self.hbuf[slot].astype(F32)).astype(BF)
            send(self.fin.at[slot], self.fin.at[slot], self.s2.at[slot], self.r_f.at[slot], {"tp": at.my_leaf})

    def get(self, slot):
        @when(self.at.leaf)
        def _():
            wait_dma(self.fin.at[slot], self.r_f.at[slot])

        return self.fin[slot].astype(F32)

    def drain(self, total):
        self.serve_first(total - 2)
        self.serve_first(total - 1)
        for k in range(4):
            self.serve_second(total - 4 + k)

    def close(self):
        def body(slot, carry):
            wait_dma(self.part.at[slot], self.s1.at[slot])

            @when(self.at.hub)
            def _():
                wait_dma(self.fin.at[slot], self.s2.at[slot])

            return carry

        lax.fori_loop(0, SLOTS, body, 0)


LINE_SCRATCH = [pltpu.VMEM((SLOTS, CH, D), BF)] * 5 + [pltpu.SemaphoreType.DMA((SLOTS,))] * 5


def head_stack(v):
    lane = lax.broadcasted_iota(jnp.int32, v.shape, 1)
    zero = jnp.zeros_like(v)
    return jnp.concatenate([jnp.where(lane < 64, v, zero), jnp.where(lane < 64, zero, v)], axis=0)


def head_merge(v):
    lane = lax.broadcasted_iota(jnp.int32, (CH, W), 1)
    return jnp.where(lane < 64, v[:CH], v[CH:])


def forward_kernel(x_in, wq, wo, w1, w2, ws,
                   h_out, xs, xm, kvs, qs, os_, lses, wqa, woa, w1a, w2a, wsa,
                   wqv, wov, w1v, w2v, wsv, kv, xcur, xmid, q_all, o_all, lse_all, scores, acc, lsum,
                   part, lbuf, hbuf, sbuf, fin, s1, s2, r_l, r_h, r_f,
                   x_sem, w_local, w_send, w_recv, w_fwd, kv_s, kv_r, ho_s, ho_r, save):
    at = Place()
    line = LineSum(at, part, lbuf, hbuf, sbuf, fin, s1, s2, r_l, r_h, r_f)
    y, c, p = at.y, at.c, at.p
    w_hbm = (wq, wo, ws, w1, w2)
    w_vm = (wqv, wov, wsv, w1v, w2v)
    group_a, group_m = (0, 1, 2), (3, 4)

    for j in range(NJ):
        pltpu.make_async_copy(x_in.at[y, at.tile_rows(j)], xcur.at[chunk_rows(j)], x_sem.at[j]).start()
    for k in range(5):
        pltpu.make_async_copy(w_hbm[k], w_vm[k].at[p], w_local.at[k]).start()

    at.enter()

    def send_across():
        for k in range(5):
            send(w_hbm[k], w_vm[k].at[p], w_send.at[1, k], w_recv.at[p, k], {"pp": at.across})

    @when(c == 0)
    def _():
        send_across()

    for k in range(5):
        send(w_hbm[k], w_vm[k].at[p], w_send.at[0, k], w_recv.at[p, k], {"pp": at.mate})

    def weights_ready(s, group):
        @when(p == s)
        def _():
            for k in group:
                wait_dma(w_vm[k].at[p], w_local.at[k])

        @when(p != s)
        def _():
            for k in group:
                wait_dma(w_vm[k].at[s], w_recv.at[s, k])

        @when((y != s // 2) & (c == s % 2))
        def _():
            for k in group:
                send(w_vm[k].at[s], w_vm[k].at[s], w_fwd.at[k], w_recv.at[s, k], {"pp": at.mate})

    weights_ready(0, group_a)

    def finish_y(l, j):
        rows = chunk_rows(j)
        total = line.get(NJ + j)
        b2 = wsv[l, 5:6, :].astype(F32)
        out = (xmid[rows, :].astype(F32) + total + b2).astype(BF)

        @when(l > 0)
        def _():
            wait_dma(xcur.at[rows], ho_s.at[j])

        xcur[rows, :] = out
        dst = h_out.at[y, at.tile_rows(j)]

        @when(p == l)
        def _():
            pltpu.make_async_copy(xcur.at[rows], dst, ho_s.at[j]).start()

        @when(p != l)
        def _():
            send(xcur.at[rows], dst, ho_s.at[j], ho_r.at[p], {"pp": l})

    def attn_op(l, j):
        rows = chunk_rows(j)
        par = l % 2

        @when(l == 0)
        def _():
            wait_dma(xcur.at[rows], x_sem.at[j])

        @when(l > 0)
        def _():
            finish_y(l - 1, j)

        small = wsv[l].astype(F32)
        xhat, _ = ln_stats(xcur[rows, :].astype(F32))
        h1 = (xhat * small[0:1] + small[1:2]).astype(BF)
        qkv = (nn(h1, wqv[l]) + small[7:8, :384]).astype(BF)
        q = qkv[:, :W]
        mine = at.tile_rows(j)
        kv[par, mine, :] = qkv[:, W:384]
        send(kv.at[par, mine], kv.at[par, mine], kv_s.at[j], kv_r.at[j], {"pp": at.mate})
        q_all[rows, :] = q
        q2 = head_stack(q * jnp.asarray(0.125, BF))

        def score(kb):
            return nt(q2, kv[par, pl.ds(pl.multiple_of(kb * KB, KB), KB), 0:W])

        def pass_one(kb, best):
            s = score(kb)
            scores[kb] = s
            return jnp.maximum(best, jnp.maximum(s[:, :W], s[:, W:]))

        best = lax.fori_loop(0, j, pass_one, jnp.full((KB, W), -1e30, F32))
        wait_dma(kv.at[par, mine], kv_r.at[j])
        s = score(j)
        row = lax.broadcasted_iota(jnp.int32, (KB, KB), 0) % CH + CH * ((c + j) % 2)
        col = lax.broadcasted_iota(jnp.int32, (KB, KB), 1)
        s = jnp.where(row >= col, s, -1e30)
        scores[j] = s
        best = jnp.maximum(best, jnp.maximum(s[:, :W], s[:, W:]))
        top = jnp.max(best, axis=-1, keepdims=True)
        acc[...] = jnp.zeros_like(acc)
        lsum[...] = jnp.zeros_like(lsum)

        def pass_two(kb, carry):
            e = jnp.exp(scores[kb] - top)
            lsum[...] += e[:, :W] + e[:, W:]
            acc[...] += nn(e.astype(BF), kv[par, pl.ds(pl.multiple_of(kb * KB, KB), KB), W:KB])
            return carry

        lax.fori_loop(0, j + 1, pass_two, 0)
        den = jnp.sum(lsum[...], axis=-1, keepdims=True)
        o = head_merge(acc[...] / den).astype(BF)
        o_all[rows, :] = o
        lse = jnp.broadcast_to(top + jnp.log(den), (KB, W))
        lse_all[pl.ds(pl.multiple_of(j * 8, 8), 8), :] = lse.T[:8]
        line.emit(2 * NJ * l + j, nn(o, wov[l]))

    def mlp_op(l, j):
        rows = chunk_rows(j)
        small = wsv[l].astype(F32)
        xm_new = (xcur[rows, :].astype(F32) + line.get(j) + small[4:5]).astype(BF)
        xmid[rows, :] = xm_new
        xhat, _ = ln_stats(xm_new.astype(F32))
        h2 = (xhat * small[2:3] + small[3:4]).astype(BF)
        u = nn(h2, w1v[l]) + small[6:7]
        a = 0.5 * u * (1.0 + jnp.tanh(GELU_C * (u + GELU_A * u * u * u)))
        line.emit(2 * NJ * l + NJ + j, nn(a.astype(BF), w2v[l]))

    a_saves = ((xcur, xs), (kv, kvs), (q_all, qs), (o_all, os_), (lse_all, lses))

    def layer(l, carry):
        @when(l > 0)
        def _():
            for k in (2, 3, 4):
                wait_dma(a_saves[k][0], save.at[k])
            wait_dma(kv.at[0], save.at[1])
            wait_dma(xcur, save.at[0])

        def attn_step(j, carry):
            attn_op(l, j)
            return carry

        lax.fori_loop(0, NJ, attn_step, 0)
        par = l % 2
        for k in (0, 2, 3, 4):
            pltpu.make_async_copy(a_saves[k][0], a_saves[k][1].at[l], save.at[k]).start()
        pltpu.make_async_copy(kv.at[par], kvs.at[l], save.at[1]).start()

        @when(l == 0)
        def _():
            @when(c == 1)
            def _():
                send_across()

            weights_ready(0, group_m)

        @when(l > 0)
        def _():
            wait_dma(xmid, save.at[5])

        def mlp_step(j, carry):
            mlp_op(l, j)

            @when((j == 6) & (l < LAYERS - 1))
            def _():
                weights_ready(l + 1, group_a + group_m)

            return carry

        lax.fori_loop(0, NJ, mlp_step, 0)
        pltpu.make_async_copy(xmid, xm.at[l], save.at[5]).start()

        def kv_sent(j, carry):
            wait_dma(kv.at[0, pl.ds(0, CH)], kv_s.at[j])
            return carry

        lax.fori_loop(0, NJ, kv_sent, 0)
        return carry

    lax.fori_loop(0, LAYERS, layer, 0)
    outs_w = (wqa, woa, wsa, w1a, w2a)
    for k in range(5):
        pltpu.make_async_copy(w_vm[k], outs_w[k], w_local.at[k]).start()
    line.drain(LAYERS * SLOTS)
    wait_dma(xcur, save.at[0])

    def last(j, carry):
        finish_y(LAYERS - 1, j)
        return carry

    lax.fori_loop(0, NJ, last, 0)

    def ho_done(j, carry):
        wait_dma(xcur.at[pl.ds(0, CH)], ho_s.at[j])
        return carry

    lax.fori_loop(0, NJ, ho_done, 0)
    for k in range(1, 4):
        wait_dma(h_out.at[0, pl.ds(0, ROWS)], ho_r.at[(p + k) % 4])
    wait_dma(kv.at[0], save.at[1])
    for k in (2, 3, 4):
        wait_dma(a_saves[k][0], save.at[k])
    wait_dma(xmid, save.at[5])
    for k in range(5):
        wait_dma(w_vm[k], w_local.at[k])
        wait_dma(w_vm[k].at[0], w_send.at[0, k])
        wait_dma(w_vm[k].at[0], w_send.at[1, k])
        wait_dma(w_vm[k].at[0], w_fwd.at[k])
    line.close()


def run_forward(x_in, wq, wo, w1, w2, ws):
    hbm = pl.BlockSpec(memory_space=pl.ANY)
    sds = jax.ShapeDtypeStruct
    dma = pltpu.SemaphoreType.DMA
    return pl.pallas_call(
        forward_kernel,
        out_shape=(sds((2, SEQ, D), BF), sds((LAYERS, ROWS, D), BF), sds((LAYERS, ROWS, D), BF),
                   sds((LAYERS, SEQ, KB), BF), sds((LAYERS, ROWS, W), BF), sds((LAYERS, ROWS, W), BF),
                   sds((LAYERS, 8 * NJ, KB), F32),
                   sds((LAYERS, D, 384), BF), sds((LAYERS, W, D), BF), sds((LAYERS, D, D), BF),
                   sds((LAYERS, D, D), BF), sds((LAYERS, 16, D), BF)),
        in_specs=[hbm] * 6,
        out_specs=[hbm] * 12,
        scratch_shapes=[
            pltpu.VMEM((LAYERS, D, 384), BF), pltpu.VMEM((LAYERS, W, D), BF), pltpu.VMEM((LAYERS, D, D), BF),
            pltpu.VMEM((LAYERS, D, D), BF), pltpu.VMEM((LAYERS, 16, D), BF),
            pltpu.VMEM((2, SEQ, KB), BF), pltpu.VMEM((ROWS, D), BF), pltpu.VMEM((ROWS, D), BF),
            pltpu.VMEM((ROWS, W), BF), pltpu.VMEM((ROWS, W), BF), pltpu.VMEM((8 * NJ, KB), F32),
            pltpu.VMEM((NJ, KB, KB), F32), pltpu.VMEM((KB, W), F32), pltpu.VMEM((KB, W), F32),
            *LINE_SCRATCH,
            dma((NJ,)), dma((5,)), dma((2, 5)), dma((LAYERS, 5)), dma((5,)), dma((NJ,)), dma((NJ,)), dma((NJ,)), dma((4,)), dma((6,)),
        ],
        compiler_params=pltpu.CompilerParams(collective_id=0, has_side_effects=True, vmem_limit_bytes=60 * 2**20),
        name="forward_layers",
    )(x_in, wq, wo, w1, w2, ws)


def backward_kernel(dy, xs, xm, kvs, qs, os_, lses, wqa, woa, w1a, w2a, wsa,
                    g_in, o_mlp, o_q, o_o, o_sm,
                    wqv, wov, w1v, w2v, wsv, xsv, xmv, kvv, qv, ov, lsev,
                    gcur, gm, dkv, pk, dqs, dq_acc, a_mlp, a_q, a_o, sm, rd_mlp, rd_q, rd_o, ry_mlp, ry_q, ry_o, rsm,
                    part, lbuf, hbuf, sbuf, fin, s1, s2, r_l, r_h, r_f,
                    load, dy_sem, dk_s, dk_r, gi_s, gi_r, d_s, d_r, y_s, y_r, o_sem, sm_s, sm_r):
    at = Place()
    line = LineSum(at, part, lbuf, hbuf, sbuf, fin, s1, s2, r_l, r_h, r_f)
    y, c, p = at.y, at.c, at.p
    loads = ((wsa, wsv), (xm, xmv), (w1a, w1v), (w2a, w2v), (xs, xsv), (kvs, kvv), (qs, qv), (os_, ov), (lses, lsev),
             (wqa, wqv), (woa, wov))

    for j in range(NJ):
        pltpu.make_async_copy(dy.at[y, at.tile_rows(j)], gcur.at[chunk_rows(j)], dy_sem.at[j]).start()
    for l in reversed(range(LAYERS)):
        for k, (src, dst) in enumerate(loads):
            pltpu.make_async_copy(src.at[l], dst.at[l], load.at[l, k]).start()
    at.enter()

    groups = {0: ((a_mlp, rd_mlp, ry_mlp, o_mlp),), 1: ((a_q, rd_q, ry_q, o_q), (a_o, rd_o, ry_o, o_o))}

    def add_into(dst, src):
        n = dst.shape[0]

        def body(i, carry):
            rows = pl.ds(pl.multiple_of(i * 64, 64), 64)
            dst[rows, :] += src[rows, :]
            return carry

        lax.fori_loop(0, n // 64, body, 0)

    def clear(dst):
        n = dst.shape[0]

        def body(i, carry):
            rows = pl.ds(pl.multiple_of(i * 64, 64), 64)
            dst[rows, :] = jnp.zeros((64, dst.shape[1]), F32)
            return carry

        lax.fori_loop(0, n // 64, body, 0)

    def grad_to_mate(l, g):
        @when(c != l % 2)
        def _():
            for k, (acc, rd, _, _) in enumerate(groups[g]):
                send(acc, rd, d_s.at[g, k], d_r.at[g, k], {"pp": at.mate})

    def grad_across(l, g):
        @when(c != l % 2)
        def _():
            for k, (acc, rd, _, _) in enumerate(groups[g]):
                wait_dma(acc, d_s.at[g, k])

        @when(c == l % 2)
        def _():
            for k, (acc, rd, ry, _) in enumerate(groups[g]):
                wait_dma(rd, d_r.at[g, k])
                add_into(rd, acc)

                @when(y != l // 2)
                def _():
                    send(rd, ry, y_s.at[g, k], y_r.at[g, k], {"pp": at.across})

    def grad_home(l, g):
        @when((c == l % 2) & (y != l // 2))
        def _():
            for k, (_, rd, _, _) in enumerate(groups[g]):
                wait_dma(rd, y_s.at[g, k])

        @when(p == l)
        def _():
            for k, (_, rd, ry, out) in enumerate(groups[g]):
                wait_dma(ry, y_r.at[g, k])
                add_into(ry, rd)
                pltpu.make_async_copy(ry, out, o_sem.at[g, k]).start()

    def add_small(l, r, value):
        sm[l, r:r + 1, :] += value

    for l in range(LAYERS):
        sm[l] = jnp.zeros((16, D), F32)

    def finish_layer(l, j):
        rows = chunk_rows(j)
        dh1 = line.get(NJ + (NJ - 1 - j))
        small = wsv[l].astype(F32)
        xhat, rstd = ln_stats(xsv[l, rows, :].astype(F32))
        add_small(l, 0, colsum(dh1 * xhat))
        add_small(l, 1, colsum(dh1))
        out = (gm[rows, :] + ln_back(dh1, xhat, rstd, small[0:1])).astype(BF)

        @when(l < LAYERS - 1)
        def _():
            wait_dma(gcur.at[rows], gi_s.at[j])

        gcur[rows, :] = out
        dst = g_in.at[y, at.tile_rows(j)]

        @when(p == l)
        def _():
            pltpu.make_async_copy(gcur.at[rows], dst, gi_s.at[j]).start()

        @when(p != l)
        def _():
            send(gcur.at[rows], dst, gi_s.at[j], gi_r.at[p], {"pp": l})

    def mlp_back(l, i):
        j = NJ - 1 - i
        rows = chunk_rows(j)

        @when(l == LAYERS - 1)
        def _():
            wait_dma(gcur.at[rows], dy_sem.at[j])

        @when(l < LAYERS - 1)
        def _():
            finish_layer(l + 1, j)

        small = wsv[l].astype(F32)
        g = gcur[rows, :]
        xhat, _ = ln_stats(xmv[l, rows, :].astype(F32))
        h2 = (xhat * small[2:3] + small[3:4]).astype(BF)
        u = nn(h2, w1v[l]) + small[6:7]
        t = jnp.tanh(GELU_C * (u + GELU_A * u * u * u))
        half = 0.5 * (1.0 + t)
        a = (u * half).astype(BF)
        slope = half + 0.5 * u * (1.0 - t * t) * (GELU_C * (1.0 + 3.0 * GELU_A * u * u))
        dpre = nt(g, w2v[l]) * slope
        add_small(l, 5, colsum(g.astype(F32)))
        add_small(l, 6, colsum(dpre))
        dpre = dpre.astype(BF)
        line.emit(2 * NJ * (LAYERS - 1 - l) + i, nt(dpre, w1v[l]))
        a_mlp[0:D, :] += tn(h2, dpre)
        a_mlp[D:2 * D, :] += tn(a, g)

    def attn_back(l, i):
        j = NJ - 1 - i
        rows = chunk_rows(j)
        small = wsv[l].astype(F32)
        dh2 = line.get(i)
        xhat, rstd = ln_stats(xmv[l, rows, :].astype(F32))
        add_small(l, 2, colsum(dh2 * xhat))
        add_small(l, 3, colsum(dh2))
        wide = gcur[rows, :].astype(F32) + ln_back(dh2, xhat, rstd, small[2:3])
        gm[rows, :] = wide
        add_small(l, 4, colsum(wide))
        gmid = wide.astype(BF)
        o = ov[l, rows, :]
        a_o[...] += tn(o, gmid)
        do = nt(gmid, wov[l]).astype(BF)
        prod = do.astype(F32) * o.astype(F32)
        delta = jnp.sum(head_stack(prod), axis=-1, keepdims=True)
        delta = jnp.broadcast_to(delta, (KB, W)).T[0:1]
        lse = lsev[l, pl.ds(pl.multiple_of(j * 8, 8), 8), :][0:1]
        q2 = head_stack(qv[l, rows, :] * jnp.asarray(0.125, BF))
        do2 = head_stack(do)
        dq_acc[...] = jnp.zeros_like(dq_acc)

        def block(kb, masked):
            krows = pl.ds(pl.multiple_of(kb * KB, KB), KB)
            k = kvv[l, krows, 0:W]
            v = kvv[l, krows, W:KB]
            st = nt(k, q2)
            if masked:
                row = lax.broadcasted_iota(jnp.int32, (KB, KB), 0)
                col = lax.broadcasted_iota(jnp.int32, (KB, KB), 1) % CH + CH * ((c + j) % 2)
                st = jnp.where(col >= row, st, -1e30)
            pt = jnp.exp(st - lse)
            dpt = nt(v, do2)
            dst = (pt * (dpt - delta)).astype(BF)
            dkv[krows, 0:W] += nn(dst, q2)
            dkv[krows, W:KB] += nn(pt.astype(BF), do2)
            dq_acc[...] += tn(dst, k)

        def body(kb, carry):
            block(kb, False)
            return carry

        lax.fori_loop(0, j, body, 0)
        block(j, True)
        dqs[rows, :] = (head_merge(dq_acc[...]) * 0.125).astype(BF)
        theirs = at.mate_rows(j)
        send(dkv.at[theirs], pk.at[j], dk_s.at[j], dk_r.at[j], {"pp": at.mate})

    def qkv_back(l, i):
        j = NJ - 1 - i
        rows = chunk_rows(j)
        small = wsv[l].astype(F32)
        wait_dma(pk.at[j], dk_r.at[j])
        dkv_own = (dkv[at.tile_rows(j), :] + pk[j]).astype(BF)
        dqkv = jnp.concatenate([dqs[rows, :], dkv_own], axis=1)
        sm[l, 7:8, 0:384] += colsum(dqkv.astype(F32))
        line.emit(2 * NJ * (LAYERS - 1 - l) + NJ + i, nt(dqkv, wqv[l]))
        xhat, _ = ln_stats(xsv[l, rows, :].astype(F32))
        h1 = (xhat * small[0:1] + small[1:2]).astype(BF)
        a_q[...] += tn(h1, dqkv)

    def layer(n, carry):
        l = LAYERS - 1 - n
        for k, (_, dst) in enumerate(loads):
            wait_dma(dst.at[l], load.at[l, k])
        clear(a_mlp)

        def first_half(i, carry):
            @when((i == 4) & (l < LAYERS - 2))
            def _():
                grad_home(l + 2, 1)

            @when((i == 4) & (l < LAYERS - 1))
            def _():
                grad_across(l + 1, 1)

            mlp_back(l, i)
            return carry

        lax.fori_loop(0, NJ, first_half, 0)
        grad_to_mate(l, 0)
        clear(a_q)
        clear(a_o)
        clear(dkv)

        def second_half(i, carry):
            @when((i == 4) & (l < LAYERS - 1))
            def _():
                grad_home(l + 1, 0)

            @when(i == 4)
            def _():
                grad_across(l, 0)

            @when(i < NJ)
            def _():
                attn_back(l, i)

            @when(i > 0)
            def _():
                qkv_back(l, i - 1)

            return carry

        lax.fori_loop(0, NJ + 1, second_half, 0)
        grad_to_mate(l, 1)

        def dk_sent(j, carry):
            wait_dma(pk.at[j], dk_s.at[j])
            return carry

        lax.fori_loop(0, NJ, dk_sent, 0)
        return carry

    lax.fori_loop(0, LAYERS, layer, 0)
    grad_home(1, 1)
    grad_across(0, 1)
    line.drain(LAYERS * SLOTS)

    def last(i, carry):
        finish_layer(0, NJ - 1 - i)
        return carry

    lax.fori_loop(0, NJ, last, 0)
    for s in range(LAYERS):
        @when(p != s)
        def _():
            send(sm.at[s], rsm.at[p], sm_s.at[s], sm_r.at[p], {"pp": s})
    grad_home(0, 0)
    grad_home(0, 1)

    def gi_done(j, carry):
        wait_dma(gcur.at[pl.ds(0, CH)], gi_s.at[j])
        return carry

    lax.fori_loop(0, NJ, gi_done, 0)
    for s in range(LAYERS):
        @when(p != s)
        def _():
            wait_dma(sm.at[s], sm_s.at[s])
            wait_dma(rsm.at[s], sm_r.at[s])
    rsm[p] = sm[p]
    o_sm[...] = (rsm[0] + rsm[1]) + (rsm[2] + rsm[3])
    for k in range(1, 4):
        wait_dma(g_in.at[0, pl.ds(0, ROWS)], gi_r.at[(p + k) % 4])
    for g, items in groups.items():
        for k, (_, _, ry, _) in enumerate(items):
            wait_dma(ry, o_sem.at[g, k])
    line.close()


def run_backward(*args):
    hbm = pl.BlockSpec(memory_space=pl.ANY)
    sds = jax.ShapeDtypeStruct
    dma = pltpu.SemaphoreType.DMA
    grads = [pltpu.VMEM((2 * D, D), F32), pltpu.VMEM((D, 384), F32), pltpu.VMEM((W, D), F32)]
    return pl.pallas_call(
        backward_kernel,
        out_shape=(sds((2, SEQ, D), BF), sds((2 * D, D), F32), sds((D, 384), F32), sds((W, D), F32), sds((16, D), F32)),
        in_specs=[hbm] * 12,
        out_specs=[hbm] * 4 + [pl.BlockSpec(memory_space=pltpu.VMEM)],
        scratch_shapes=[
            pltpu.VMEM((LAYERS, D, 384), BF), pltpu.VMEM((LAYERS, W, D), BF), pltpu.VMEM((LAYERS, D, D), BF),
            pltpu.VMEM((LAYERS, D, D), BF), pltpu.VMEM((LAYERS, 16, D), BF),
            pltpu.VMEM((LAYERS, ROWS, D), BF), pltpu.VMEM((LAYERS, ROWS, D), BF), pltpu.VMEM((LAYERS, SEQ, KB), BF),
            pltpu.VMEM((LAYERS, ROWS, W), BF), pltpu.VMEM((LAYERS, ROWS, W), BF), pltpu.VMEM((LAYERS, 8 * NJ, KB), F32),
            pltpu.VMEM((ROWS, D), BF), pltpu.VMEM((ROWS, D), F32), pltpu.VMEM((SEQ, KB), F32), pltpu.VMEM((NJ, CH, KB), F32),
            pltpu.VMEM((ROWS, W), BF), pltpu.VMEM((KB, W), F32),
            *grads, pltpu.VMEM((LAYERS, 16, D), F32), *grads, *grads, pltpu.VMEM((LAYERS, 16, D), F32),
            *LINE_SCRATCH,
            dma((LAYERS, 11)), dma((NJ,)), dma((NJ,)), dma((NJ,)), dma((NJ,)), dma((4,)),
            dma((2, 2)), dma((2, 2)), dma((2, 2)), dma((2, 2)), dma((2, 2)), dma((4,)), dma((4,)),
        ],
        compiler_params=pltpu.CompilerParams(collective_id=1, has_side_effects=True, vmem_limit_bytes=63 * 2**20),
        name="backward_layers",
    )(*args)


def solution(mesh):
    def program(x_in, dy_out, w_qkv, b_qkv, w_out, b_out, ln_par, w_fc1, b_fc1, w_fc2, b_fc2):
        wq = w_qkv[0].transpose(1, 0, 2, 3).reshape(D, 384)
        wo = w_out[0].reshape(W, D)
        bq = jnp.pad(b_qkv[0].reshape(1, 384), ((0, 0), (0, D - 384)))
        ws = jnp.concatenate([ln_par[0], b_out, b_fc2, b_fc1, bq, jnp.zeros((8, D), BF)], axis=0)
        fwd = run_forward(x_in.reshape(2, SEQ, D), wq, wo, w_fc1[0], w_fc2[0], ws)
        g_in, d_mlp, d_q, d_o, d_sm = run_backward(dy_out.reshape(2, SEQ, D), *fwd[1:])
        return (fwd[0].reshape(1, 2, 1, SEQ, D), g_in.reshape(1, 2, 1, SEQ, D),
                d_q.reshape(D, 3, 2, 64).transpose(1, 0, 2, 3)[None], d_sm[7, :384].reshape(1, 3, 2, 64),
                d_o.reshape(1, 2, 64, D), d_sm[4:5], d_sm[None, 0:4],
                d_mlp[None, :D], d_sm[6:7], d_mlp[None, D:], d_sm[5:6])

    act_spec = P(NO, "dp", NO, NO)
    arg_specs = (act_spec, act_spec,
                 P("pp", NO, NO, "tp", NO), P("pp", NO, "tp", NO), P("pp", "tp", NO, NO),
                 P("pp", NO), P("pp", NO, NO), P("pp", NO, "tp"), P("pp", "tp"),
                 P("pp", "tp", NO), P("pp", NO))
    stage_spec = P("pp", NO, "dp", NO, NO)
    grad_axes = ("dp", "pp")
    result_specs = (stage_spec, stage_spec,
                    P(grad_axes, NO, NO, "tp", NO), P(grad_axes, NO, "tp", NO), P(grad_axes, "tp", NO, NO),
                    P(grad_axes, NO), P(grad_axes, NO, NO), P(grad_axes, NO, "tp"), P(grad_axes, "tp"),
                    P(grad_axes, "tp", NO), P(grad_axes, NO))
    return jax.shard_map(program, mesh=mesh, in_specs=arg_specs, out_specs=result_specs, check_vma=False)
```

```python
import jax
import jax.numpy as jnp
from jax import lax
from jax.experimental import pallas as pl
from jax.experimental.pallas import tpu as pltpu
from jax.sharding import PartitionSpec as P

LN_EPS = 1e-5
BF = jnp.bfloat16
F32 = jnp.float32
MESH = pl.DeviceIdType.MESH

LAYERS = 4
SEQ = 2048
D = 512
CH = 128
NJ = 8
PAIRS = NJ // 2
ROWS = CH * NJ
SLOTS = 2 * NJ
FWD = LAYERS * SLOTS
W = 128
QKV = 3 * W
KB = 256
WIDE = 2 * KB
SMALL = 16
GELU_C = 0.7978845608028654
GELU_A = 0.044715
MASKED = -1e30
NO = None
GAIN1, SHIFT1, GAIN2, SHIFT2, BOUT, BFC2, BFC1, BQKV = range(8)


def nn(a, b):
    return lax.dot_general(a, b, (((1,), (0,)), ((), ())), preferred_element_type=F32)


def nt(a, b):
    return lax.dot_general(a, b, (((1,), (1,)), ((), ())), preferred_element_type=F32)


def tn(a, b):
    return lax.dot_general(a, b, (((0,), (0,)), ((), ())), preferred_element_type=F32)


def ln_stats(x_wide):
    mean = jnp.mean(x_wide, axis=-1, keepdims=True)
    cent = x_wide - mean
    var = jnp.mean(cent * cent, axis=-1, keepdims=True)
    rstd = lax.rsqrt(var + LN_EPS)
    return cent * rstd, rstd


def ln_back(dy, xhat, rstd, gain):
    dxhat = dy * gain
    m1 = jnp.mean(dxhat, axis=-1, keepdims=True)
    m2 = jnp.mean(dxhat * xhat, axis=-1, keepdims=True)
    return rstd * (dxhat - m1 - xhat * m2)


def colsum(v):
    return jnp.sum(v, axis=0, keepdims=True)


def row(small, r):
    return small[r:r + 1]


def blk(i, n):
    return pl.ds(pl.multiple_of(i * n, n), n)


def chunk(j):
    return blk(j, CH)


def loop(n, body):
    def step(i, carry):
        body(i)
        return carry

    lax.fori_loop(0, n, step, 0)


when = pl.when


def wait_dma(ref, sem):
    pltpu.make_async_copy(ref, ref, sem).wait()


def local(src, dst, sem):
    pltpu.make_async_copy(src, dst, sem).start()


def send(src, dst, ssem, rsem, dev):
    pltpu.make_async_remote_copy(src, dst, ssem, rsem, device_id=dev, device_id_type=MESH).start()


class Place:
    def __init__(self):
        self.z = lax.axis_index("tp")
        self.p = lax.axis_index("pp")
        self.y = self.p // 2
        self.c = self.p % 2
        self.hub = (self.z == 1) | (self.z == 2)
        self.leaf = jnp.logical_not(self.hub)
        self.my_hub = {"tp": jnp.where(self.z == 0, 1, 2)}
        self.my_leaf = {"tp": jnp.where(self.z == 1, 0, 3)}
        self.other_hub = {"tp": 3 - self.z}
        self.mate = {"pp": self.p + 1 - 2 * self.c}
        self.across = {"pp": 2 * (1 - self.y) + self.c}

    def rows_of(self, j):
        return chunk(2 * j + (self.c + j) % 2)

    def mate_rows(self, j):
        return chunk(2 * j + (self.c + j + 1) % 2)

    def enter(self):
        bar = pltpu.get_barrier_semaphore()

        def greet(dev):
            pl.semaphore_signal(bar, inc=1, device_id=dev, device_id_type=MESH)

        for k in range(1, LAYERS):
            greet({"pp": (self.p + k) % LAYERS})

        @when(self.z > 0)
        def _():
            greet({"tp": self.z - 1})

        @when(self.z < 3)
        def _():
            greet({"tp": self.z + 1})

        @when(self.hub)
        def _():
            pl.semaphore_wait(bar, 5)

        @when(self.leaf)
        def _():
            pl.semaphore_wait(bar, 4)


class LineSum:
    def __init__(self, at, part, lbuf, hbuf, fin, s1, s2, r_l, r_h, r_f):
        self.at, self.part, self.lbuf, self.hbuf, self.fin = at, part, lbuf, hbuf, fin
        self.s1, self.s2, self.r_l, self.r_h, self.r_f = s1, s2, r_l, r_h, r_f

    def emit(self, e, value):
        slot = e % SLOTS

        @when(e >= SLOTS)
        def _():
            wait_dma(self.part.at[slot], self.s1.at[slot])

        self.part[slot] = value.astype(BF)

        @when(self.at.leaf)
        def _():
            send(self.part.at[slot], self.lbuf.at[slot], self.s1.at[slot], self.r_l.at[slot], self.at.my_hub)

        self.serve_first(e - 2)
        self.serve_second(e - 4)

    def serve_first(self, e):
        slot = (e + SLOTS) % SLOTS

        @when(self.at.hub & (e >= 0))
        def _():
            wait_dma(self.lbuf.at[slot], self.r_l.at[slot])
            self.part[slot] = (self.part[slot].astype(F32) + self.lbuf[slot].astype(F32)).astype(BF)
            send(self.part.at[slot], self.hbuf.at[slot], self.s1.at[slot], self.r_h.at[slot], self.at.other_hub)

    def serve_second(self, e):
        slot = (e + SLOTS) % SLOTS

        @when(self.at.hub & (e >= 0))
        def _():
            wait_dma(self.hbuf.at[slot], self.r_h.at[slot])

            @when(e >= SLOTS)
            def _():
                wait_dma(self.fin.at[slot], self.s2.at[slot])

            self.fin[slot] = (self.part[slot].astype(F32) + self.hbuf[slot].astype(F32)).astype(BF)
            send(self.fin.at[slot], self.fin.at[slot], self.s2.at[slot], self.r_f.at[slot], self.at.my_leaf)

    def get(self, slot):
        @when(self.at.leaf)
        def _():
            wait_dma(self.fin.at[slot], self.r_f.at[slot])

        return self.fin[slot].astype(F32)

    def drain(self, total):
        self.serve_first(total - 2)
        self.serve_first(total - 1)
        for k in range(4):
            self.serve_second(total - 4 + k)

    def close(self):
        def body(slot):
            wait_dma(self.part.at[slot], self.s1.at[slot])

            @when(self.at.hub)
            def _():
                wait_dma(self.fin.at[slot], self.s2.at[slot])

        loop(SLOTS, body)


def head_stack(v):
    first = lax.broadcasted_iota(jnp.int32, v.shape, 1) < W // 2
    zero = jnp.zeros_like(v)
    return jnp.concatenate([jnp.where(first, v, zero), jnp.where(first, zero, v)], axis=0)


def head_merge(v):
    first = lax.broadcasted_iota(jnp.int32, (CH, W), 1) < W // 2
    return jnp.where(first, v[:CH], v[CH:])


def fold(v, op):
    out = v[:, :W]
    for k in range(1, v.shape[1] // W):
        out = op(out, v[:, k * W:(k + 1) * W])
    return out


def decoder_kernel(x_in, dy, wq, wo, w1, w2, ws,
                   h_out, g_in, o_w1, o_w2, o_q, o_o, o_sm,
                   wqv, wov, w1v, w2v, wsv, kv, xs, xm, qs, os_, lses, scores, acc, lsum,
                   gcur, gm, dkv, pk, buf_a, buf_b, buf_c, dq_acc,
                   a_w1, a_w2, a_q, a_o, d_w1, d_w2, d_q, d_o, y_w1, y_w2, y_q, y_o, sm, rsm,
                   part, lbuf, hbuf, fin, s1, s2, r_l, r_h, r_f,
                   x_sem, w_local, w_send, w_recv, w_fwd, kv_s, kv_r, ho_s, ho_r,
                   dy_sem, dk_s, dk_r, gi_s, gi_r, d_s, d_r, y_s, y_r, o_sem, sm_s, sm_r):
    at = Place()
    line = LineSum(at, part, lbuf, hbuf, fin, s1, s2, r_l, r_h, r_f)
    y, c, p = at.y, at.c, at.p
    w_hbm = (ws, wq, wo, w1, w2)
    w_vm = (wsv, wqv, wov, w1v, w2v)
    every = range(len(w_hbm))
    group_a, group_m = every[:3], every[3:]

    for j in range(NJ):
        local(x_in.at[y, at.rows_of(j)], xs.at[0, chunk(j)], x_sem.at[j])
    for k in every:
        local(w_hbm[k], w_vm[k].at[p], w_local.at[k])

    at.enter()

    def send_across():
        for k in every:
            send(w_hbm[k], w_vm[k].at[p], w_send.at[1, k], w_recv.at[p, k], at.across)

    @when(c == 0)
    def _():
        send_across()

    for k in every:
        send(w_hbm[k], w_vm[k].at[p], w_send.at[0, k], w_recv.at[p, k], at.mate)
    for j in range(NJ):
        local(dy.at[y, at.rows_of(j)], gcur.at[chunk(j)], dy_sem.at[j])

    def weights_ready(s, group):
        @when(p == s)
        def _():
            for k in group:
                wait_dma(w_vm[k].at[p], w_local.at[k])

        @when(p != s)
        def _():
            for k in group:
                wait_dma(w_vm[k].at[s], w_recv.at[s, k])

        @when((y != s // 2) & (c == s % 2))
        def _():
            for k in group:
                send(w_vm[k].at[s], w_vm[k].at[s], w_fwd.at[k], w_recv.at[s, k], at.mate)

    def send_home(l, src, dst, ssem, rsem):
        @when(p == l)
        def _():
            local(src, dst, ssem)

        @when(p != l)
        def _():
            send(src, dst, ssem, rsem.at[p], {"pp": l})

    weights_ready(0, group_a)

    def finish_y(l, j):
        rows = chunk(j)
        total = line.get(NJ + j)
        out = (xm[l, rows, :].astype(F32) + total + row(wsv[l].astype(F32), BFC2)).astype(BF)

        @when(l > 0)
        def _():
            wait_dma(gcur.at[rows], ho_s.at[j])

        xs[l + 1, rows, :] = out
        send_home(l, xs.at[l + 1, rows], h_out.at[y, at.rows_of(j)], ho_s.at[j], ho_r)

    def attn_op(l, jj, odd):
        j = 2 * jj + odd
        rows = chunk(j)

        @when(l == 0)
        def _():
            wait_dma(xs.at[0, rows], x_sem.at[j])

        @when(l > 0)
        def _():
            finish_y(l - 1, j)

        small = wsv[l].astype(F32)
        xhat, _ = ln_stats(xs[l, rows, :].astype(F32))
        h1 = (xhat * row(small, GAIN1) + row(small, SHIFT1)).astype(BF)
        qkv = (nt(h1, wqv[l]) + row(small, BQKV)[:, :QKV]).astype(BF)
        q = qkv[:, :W]
        mine = at.rows_of(j)
        kv[l, mine, :] = qkv[:, W:]
        send(kv.at[l, mine], kv.at[l, mine], kv_s.at[j], kv_r.at[j], at.mate)
        qs[l, rows, :] = q
        q2 = head_stack(q * jnp.asarray(0.125, BF))

        def pass_one(kb, best):
            s = nt(q2, kv[l, blk(kb, WIDE), 0:W])
            scores[kb] = s
            return jnp.maximum(best, fold(s, jnp.maximum))

        best = lax.fori_loop(0, jj, pass_one, jnp.full((KB, W), MASKED, F32))
        wait_dma(kv.at[l, mine], kv_r.at[j])
        width = KB * (1 + odd)
        tail = pl.ds(pl.multiple_of(jj * WIDE, WIDE), width)
        s = nt(q2, kv[l, tail, 0:W])
        pos = lax.broadcasted_iota(jnp.int32, (KB, width), 0) % CH + (KB * odd + CH * ((c + odd) % 2))
        s = jnp.where(pos >= lax.broadcasted_iota(jnp.int32, (KB, width), 1), s, MASKED)
        scores[jj, :, 0:width] = s
        top = jnp.max(jnp.maximum(best, fold(s, jnp.maximum)), axis=-1, keepdims=True)
        acc[...] = jnp.zeros_like(acc)
        lsum[...] = jnp.zeros_like(lsum)

        def weigh(s, keys):
            e = jnp.exp(s - top)
            lsum[...] += fold(e, jnp.add)
            acc[...] += nn(e.astype(BF), kv[l, keys, W:])

        loop(jj, lambda kb: weigh(scores[kb], blk(kb, WIDE)))
        weigh(scores[jj, :, 0:width], tail)
        den = jnp.sum(lsum[...], axis=-1, keepdims=True)
        o = head_merge(acc[...] / den).astype(BF)
        os_[l, rows, :] = o
        lses[l, blk(j, 8), :] = jnp.broadcast_to(top + jnp.log(den), (KB, W)).T[:8]
        line.emit(SLOTS * l + j, nn(o, wov[l]))

    def mlp_op(l, j):
        rows = chunk(j)
        small = wsv[l].astype(F32)
        mid = (xs[l, rows, :].astype(F32) + line.get(j) + row(small, BOUT)).astype(BF)
        xm[l, rows, :] = mid
        xhat, _ = ln_stats(mid.astype(F32))
        h2 = (xhat * row(small, GAIN2) + row(small, SHIFT2)).astype(BF)
        u = nn(h2, w1v[l]) + row(small, BFC1)
        a = 0.5 * u * (1.0 + jnp.tanh(GELU_C * (u + GELU_A * u * u * u)))
        line.emit(SLOTS * l + NJ + j, nn(a.astype(BF), w2v[l]))

    def forward_layer(l):
        def attn_pair(jj):
            with jax.named_scope("attn"):
                attn_op(l, jj, 0)
            with jax.named_scope("attn"):
                attn_op(l, jj, 1)

            @when((l == 0) & (jj == 0) & (c == 1))
            def _():
                send_across()

        loop(PAIRS, attn_pair)

        @when(l == 0)
        def _():
            weights_ready(0, group_m)

        def mlp_step(j):
            with jax.named_scope("mlp"):
                mlp_op(l, j)

            @when((j == NJ - 2) & (l < LAYERS - 1))
            def _():
                weights_ready(l + 1, every)

        loop(NJ, mlp_step)
        loop(NJ, lambda j: wait_dma(kv.at[0, chunk(0)], kv_s.at[j]))

    for l in range(LAYERS):
        sm[l] = jnp.zeros((SMALL, D), F32)
    loop(LAYERS, forward_layer)

    groups = (((a_w1, d_w1, y_w1, o_w1), (a_w2, d_w2, y_w2, o_w2)), ((a_q, d_q, y_q, o_q), (a_o, d_o, y_o, o_o)))

    def add_into(dst, src):
        def body(i):
            rows = blk(i, 64)
            dst[rows, :] += src[rows, :]

        loop(dst.shape[0] // 64, body)

    def grad_to_mate(l, g):
        @when(c != l % 2)
        def _():
            for k, (own, mid, _, _) in enumerate(groups[g]):
                send(own, mid, d_s.at[g, k], d_r.at[g, k], at.mate)

    def grad_across(l, g):
        @when(c != l % 2)
        def _():
            for k, (own, _, _, _) in enumerate(groups[g]):
                wait_dma(own, d_s.at[g, k])

        @when(c == l % 2)
        def _():
            for k, (own, mid, far, _) in enumerate(groups[g]):
                wait_dma(mid, d_r.at[g, k])
                add_into(mid, own)

                @when(y != l // 2)
                def _():
                    send(mid, far, y_s.at[g, k], y_r.at[g, k], at.across)

    def grad_home(l, g):
        @when((c == l % 2) & (y != l // 2))
        def _():
            for k, (_, mid, _, _) in enumerate(groups[g]):
                wait_dma(mid, y_s.at[g, k])

        @when(p == l)
        def _():
            for k, (_, mid, far, out) in enumerate(groups[g]):
                wait_dma(far, y_r.at[g, k])
                add_into(far, mid)
                local(far, out, o_sem.at[g, k])

    def add_small(l, r, value):
        sm[l, r:r + 1, :] += value

    def finish_layer(l, j):
        rows = chunk(j)
        dh1 = line.get(SLOTS - 1 - j)
        xhat, rstd = ln_stats(xs[l, rows, :].astype(F32))
        add_small(l, GAIN1, colsum(dh1 * xhat))
        add_small(l, SHIFT1, colsum(dh1))
        out = (gm[rows, :] + ln_back(dh1, xhat, rstd, row(wsv[l].astype(F32), GAIN1))).astype(BF)

        @when(l < LAYERS - 1)
        def _():
            wait_dma(gcur.at[rows], gi_s.at[j])

        gcur[rows, :] = out
        send_home(l, gcur.at[rows], g_in.at[y, at.rows_of(j)], gi_s.at[j], gi_r)

    def mlp_back(l, i):
        j = NJ - 1 - i
        rows = chunk(j)

        @when(l == LAYERS - 1)
        def _():
            wait_dma(gcur.at[rows], dy_sem.at[j])
            finish_y(l, i)

        @when(l < LAYERS - 1)
        def _():
            finish_layer(l + 1, j)

        small = wsv[l].astype(F32)
        g = gcur[rows, :]
        xhat, _ = ln_stats(xm[l, rows, :].astype(F32))
        h2 = (xhat * row(small, GAIN2) + row(small, SHIFT2)).astype(BF)
        u = nn(h2, w1v[l]) + row(small, BFC1)
        t = jnp.tanh(GELU_C * (u + GELU_A * u * u * u))
        half = 0.5 * (1.0 + t)
        slope = half + 0.5 * u * (1.0 - t * t) * (GELU_C * (1.0 + 3.0 * GELU_A * u * u))
        dpre = nt(g, w2v[l]) * slope
        add_small(l, BFC2, colsum(g.astype(F32)))
        add_small(l, BFC1, colsum(dpre))
        dpre = dpre.astype(BF)
        buf_a[rows, :] = h2
        buf_b[rows, :] = dpre
        buf_c[rows, :] = (u * half).astype(BF)
        line.emit(FWD + SLOTS * (LAYERS - 1 - l) + i, nt(dpre, w1v[l]))

    def mlp_weight_grads():
        def body(t):
            cols = blk(t, KB)
            a_w1[:, cols] = tn(buf_a[...], buf_b[:, cols])
            a_w2[:, cols] = tn(buf_c[...], gcur[:, cols])

        loop(D // KB, body)

    def attn_back(l, jj, odd):
        j = 2 * jj + odd
        rows = chunk(j)
        small = wsv[l].astype(F32)
        dh2 = line.get(NJ - 1 - j)
        xhat, rstd = ln_stats(xm[l, rows, :].astype(F32))
        add_small(l, GAIN2, colsum(dh2 * xhat))
        add_small(l, SHIFT2, colsum(dh2))
        wide = gcur[rows, :].astype(F32) + ln_back(dh2, xhat, rstd, row(small, GAIN2))
        gm[rows, :] = wide
        add_small(l, BOUT, colsum(wide))
        gmid = wide.astype(BF)
        buf_c[rows, :] = gmid
        do = nt(gmid, wov[l]).astype(BF)
        delta = jnp.sum(head_stack(do.astype(F32) * os_[l, rows, :].astype(F32)), axis=-1, keepdims=True)
        delta = jnp.broadcast_to(delta, (KB, W)).T[0:1]
        lse = lses[l, blk(j, 8), :][0:1]
        q2 = head_stack(qs[l, rows, :] * jnp.asarray(0.125, BF))
        do2 = head_stack(do)
        dq_acc[...] = jnp.zeros_like(dq_acc)

        def block(keys, width, masked):
            k = kv[l, keys, 0:W]
            st = nt(k, q2)
            if masked:
                pos = lax.broadcasted_iota(jnp.int32, (width, KB), 1) % CH + (KB * odd + CH * ((c + odd) % 2))
                st = jnp.where(pos >= lax.broadcasted_iota(jnp.int32, (width, KB), 0), st, MASKED)
            pt = jnp.exp(st - lse)
            dst = (pt * (nt(kv[l, keys, W:], do2) - delta)).astype(BF)
            dk = nn(dst, q2)
            dv = nn(pt.astype(BF), do2)
            dq_acc[...] += tn(dst, k)
            dkv[keys, 0:W] += dk
            dkv[keys, W:] += dv

        loop(jj, lambda kb: block(blk(kb, WIDE), WIDE, False))
        width = KB * (1 + odd)
        block(pl.ds(pl.multiple_of(jj * WIDE, WIDE), width), width, True)
        buf_b[rows, 0:W] = (head_merge(dq_acc[...]) * 0.125).astype(BF)
        send(dkv.at[at.mate_rows(j)], pk.at[j], dk_s.at[j], dk_r.at[j], at.mate)

    def qkv_back(l, j):
        rows = chunk(j)
        small = wsv[l].astype(F32)
        xhat, _ = ln_stats(xs[l, rows, :].astype(F32))
        buf_a[rows, :] = (xhat * row(small, GAIN1) + row(small, SHIFT1)).astype(BF)
        wait_dma(pk.at[j], dk_r.at[j])
        dkv_own = (dkv[at.rows_of(j), :] + pk[j]).astype(BF)
        buf_b[rows, W:QKV] = dkv_own
        dqkv = jnp.concatenate([buf_b[rows, 0:W], dkv_own], axis=1)
        sm[l, BQKV:BQKV + 1, 0:QKV] += colsum(dqkv.astype(F32))
        line.emit(FWD + SLOTS * (LAYERS - l) - 1 - j, nn(dqkv, wqv[l]))

    def backward_layer(n):
        l = LAYERS - 1 - n

        def first_half(i):
            @when(i == 2)
            def _():
                @when(l < LAYERS - 2)
                def _():
                    grad_home(l + 2, 1)

                @when(l < LAYERS - 1)
                def _():
                    grad_across(l + 1, 1)

            with jax.named_scope("B1"):
                mlp_back(l, i)

        loop(NJ, first_half)
        with jax.named_scope("dw1"):
            mlp_weight_grads()
        grad_to_mate(l, 0)

        def clear(i):
            dkv[blk(i, 64), :] = jnp.zeros((64, KB), F32)

        loop(SEQ // 64, clear)

        def second_half(ii):
            jj = PAIRS - 1 - ii

            @when(ii == 1)
            def _():
                @when(l < LAYERS - 1)
                def _():
                    grad_home(l + 1, 0)

                grad_across(l, 0)

            with jax.named_scope("B2"):
                attn_back(l, jj, 1)

            @when(ii > 0)
            def _():
                with jax.named_scope("B3"):
                    qkv_back(l, 2 * jj + 2)

            with jax.named_scope("B2"):
                attn_back(l, jj, 0)
            with jax.named_scope("B3"):
                qkv_back(l, 2 * jj + 1)

        loop(PAIRS, second_half)
        qkv_back(l, 0)
        with jax.named_scope("dw2"):
            a_q[...] = tn(buf_b[:, 0:QKV], buf_a[...])
            a_o[...] = tn(os_[l], buf_c[...])
        grad_to_mate(l, 1)
        loop(NJ, lambda j: wait_dma(pk.at[j], dk_s.at[j]))

    loop(LAYERS, backward_layer)
    line.drain(FWD + LAYERS * SLOTS)
    grad_across(0, 1)
    loop(NJ, lambda i: finish_layer(0, NJ - 1 - i))
    for s in range(LAYERS):
        @when(p != s)
        def _():
            send(sm.at[s], rsm.at[p], sm_s.at[s], sm_r.at[p], {"pp": s})
    grad_home(1, 1)
    grad_home(0, 0)
    grad_home(0, 1)
    for s in range(LAYERS):
        @when(p != s)
        def _():
            wait_dma(sm.at[s], sm_s.at[s])
            wait_dma(rsm.at[s], sm_r.at[s])
    rsm[p] = sm[p]
    o_sm[...] = (rsm[0] + rsm[1]) + (rsm[2] + rsm[3])

    def sent(j):
        wait_dma(gcur.at[chunk(0)], ho_s.at[j])
        wait_dma(gcur.at[chunk(0)], gi_s.at[j])

    loop(NJ, sent)
    for k in range(1, LAYERS):
        wait_dma(h_out.at[0, pl.ds(0, ROWS)], ho_r.at[(p + k) % LAYERS])
        wait_dma(g_in.at[0, pl.ds(0, ROWS)], gi_r.at[(p + k) % LAYERS])
    for g, items in enumerate(groups):
        for k, (_, _, far, _) in enumerate(items):
            wait_dma(far, o_sem.at[g, k])
    for k in every:
        wait_dma(w_vm[k].at[0], w_send.at[0, k])
        wait_dma(w_vm[k].at[0], w_send.at[1, k])
        wait_dma(w_vm[k].at[0], w_fwd.at[k])
    line.close()


def run_layers(*args):
    hbm = pl.BlockSpec(memory_space=pl.ANY)
    dma = pltpu.SemaphoreType.DMA
    slots = pltpu.VMEM((SLOTS, CH, D), BF)
    slot_sem = dma((SLOTS,))
    chunk_sem = dma((NJ,))
    stage_sem = dma((LAYERS,))
    pair_sem = dma((2, 2))

    def bf(*shape):
        return pltpu.VMEM(shape, BF)

    def f32(*shape):
        return pltpu.VMEM(shape, F32)

    grad_shapes = ((D, D), (D, D), (QKV, D), (W, D))
    grads = [f32(*shape) for shape in grad_shapes]
    acts = jax.ShapeDtypeStruct((2, SEQ, D), BF)
    return pl.pallas_call(
        decoder_kernel,
        out_shape=[acts, acts, *(jax.ShapeDtypeStruct(shape, F32) for shape in (*grad_shapes, (SMALL, D)))],
        in_specs=[hbm] * len(args),
        out_specs=[hbm] * 6 + [pl.BlockSpec(memory_space=pltpu.VMEM)],
        scratch_shapes=[
            bf(LAYERS, QKV, D), bf(LAYERS, W, D), bf(LAYERS, D, D), bf(LAYERS, D, D), bf(LAYERS, SMALL, D),
            bf(LAYERS, SEQ, KB), bf(LAYERS + 1, ROWS, D), bf(LAYERS, ROWS, D), bf(LAYERS, ROWS, W), bf(LAYERS, ROWS, W),
            f32(LAYERS, NJ * 8, KB), f32(PAIRS, KB, WIDE), f32(KB, W), f32(KB, W),
            bf(ROWS, D), f32(ROWS, D), f32(SEQ, KB), f32(NJ, CH, KB), bf(ROWS, D), bf(ROWS, D), bf(ROWS, D), f32(KB, W),
            *grads, *grads, *grads, f32(LAYERS, SMALL, D), f32(LAYERS, SMALL, D),
            *[slots] * 4, *[slot_sem] * 5,
            chunk_sem, dma((len(args) - 2,)), dma((2, len(args) - 2)), dma((LAYERS, len(args) - 2)), dma((len(args) - 2,)),
            chunk_sem, chunk_sem, chunk_sem, stage_sem,
            chunk_sem, chunk_sem, chunk_sem, chunk_sem, stage_sem, *[pair_sem] * 5, stage_sem, stage_sem,
        ],
        compiler_params=pltpu.CompilerParams(collective_id=0, has_side_effects=True, vmem_limit_bytes=67043328),
        name="decoder_layers",
    )(*args)


def solution(mesh):
    def program(x_in, dy_out, w_qkv, b_qkv, w_out, b_out, ln_par, w_fc1, b_fc1, w_fc2, b_fc2):
        layers, parts, _, heads, width = w_qkv.shape
        wq = w_qkv.transpose(0, 1, 3, 4, 2).reshape(QKV, D)
        bq = jnp.pad(b_qkv.reshape(1, QKV), ((0, 0), (0, D - QKV)))
        ws = jnp.concatenate([ln_par.reshape(4, D), b_out, b_fc2, b_fc1, bq, jnp.zeros((8, D), BF)], axis=0)
        h_out, g_in, d_w1, d_w2, d_q, d_o, sm = run_layers(
            x_in.reshape(2, SEQ, D), dy_out.reshape(2, SEQ, D), wq, w_out.reshape(W, D), w_fc1.reshape(D, D), w_fc2.reshape(D, D), ws)
        acts = (layers, *x_in.shape)
        return (h_out.reshape(acts), g_in.reshape(acts),
                d_q.reshape(layers, parts, heads, width, D).transpose(0, 1, 4, 2, 3), sm[BQKV, :QKV].reshape(b_qkv.shape),
                d_o.reshape(w_out.shape), row(sm, BOUT), sm[GAIN1:BOUT].reshape(ln_par.shape),
                d_w1.reshape(w_fc1.shape), row(sm, BFC1), d_w2.reshape(w_fc2.shape), row(sm, BFC2))

    act_spec = P(NO, "dp", NO, NO)
    arg_specs = (act_spec, act_spec,
                 P("pp", NO, NO, "tp", NO), P("pp", NO, "tp", NO), P("pp", "tp", NO, NO),
                 P("pp", NO), P("pp", NO, NO), P("pp", NO, "tp"), P("pp", "tp"),
                 P("pp", "tp", NO), P("pp", NO))
    stage_spec = P("pp", NO, "dp", NO, NO)
    grad_axes = ("dp", "pp")
    result_specs = (stage_spec, stage_spec,
                    P(grad_axes, NO, NO, "tp", NO), P(grad_axes, NO, "tp", NO), P(grad_axes, "tp", NO, NO),
                    P(grad_axes, NO), P(grad_axes, NO, NO), P(grad_axes, NO, "tp"), P(grad_axes, "tp"),
                    P(grad_axes, "tp", NO), P(grad_axes, NO))
    return jax.shard_map(program, mesh=mesh, in_specs=arg_specs, out_specs=result_specs, check_vma=False)
```

```python
import jax
import jax.numpy as jnp
from jax import lax
from jax.experimental import pallas as pl
from jax.experimental.pallas import tpu as pltpu
from jax.sharding import PartitionSpec as P

LN_EPS = 1e-5
BF = jnp.bfloat16
F32 = jnp.float32
MESH = pl.DeviceIdType.MESH

LAYERS = 4
SEQ = 2048
D = 512
CH = 128
NJ = 8
PAIRS = NJ // 2
ROWS = CH * NJ
SLOTS = 2 * NJ
FWD = LAYERS * SLOTS
W = 128
QKV = 3 * W
KB = 256
WIDE = 2 * KB
SMALL = 16
GELU_C = 0.7978845608028654
GELU_A = 0.044715
MASKED = -1e30
NO = None
GAIN1, SHIFT1, GAIN2, SHIFT2, BOUT, BFC2, BFC1, BQKV = range(8)


def nn(a, b):
    return lax.dot_general(a, b, (((1,), (0,)), ((), ())), preferred_element_type=F32)


def nt(a, b):
    return lax.dot_general(a, b, (((1,), (1,)), ((), ())), preferred_element_type=F32)


def tn(a, b):
    return lax.dot_general(a, b, (((0,), (0,)), ((), ())), preferred_element_type=F32)


def ln_stats(x_wide):
    mean = jnp.mean(x_wide, axis=-1, keepdims=True)
    cent = x_wide - mean
    var = jnp.mean(cent * cent, axis=-1, keepdims=True)
    rstd = lax.rsqrt(var + LN_EPS)
    return cent * rstd, rstd


def ln_back(dy, xhat, rstd, gain):
    dxhat = dy * gain
    m1 = jnp.mean(dxhat, axis=-1, keepdims=True)
    m2 = jnp.mean(dxhat * xhat, axis=-1, keepdims=True)
    return rstd * (dxhat - m1 - xhat * m2)


def colsum(v):
    return jnp.sum(v, axis=0, keepdims=True)


def row(small, r):
    return small[r:r + 1]


def blk(i, n):
    return pl.ds(pl.multiple_of(i * n, n), n)


def chunk(j):
    return blk(j, CH)


def loop(n, body):
    def step(i, carry):
        body(i)
        return carry

    lax.fori_loop(0, n, step, 0)


when = pl.when


def wait_dma(ref, sem):
    pltpu.make_async_copy(ref, ref, sem).wait()


def local(src, dst, sem):
    pltpu.make_async_copy(src, dst, sem).start()


def send(src, dst, ssem, rsem, dev):
    pltpu.make_async_remote_copy(src, dst, ssem, rsem, device_id=dev, device_id_type=MESH).start()


class Place:
    def __init__(self):
        self.z = lax.axis_index("tp")
        self.p = lax.axis_index("pp")
        self.y = self.p // 2
        self.c = self.p % 2
        self.hub = (self.z == 1) | (self.z == 2)
        self.leaf = jnp.logical_not(self.hub)
        self.my_hub = {"tp": jnp.where(self.z == 0, 1, 2)}
        self.my_leaf = {"tp": jnp.where(self.z == 1, 0, 3)}
        self.other_hub = {"tp": 3 - self.z}
        self.mate = {"pp": self.p + 1 - 2 * self.c}
        self.across = {"pp": 2 * (1 - self.y) + self.c}

    def rows_of(self, j):
        return chunk(2 * j + (self.c + j) % 2)

    def mate_rows(self, j):
        return chunk(2 * j + (self.c + j + 1) % 2)

    def enter(self):
        bar = pltpu.get_barrier_semaphore()

        def greet(dev):
            pl.semaphore_signal(bar, inc=1, device_id=dev, device_id_type=MESH)

        for k in range(1, 4):
            greet({"pp": (self.p + k) % 4})
            greet({"tp": (self.z + k) % 4})

        pl.semaphore_wait(bar, 6)


def is_gather(e):
    return (e < FWD) & (e % SLOTS < NJ)


class LineSum:
    def __init__(self, at, gather, part, lbuf, hbuf, fin, s1, s2, r_l, r_h, r_f):
        self.gather = gather
        self.at, self.part, self.lbuf, self.hbuf, self.fin = at, part, lbuf, hbuf, fin
        self.s1, self.s2, self.r_l, self.r_h, self.r_f = s1, s2, r_l, r_h, r_f

    def emit(self, e, value):
        slot = e % SLOTS

        @when((e >= SLOTS) & jnp.logical_not(is_gather(e - SLOTS)))
        def _():
            wait_dma(self.part.at[slot], self.s1.at[slot])

        self.part[slot] = value.astype(BF)

        @when(self.at.leaf)
        def _():
            send(self.part.at[slot], self.lbuf.at[slot], self.s1.at[slot], self.r_l.at[slot], self.at.my_hub)

        self.serve(e)

    def serve(self, e):
        for back, mine, other in ((2, self.serve_first, self.gather.serve_first), (4, self.serve_second, self.gather.serve_second)):
            mine(e - back)

            @when(self.at.hub & (e >= back) & is_gather(e - back))
            def _():
                other((e - back + SLOTS) % SLOTS)

    def serve_first(self, e):
        slot = (e + SLOTS) % SLOTS

        @when(self.at.hub & (e >= 0) & jnp.logical_not(is_gather(e)))
        def _():
            wait_dma(self.lbuf.at[slot], self.r_l.at[slot])
            self.part[slot] = (self.part[slot].astype(F32) + self.lbuf[slot].astype(F32)).astype(BF)
            send(self.part.at[slot], self.hbuf.at[slot], self.s1.at[slot], self.r_h.at[slot], self.at.other_hub)

    def serve_second(self, e):
        slot = (e + SLOTS) % SLOTS

        @when(self.at.hub & (e >= 0) & jnp.logical_not(is_gather(e)))
        def _():
            wait_dma(self.hbuf.at[slot], self.r_h.at[slot])

            @when((e >= SLOTS) & jnp.logical_not(is_gather(e - SLOTS)))
            def _():
                wait_dma(self.fin.at[slot], self.s2.at[slot])

            self.fin[slot] = (self.part[slot].astype(F32) + self.hbuf[slot].astype(F32)).astype(BF)
            send(self.fin.at[slot], self.fin.at[slot], self.s2.at[slot], self.r_f.at[slot], self.at.my_leaf)

    def get(self, slot):
        @when(self.at.leaf)
        def _():
            wait_dma(self.fin.at[slot], self.r_f.at[slot])

        return self.fin[slot].astype(F32)

    def close(self):
        def body(slot):
            wait_dma(self.part.at[slot], self.s1.at[slot])

            @when(self.at.hub)
            def _():
                wait_dma(self.fin.at[slot], self.s2.at[slot])

        loop(SLOTS, body)


class LineGather:
    def __init__(self, at, buf, s_a, s_b, s_c, r_a, r_b):
        self.at, self.buf, self.s_a, self.s_b, self.s_c, self.r_a, self.r_b = at, buf, s_a, s_b, s_c, r_a, r_b
        side = at.z // 2
        self.mine, self.theirs = pl.ds(2 * side, 2), pl.ds(2 - 2 * side, 2)

    def sent(self, j):
        own, pair = self.buf.at[j, 0], self.buf.at[j, pl.ds(0, 2)]
        wait_dma(own, self.s_a.at[j])

        @when(self.at.hub)
        def _():
            wait_dma(pair, self.s_b.at[j])
            wait_dma(pair, self.s_c.at[j])

    def emit(self, j, value):
        at = self.at
        self.buf[j, at.z] = value
        own = self.buf.at[j, at.z]

        @when(at.leaf)
        def _():
            send(own, own, self.s_a.at[j], self.r_a.at[j], at.my_hub)

        @when(at.hub)
        def _():
            send(own, own, self.s_a.at[j], self.r_a.at[j], at.my_leaf)

    def serve_first(self, j):
        wait_dma(self.buf.at[j, 0], self.r_a.at[j])
        pair = self.buf.at[j, self.mine]
        send(pair, pair, self.s_b.at[j], self.r_b.at[j], self.at.other_hub)

    def serve_second(self, j):
        pair = self.buf.at[j, self.theirs]
        wait_dma(pair, self.r_b.at[j])
        send(pair, pair, self.s_c.at[j], self.r_b.at[j], self.at.my_leaf)

    def get(self, j):
        @when(self.at.leaf)
        def _():
            wait_dma(self.buf.at[j, 0], self.r_a.at[j])
            wait_dma(self.buf.at[j, self.theirs], self.r_b.at[j])

        return jnp.concatenate([self.buf[j, k] for k in range(4)], axis=1)


def head_stack(v):
    first = lax.broadcasted_iota(jnp.int32, v.shape, 1) < W // 2
    zero = jnp.zeros_like(v)
    return jnp.concatenate([jnp.where(first, v, zero), jnp.where(first, zero, v)], axis=0)


def head_merge(v):
    first = lax.broadcasted_iota(jnp.int32, (CH, W), 1) < W // 2
    return jnp.where(first, v[:CH], v[CH:])


def fold(v, op):
    out = v[:, :W]
    for k in range(1, v.shape[1] // W):
        out = op(out, v[:, k * W:(k + 1) * W])
    return out


def decoder_kernel(x_in, dy, wq, wo, w1, w2, ws,
                   h_out, g_in, o_w1, o_w2, o_q, o_o, o_sm,
                   wsv, wqv, w1v, w2v, wov, kv, xs, xm, qs, os_, lses, scores, acc, lsum,
                   gcur, gm, dkv, pk, h1s, dqkvs, gms, h2p, dprep, ap, dq_acc, xm_far, g_far,
                   a_w1, a_w2, a_q, a_o, d_w1, d_w2, d_q, d_o, y_w1, y_w2, y_q, y_o, sm, rsm,
                   part, lbuf, hbuf, fin, s1, s2, r_l, r_h, r_f, og, gs_a, gs_b, gs_c, gr_a, gr_b,
                   x_sem, wz_s, wz_r, w_local, w_send, w_recv, w_fwd, kv_s, kv_r, ho_s, ho_r,
                   dy_sem, dk_s, dk_r, gi_s, gi_r, d_s, d_r, y_s, y_r, o_sem, sm_s, sm_r, xf_s, xf_r, gf_s, gf_r):
    at = Place()
    gather = LineGather(at, og, gs_a, gs_b, gs_c, gr_a, gr_b)
    line = LineSum(at, gather, part, lbuf, hbuf, fin, s1, s2, r_l, r_h, r_f)
    y, c, p = at.y, at.c, at.p
    w_hbm = (ws, wq, w1, w2)
    w_vm = (wsv, wqv, w1v, w2v, wov)
    every = range(len(w_vm))
    at_once, group_a, group_m, out_proj = every[:4], every[:2], every[2:], every[4:]
    wo_mine = wov.at[p, chunk(at.z)]

    for j in range(NJ):
        local(x_in.at[y, at.rows_of(j)], xs.at[0, chunk(j)], x_sem.at[j])
    for k in at_once:
        local(w_hbm[k], w_vm[k].at[p], w_local.at[k])
    local(wo, wo_mine, w_local.at[4])

    at.enter()

    def spread(group, way, dev):
        for k in group:
            src = w_hbm[k] if k < 4 else wov.at[p]
            send(src, w_vm[k].at[p], w_send.at[way, k], w_recv.at[p, k], dev)

    @when(c == 0)
    def _():
        spread(at_once, 1, at.across)

    spread(at_once, 0, at.mate)
    for k in range(1, 4):
        send(wo, wo_mine, wz_s.at[k], wz_r.at[at.z], {"tp": (at.z + k) % 4})

    def spread_out_proj():
        wait_dma(wo_mine, w_local.at[4])
        for k in range(1, 4):
            wait_dma(wo_mine, wz_r.at[(at.z + k) % 4])
            wait_dma(wo_mine, wz_s.at[k])
        spread(out_proj, 0, at.mate)

        @when(c == 0)
        def _():
            spread(out_proj, 1, at.across)
    for j in range(NJ):
        local(dy.at[y, at.rows_of(j)], gcur.at[chunk(j)], dy_sem.at[j])

    def weights_ready(s, group):
        @when(p == s)
        def _():
            for k in group:
                if k < 4:
                    wait_dma(w_vm[k].at[p], w_local.at[k])

        @when(p != s)
        def _():
            for k in group:
                wait_dma(w_vm[k].at[s], w_recv.at[s, k])

        @when((y != s // 2) & (c == s % 2))
        def _():
            for k in group:
                send(w_vm[k].at[s], w_vm[k].at[s], w_fwd.at[k], w_recv.at[s, k], at.mate)

    def send_home(l, src, dst, ssem, rsem):
        @when(p == l)
        def _():
            local(src, dst, ssem)

        @when(p != l)
        def _():
            send(src, dst, ssem, rsem.at[p], {"pp": l})

    weights_ready(0, group_a)

    def finish_y(l, j):
        rows = chunk(j)
        total = line.get(NJ + j)
        out = (xm[l, rows, :].astype(F32) + total + row(wsv[l].astype(F32), BFC2)).astype(BF)

        @when(l > 0)
        def _():
            wait_dma(gcur.at[rows], ho_s.at[j])

        xs[l + 1, rows, :] = out
        send_home(l, xs.at[l + 1, rows], h_out.at[y, at.rows_of(j)], ho_s.at[j], ho_r)

    def attn_op(l, jj, odd):
        j = 2 * jj + odd
        rows = chunk(j)

        @when(l == 0)
        def _():
            wait_dma(xs.at[0, rows], x_sem.at[j])

        @when(l > 0)
        def _():
            finish_y(l - 1, j)

        small = wsv[l].astype(F32)
        xhat, _ = ln_stats(xs[l, rows, :].astype(F32))
        h1 = (xhat * row(small, GAIN1) + row(small, SHIFT1)).astype(BF)
        qkv = (nt(h1, wqv[l]) + row(small, BQKV)[:, :QKV]).astype(BF)
        q = qkv[:, :W]
        mine = at.rows_of(j)
        kv[l, mine, :] = qkv[:, W:]
        send(kv.at[l, mine], kv.at[l, mine], kv_s.at[j], kv_r.at[j], at.mate)
        qs[l, rows, :] = q
        q2 = head_stack(q * jnp.asarray(0.125, BF))

        def pass_one(kb, best):
            s = nt(q2, kv[l, blk(kb, WIDE), 0:W])
            scores[kb] = s
            return jnp.maximum(best, fold(s, jnp.maximum))

        best = lax.fori_loop(0, jj, pass_one, jnp.full((KB, W), MASKED, F32))
        wait_dma(kv.at[l, mine], kv_r.at[j])
        width = KB * (1 + odd)
        tail = pl.ds(pl.multiple_of(jj * WIDE, WIDE), width)
        s = nt(q2, kv[l, tail, 0:W])
        pos = lax.broadcasted_iota(jnp.int32, (KB, width), 0) % CH + (KB * odd + CH * ((c + odd) % 2))
        s = jnp.where(pos >= lax.broadcasted_iota(jnp.int32, (KB, width), 1), s, MASKED)
        scores[jj, :, 0:width] = s
        top = jnp.max(jnp.maximum(best, fold(s, jnp.maximum)), axis=-1, keepdims=True)
        acc[...] = jnp.zeros_like(acc)
        lsum[...] = jnp.zeros_like(lsum)

        def weigh(s, keys):
            e = jnp.exp(s - top)
            lsum[...] += fold(e, jnp.add)
            acc[...] += nn(e.astype(BF), kv[l, keys, W:])

        loop(jj, lambda kb: weigh(scores[kb], blk(kb, WIDE)))
        weigh(scores[jj, :, 0:width], tail)
        den = jnp.sum(lsum[...], axis=-1, keepdims=True)
        o = head_merge(acc[...] / den).astype(BF)
        os_[l, rows, :] = o
        lses[l, blk(j, 8), :] = jnp.broadcast_to(top + jnp.log(den), (KB, W)).T[:8]
        gather.emit(j, o)
        line.serve(SLOTS * l + j)

    def mlp_op(l, j):
        rows = chunk(j)
        small = wsv[l].astype(F32)
        gather.sent(j)
        mid = (xs[l, rows, :].astype(F32) + nn(gather.get(j), wov[l]) + row(small, BOUT)).astype(BF)
        xm[l, rows, :] = mid

        @when((l == 0) & (y == 1))
        def _():
            send(xm.at[0, rows], xm_far.at[rows], xf_s.at[j], xf_r.at[j], at.across)

        xhat, _ = ln_stats(mid.astype(F32))
        h2 = (xhat * row(small, GAIN2) + row(small, SHIFT2)).astype(BF)
        u = nn(h2, w1v[l]) + row(small, BFC1)
        a = 0.5 * u * (1.0 + jnp.tanh(GELU_C * (u + GELU_A * u * u * u)))
        line.emit(SLOTS * l + NJ + j, nn(a.astype(BF), w2v[l]))

    def forward_layer(l):
        def attn_pair(jj):
            with jax.named_scope("attn"):
                attn_op(l, jj, 0)
            with jax.named_scope("attn"):
                attn_op(l, jj, 1)

            @when((l == 0) & (jj == 1))
            def _():
                spread_out_proj()

            @when((l == 0) & (jj == PAIRS - 2) & (c == 1))
            def _():
                spread(every, 1, at.across)

        loop(PAIRS, attn_pair)

        @when(l == 0)
        def _():
            weights_ready(0, group_m)

        def mlp_step(j):
            with jax.named_scope("mlp"):
                mlp_op(l, j)

            @when((j == NJ - 2) & (l < LAYERS - 1))
            def _():
                weights_ready(l + 1, every)

        loop(NJ, mlp_step)
        loop(NJ, lambda j: wait_dma(kv.at[0, chunk(0)], kv_s.at[j]))

    for l in range(LAYERS):
        sm[l] = jnp.zeros((SMALL, D), F32)
    loop(LAYERS, forward_layer)

    groups = (((a_w1, d_w1, y_w1, o_w1), (a_w2, d_w2, y_w2, o_w2)), ((a_q, d_q, y_q, o_q), (a_o, d_o, y_o, o_o)))

    def add_into(dst, src):
        def body(i):
            rows = blk(i, 64)
            dst[rows, :] += src[rows, :]

        loop(dst.shape[0] // 64, body)

    def grad_to_mate(l, g):
        @when(c != l % 2)
        def _():
            for k, (own, mid, _, _) in enumerate(groups[g]):
                send(own, mid, d_s.at[g, k], d_r.at[g, k], at.mate)

    def grad_across(l, g):
        @when(c != l % 2)
        def _():
            for k, (own, _, _, _) in enumerate(groups[g]):
                wait_dma(own, d_s.at[g, k])

        @when(c == l % 2)
        def _():
            for k, (own, mid, far, _) in enumerate(groups[g]):
                wait_dma(mid, d_r.at[g, k])
                add_into(mid, own)

                @when(y != l // 2)
                def _():
                    send(mid, far, y_s.at[g, k], y_r.at[g, k], at.across)

    def grad_home(l, g):
        @when((c == l % 2) & (y != l // 2))
        def _():
            for k, (_, mid, _, _) in enumerate(groups[g]):
                wait_dma(mid, y_s.at[g, k])

        @when(p == l)
        def _():
            for k, (_, mid, far, out) in enumerate(groups[g]):
                wait_dma(far, y_r.at[g, k])
                add_into(far, mid)
                local(far, out, o_sem.at[g, k])

    def add_small(l, r, value):
        sm[l, r:r + 1, :] += value

    def finish_layer(l, j):
        rows = chunk(j)
        dh1 = line.get(SLOTS - 1 - j)
        xhat, rstd = ln_stats(xs[l, rows, :].astype(F32))
        add_small(l, GAIN1, colsum(dh1 * xhat))
        add_small(l, SHIFT1, colsum(dh1))
        out = (gm[rows, :] + ln_back(dh1, xhat, rstd, row(wsv[l].astype(F32), GAIN1))).astype(BF)

        @when(l < LAYERS - 1)
        def _():
            wait_dma(gcur.at[rows], gi_s.at[j])

        gcur[rows, :] = out

        @when((l == 1) & (y == 1))
        def _():
            send(gcur.at[rows], g_far.at[rows], gi_s.at[j], gf_r.at[j], at.across)

        @when((l != 1) | (y == 0))
        def _():
            send_home(l, gcur.at[rows], g_in.at[y, at.rows_of(j)], gi_s.at[j], gi_r)

    def mlp_back(l, i):
        j = NJ - 1 - i
        rows = chunk(j)

        @when(l == LAYERS - 1)
        def _():
            wait_dma(gcur.at[rows], dy_sem.at[j])
            finish_y(l, i)

        @when(l < LAYERS - 1)
        def _():
            finish_layer(l + 1, j)

        g = gcur[rows, :]
        dpre = mlp_grads(l, j, xm[l, rows, :], g)
        add_small(l, BFC2, colsum(g.astype(F32)))
        add_small(l, BFC1, colsum(dpre))
        line.emit(FWD + SLOTS * (LAYERS - 1 - l) + i, nt(dpre.astype(BF), w1v[l]))

        @when((l > 0) | (y == 0))
        def _():
            mlp_weight_grads(i, gcur)

    def mlp_grads(l, j, mid, g):
        small = wsv[l].astype(F32)
        xhat, _ = ln_stats(mid.astype(F32))
        h2 = (xhat * row(small, GAIN2) + row(small, SHIFT2)).astype(BF)
        u = nn(h2, w1v[l]) + row(small, BFC1)
        t = jnp.tanh(GELU_C * (u + GELU_A * u * u * u))
        half = 0.5 * (1.0 + t)
        slope = half + 0.5 * u * (1.0 - t * t) * (GELU_C * (1.0 + 3.0 * GELU_A * u * u))
        dpre = nt(g, w2v[l]) * slope
        spot = chunk(j % 2)
        h2p[spot, :] = h2
        dprep[spot, :] = dpre.astype(BF)
        ap[spot, :] = (u * half).astype(BF)
        return dpre

    def mlp_weight_grads(i, g_ref):
        grads = blk((NJ - 1 - i) // 2, KB)

        @when(i == 1)
        def _():
            a_w1[...] = tn(h2p[...], dprep[...])
            a_w2[...] = tn(ap[...], g_ref[grads, :])

        @when((i > 1) & (i % 2 == 1))
        def _():
            a_w1[...] += tn(h2p[...], dprep[...])
            a_w2[...] += tn(ap[...], g_ref[grads, :])

    def far_mlp_weight_grads():
        def body(i):
            j = NJ - 1 - i
            rows = chunk(j)
            wait_dma(xm_far.at[rows], xf_r.at[j])
            wait_dma(g_far.at[rows], gf_r.at[j])
            dst = g_in.at[1, at.rows_of(j)]

            @when(c == 1)
            def _():
                local(g_far.at[rows], dst, gi_r.at[3])

            @when(c == 0)
            def _():
                send(g_far.at[rows], dst, gf_s.at[j], gi_r.at[2], at.mate)

            mlp_grads(0, j, xm_far[rows, :], g_far[rows, :])

            @when(i % 2 == 1)
            def _():
                a_w1[...] += tn(h2p[...], dprep[...])
                a_w2[...] += tn(ap[...], g_far[blk(j // 2, KB), :])

        loop(NJ, body)

        @when(c == 1)
        def _():
            for k, (own, mid, _, _) in enumerate(groups[0]):
                send(own, mid, d_s.at[0, k], d_r.at[0, k], at.mate)
            for k, (own, _, _, _) in enumerate(groups[0]):
                wait_dma(own, d_s.at[0, k])

        @when(c == 0)
        def _():
            for k, (own, mid, _, out) in enumerate(groups[0]):
                wait_dma(mid, d_r.at[0, k])
                add_into(mid, own)
                local(mid, out, o_sem.at[0, k])
            loop(NJ, lambda j: wait_dma(g_far.at[chunk(j)], gf_s.at[j]))

    def attn_weight_grads(l):
        a_q[...] = tn(dqkvs[...], h1s[...])
        a_o[...] = tn(os_[l], gms[...])
        grad_to_mate(l, 1)

    def attn_back(l, jj, odd):
        j = 2 * jj + odd
        rows = chunk(j)
        small = wsv[l].astype(F32)
        dh2 = line.get(NJ - 1 - j)
        xhat, rstd = ln_stats(xm[l, rows, :].astype(F32))
        add_small(l, GAIN2, colsum(dh2 * xhat))
        add_small(l, SHIFT2, colsum(dh2))
        wide = gcur[rows, :].astype(F32) + ln_back(dh2, xhat, rstd, row(small, GAIN2))
        gm[rows, :] = wide
        add_small(l, BOUT, colsum(wide))
        gmid = wide.astype(BF)
        gms[rows, :] = gmid
        do = nt(gmid, wov[l, chunk(at.z), :]).astype(BF)
        delta = jnp.sum(head_stack(do.astype(F32) * os_[l, rows, :].astype(F32)), axis=-1, keepdims=True)
        delta = jnp.broadcast_to(delta, (KB, W)).T[0:1]
        lse = lses[l, blk(j, 8), :][0:1]
        q2 = head_stack(qs[l, rows, :] * jnp.asarray(0.125, BF))
        do2 = head_stack(do)
        dq_acc[...] = jnp.zeros_like(dq_acc)

        def block(keys, width, masked):
            k = kv[l, keys, 0:W]
            st = nt(k, q2)
            if masked:
                pos = lax.broadcasted_iota(jnp.int32, (width, KB), 1) % CH + (KB * odd + CH * ((c + odd) % 2))
                st = jnp.where(pos >= lax.broadcasted_iota(jnp.int32, (width, KB), 0), st, MASKED)
            pt = jnp.exp(st - lse)
            dst = (pt * (nt(kv[l, keys, W:], do2) - delta)).astype(BF)
            dk = nn(dst, q2)
            dv = nn(pt.astype(BF), do2)
            dq_acc[...] += tn(dst, k)
            dkv[keys, 0:W] += dk
            dkv[keys, W:] += dv

        loop(jj, lambda kb: block(blk(kb, WIDE), WIDE, False))
        width = KB * (1 + odd)
        block(pl.ds(pl.multiple_of(jj * WIDE, WIDE), width), width, True)
        dqkvs[rows, 0:W] = (head_merge(dq_acc[...]) * 0.125).astype(BF)
        send(dkv.at[at.mate_rows(j)], pk.at[j], dk_s.at[j], dk_r.at[j], at.mate)

    def qkv_back(l, j):
        rows = chunk(j)
        small = wsv[l].astype(F32)
        xhat, _ = ln_stats(xs[l, rows, :].astype(F32))
        h1s[rows, :] = (xhat * row(small, GAIN1) + row(small, SHIFT1)).astype(BF)
        wait_dma(pk.at[j], dk_r.at[j])
        dkv_own = (dkv[at.rows_of(j), :] + pk[j]).astype(BF)
        dqkvs[rows, W:] = dkv_own
        dqkv = jnp.concatenate([dqkvs[rows, 0:W], dkv_own], axis=1)
        sm[l, BQKV:BQKV + 1, 0:QKV] += colsum(dqkv.astype(F32))
        line.emit(FWD + SLOTS * (LAYERS - l) - 1 - j, nn(dqkv, wqv[l]))

    def backward_layer(n):
        l = LAYERS - 1 - n

        def first_half(i):
            @when((i == 0) & (l < LAYERS - 1))
            def _():
                attn_weight_grads(l + 1)

            @when(i == 2)
            def _():
                @when(l < LAYERS - 2)
                def _():
                    grad_home(l + 2, 1)

                @when(l < LAYERS - 1)
                def _():
                    grad_across(l + 1, 1)

            with jax.named_scope("B1"):
                mlp_back(l, i)

        loop(NJ, first_half)

        @when(l > 0)
        def _():
            grad_to_mate(l, 0)

        def clear(i):
            dkv[blk(i, 64), :] = jnp.zeros((64, KB), F32)

        loop(SEQ // 64, clear)

        def second_half(ii):
            jj = PAIRS - 1 - ii

            @when((ii == 1) & (l < LAYERS - 1))
            def _():
                grad_home(l + 1, 0)

            with jax.named_scope("B2"):
                attn_back(l, jj, 1)

            @when((ii == 0) & (l > 0))
            def _():
                grad_across(l, 0)

            @when(ii > 0)
            def _():
                with jax.named_scope("B3"):
                    qkv_back(l, 2 * jj + 2)

            with jax.named_scope("B2"):
                attn_back(l, jj, 0)
            with jax.named_scope("B3"):
                qkv_back(l, 2 * jj + 1)

        loop(PAIRS, second_half)
        qkv_back(l, 0)
        loop(NJ, lambda j: wait_dma(pk.at[j], dk_s.at[j]))

    loop(LAYERS, backward_layer)
    attn_weight_grads(0)
    grad_across(0, 1)
    last = FWD + LAYERS * SLOTS - 1

    def finish_last(i):
        @when((i == 1) | (i == 2))
        def _():
            line.serve_first(last - 2 + i)

        @when(i > 3)
        def _():
            line.serve_second(last - NJ + 1 + i)

        finish_layer(0, NJ - 1 - i)

    loop(NJ, finish_last)
    for s in range(LAYERS):
        @when(p != s)
        def _():
            send(sm.at[s], rsm.at[p], sm_s.at[s], sm_r.at[p], {"pp": s})

    @when(y == 0)
    def _():
        far_mlp_weight_grads()

    @when(y == 1)
    def _():
        loop(NJ, lambda j: wait_dma(xm.at[0, chunk(j)], xf_s.at[j]))

    grad_home(1, 1)
    grad_home(0, 1)
    for s in range(LAYERS):
        @when(p != s)
        def _():
            wait_dma(sm.at[s], sm_s.at[s])
            wait_dma(rsm.at[s], sm_r.at[s])
    rsm[p] = sm[p]
    o_sm[...] = (rsm[0] + rsm[1]) + (rsm[2] + rsm[3])

    def sent(j):
        wait_dma(gcur.at[chunk(0)], ho_s.at[j])
        wait_dma(gcur.at[chunk(0)], gi_s.at[j])

    loop(NJ, sent)
    for k in range(1, LAYERS):
        wait_dma(h_out.at[0, pl.ds(0, ROWS)], ho_r.at[(p + k) % LAYERS])
        wait_dma(g_in.at[0, pl.ds(0, ROWS)], gi_r.at[(p + k) % LAYERS])
    for g, items in enumerate(groups):
        for k, (_, _, far, _) in enumerate(items):
            wait_dma(far, o_sem.at[g, k])
    for k in every:
        wait_dma(w_vm[k].at[0], w_send.at[0, k])
        wait_dma(w_vm[k].at[0], w_send.at[1, k])
        wait_dma(w_vm[k].at[0], w_fwd.at[k])
    line.close()


def run_layers(*args):
    hbm = pl.BlockSpec(memory_space=pl.ANY)
    dma = pltpu.SemaphoreType.DMA
    slots = pltpu.VMEM((SLOTS, CH, D), BF)
    slot_sem = dma((SLOTS,))
    chunk_sem = dma((NJ,))
    stage_sem = dma((LAYERS,))
    pair_sem = dma((2, 2))

    def bf(*shape):
        return pltpu.VMEM(shape, BF)

    def f32(*shape):
        return pltpu.VMEM(shape, F32)

    grad_shapes = ((D, D), (D, D), (QKV, D), (W, D))
    grads = [f32(*shape) for shape in grad_shapes]
    acts = jax.ShapeDtypeStruct((2, SEQ, D), BF)
    return pl.pallas_call(
        decoder_kernel,
        out_shape=[acts, acts, *(jax.ShapeDtypeStruct(shape, F32) for shape in (*grad_shapes, (SMALL, D)))],
        in_specs=[hbm] * len(args),
        out_specs=[hbm] * 6 + [pl.BlockSpec(memory_space=pltpu.VMEM)],
        scratch_shapes=[
            bf(LAYERS, SMALL, D), bf(LAYERS, QKV, D), *[bf(LAYERS, D, D)] * 3,
            bf(LAYERS, SEQ, KB), bf(LAYERS + 1, ROWS, D), bf(LAYERS, ROWS, D), bf(LAYERS, ROWS, W), bf(LAYERS, ROWS, W),
            f32(LAYERS, NJ * 8, KB), f32(PAIRS, KB, WIDE), f32(KB, W), f32(KB, W),
            bf(ROWS, D), f32(ROWS, D), f32(SEQ, KB), f32(NJ, CH, KB), bf(ROWS, D), bf(ROWS, QKV), bf(ROWS, D), *[bf(KB, D)] * 3, f32(KB, W), bf(ROWS, D), bf(ROWS, D),
            *grads, *grads, *grads, f32(LAYERS, SMALL, D), f32(LAYERS, SMALL, D),
            *[slots] * 4, *[slot_sem] * 5, bf(NJ, 4, CH, W), *[chunk_sem] * 5,
            chunk_sem, stage_sem, stage_sem, dma((len(args) - 2,)), dma((2, len(args) - 2)), dma((LAYERS, len(args) - 2)), dma((len(args) - 2,)),
            chunk_sem, chunk_sem, chunk_sem, stage_sem,
            chunk_sem, chunk_sem, chunk_sem, chunk_sem, stage_sem, *[pair_sem] * 5, stage_sem, stage_sem, *[chunk_sem] * 4,
        ],
        compiler_params=pltpu.CompilerParams(collective_id=0, has_side_effects=True, vmem_limit_bytes=67043328),
        name="decoder_layers",
    )(*args)


def solution(mesh):
    def program(x_in, dy_out, w_qkv, b_qkv, w_out, b_out, ln_par, w_fc1, b_fc1, w_fc2, b_fc2):
        layers, parts, _, heads, width = w_qkv.shape
        wq = w_qkv.transpose(0, 1, 3, 4, 2).reshape(QKV, D)
        bq = jnp.pad(b_qkv.reshape(1, QKV), ((0, 0), (0, D - QKV)))
        ws = jnp.concatenate([ln_par.reshape(4, D), b_out, b_fc2, b_fc1, bq, jnp.zeros((8, D), BF)], axis=0)
        h_out, g_in, d_w1, d_w2, d_q, d_o, sm = run_layers(
            x_in.reshape(2, SEQ, D), dy_out.reshape(2, SEQ, D), wq, w_out.reshape(W, D), w_fc1.reshape(D, D), w_fc2.reshape(D, D), ws)
        acts = (layers, *x_in.shape)
        return (h_out.reshape(acts), g_in.reshape(acts),
                d_q.reshape(layers, parts, heads, width, D).transpose(0, 1, 4, 2, 3), sm[BQKV, :QKV].reshape(b_qkv.shape),
                d_o.reshape(w_out.shape), row(sm, BOUT), sm[GAIN1:BOUT].reshape(ln_par.shape),
                d_w1.reshape(w_fc1.shape), row(sm, BFC1), d_w2.reshape(w_fc2.shape), row(sm, BFC2))

    act_spec = P(NO, "dp", NO, NO)
    arg_specs = (act_spec, act_spec,
                 P("pp", NO, NO, "tp", NO), P("pp", NO, "tp", NO), P("pp", "tp", NO, NO),
                 P("pp", NO), P("pp", NO, NO), P("pp", NO, "tp"), P("pp", "tp"),
                 P("pp", "tp", NO), P("pp", NO))
    stage_spec = P("pp", NO, "dp", NO, NO)
    grad_axes = ("dp", "pp")
    result_specs = (stage_spec, stage_spec,
                    P(grad_axes, NO, NO, "tp", NO), P(grad_axes, NO, "tp", NO), P(grad_axes, "tp", NO, NO),
                    P(grad_axes, NO), P(grad_axes, NO, NO), P(grad_axes, NO, "tp"), P(grad_axes, "tp"),
                    P(grad_axes, "tp", NO), P(grad_axes, NO))
    return jax.shard_map(program, mesh=mesh, in_specs=arg_specs, out_specs=result_specs, check_vma=False)
```

```python
import jax
import jax.numpy as jnp
from jax import lax
from jax.experimental import pallas as pl
from jax.experimental.pallas import tpu as pltpu
from jax.sharding import PartitionSpec as P

LN_EPS = 1e-5
BF = jnp.bfloat16
F32 = jnp.float32
MESH = pl.DeviceIdType.MESH

LAYERS = 4
SEQ = 2048
D = 512
CH = 128
NJ = 8
PAIRS = NJ // 2
ROWS = CH * NJ
SLOTS = 2 * NJ
FWD = LAYERS * SLOTS
W = 128
QKV = 3 * W
KB = 256
WIDE = 2 * KB
SMALL = 16
GELU_C = 0.7978845608028654
GELU_A = 0.044715
MASKED = -1e30
NO = None
GAIN1, SHIFT1, GAIN2, SHIFT2, BOUT, BFC2, BFC1, BQKV = range(8)


def nn(a, b):
    return lax.dot_general(a, b, (((1,), (0,)), ((), ())), preferred_element_type=F32)


def nt(a, b):
    return lax.dot_general(a, b, (((1,), (1,)), ((), ())), preferred_element_type=F32)


def tn(a, b):
    return lax.dot_general(a, b, (((0,), (0,)), ((), ())), preferred_element_type=F32)


def ln_stats(x_wide):
    mean = jnp.mean(x_wide, axis=-1, keepdims=True)
    cent = x_wide - mean
    var = jnp.mean(cent * cent, axis=-1, keepdims=True)
    rstd = lax.rsqrt(var + LN_EPS)
    return cent * rstd, rstd


def ln_back(dy, xhat, rstd, gain):
    dxhat = dy * gain
    m1 = jnp.mean(dxhat, axis=-1, keepdims=True)
    m2 = jnp.mean(dxhat * xhat, axis=-1, keepdims=True)
    return rstd * (dxhat - m1 - xhat * m2)


def colsum(v):
    return jnp.sum(v, axis=0, keepdims=True)


def row(small, r):
    return small[r:r + 1]


def blk(i, n):
    return pl.ds(pl.multiple_of(i * n, n), n)


def chunk(j):
    return blk(j, CH)


def pair(jj):
    return blk(jj, KB)


def loop(n, body):
    def step(i, carry):
        body(i)
        return carry

    lax.fori_loop(0, n, step, 0)


when = pl.when


def wait_dma(ref, sem):
    pltpu.make_async_copy(ref, ref, sem).wait()


def local(src, dst, sem):
    pltpu.make_async_copy(src, dst, sem).start()


def send(src, dst, ssem, rsem, dev):
    pltpu.make_async_remote_copy(src, dst, ssem, rsem, device_id=dev, device_id_type=MESH).start()


class Place:
    def __init__(self):
        self.z = lax.axis_index("tp")
        self.p = lax.axis_index("pp")
        self.y = self.p // 2
        self.c = self.p % 2
        self.hub = (self.z == 1) | (self.z == 2)
        self.leaf = jnp.logical_not(self.hub)
        self.my_hub = {"tp": jnp.where(self.z == 0, 1, 2)}
        self.my_leaf = {"tp": jnp.where(self.z == 1, 0, 3)}
        self.other_hub = {"tp": 3 - self.z}
        self.mate = {"pp": self.p + 1 - 2 * self.c}
        self.across = {"pp": 2 * (1 - self.y) + self.c}

    def rows_of(self, j):
        return chunk(2 * j + (self.c + j) % 2)

    def mate_rows(self, j):
        return chunk(2 * j + (self.c + j + 1) % 2)

    def enter(self):
        bar = pltpu.get_barrier_semaphore()

        def greet(dev):
            pl.semaphore_signal(bar, inc=1, device_id=dev, device_id_type=MESH)

        for k in range(1, 4):
            greet({"pp": (self.p + k) % 4})
            greet({"tp": (self.z + k) % 4})

        pl.semaphore_wait(bar, 6)


def is_gather(e):
    return (e < FWD) & (e % SLOTS < NJ)


class LineSum:
    def __init__(self, at, gather, part, lbuf, hbuf, fin, s1, s2, r_l, r_h, r_f):
        self.gather = gather
        self.at, self.part, self.lbuf, self.hbuf, self.fin = at, part, lbuf, hbuf, fin
        self.s1, self.s2, self.r_l, self.r_h, self.r_f = s1, s2, r_l, r_h, r_f

    def emit(self, e, value):
        slot = e % SLOTS

        @when((e >= SLOTS) & jnp.logical_not(is_gather(e - SLOTS)))
        def _():
            wait_dma(self.part.at[slot], self.s1.at[slot])

        self.part[slot] = value.astype(BF)

        @when(self.at.leaf)
        def _():
            send(self.part.at[slot], self.lbuf.at[slot], self.s1.at[slot], self.r_l.at[slot], self.at.my_hub)

        self.serve(e)

    def serve(self, e):
        for back, mine, other in ((2, self.serve_first, self.gather.serve_first), (4, self.serve_second, self.gather.serve_second)):
            mine(e - back)

            @when(self.at.hub & (e >= back) & is_gather(e - back))
            def _():
                other((e - back + SLOTS) % SLOTS)

    def serve_first(self, e):
        slot = (e + SLOTS) % SLOTS

        @when(self.at.hub & (e >= 0) & jnp.logical_not(is_gather(e)))
        def _():
            wait_dma(self.lbuf.at[slot], self.r_l.at[slot])
            self.part[slot] = (self.part[slot].astype(F32) + self.lbuf[slot].astype(F32)).astype(BF)
            send(self.part.at[slot], self.hbuf.at[slot], self.s1.at[slot], self.r_h.at[slot], self.at.other_hub)

    def serve_second(self, e):
        slot = (e + SLOTS) % SLOTS

        @when(self.at.hub & (e >= 0) & jnp.logical_not(is_gather(e)))
        def _():
            wait_dma(self.hbuf.at[slot], self.r_h.at[slot])

            @when((e >= SLOTS) & jnp.logical_not(is_gather(e - SLOTS)))
            def _():
                wait_dma(self.fin.at[slot], self.s2.at[slot])

            self.fin[slot] = (self.part[slot].astype(F32) + self.hbuf[slot].astype(F32)).astype(BF)
            send(self.fin.at[slot], self.fin.at[slot], self.s2.at[slot], self.r_f.at[slot], self.at.my_leaf)

    def get(self, slot):
        @when(self.at.leaf)
        def _():
            wait_dma(self.fin.at[slot], self.r_f.at[slot])

        return self.fin[slot].astype(F32)

    def close(self):
        def body(slot):
            wait_dma(self.part.at[slot], self.s1.at[slot])

            @when(self.at.hub)
            def _():
                wait_dma(self.fin.at[slot], self.s2.at[slot])

        loop(SLOTS, body)


class LineGather:
    def __init__(self, at, buf, s_a, s_b, s_c, r_a, r_b):
        self.at, self.buf, self.s_a, self.s_b, self.s_c, self.r_a, self.r_b = at, buf, s_a, s_b, s_c, r_a, r_b
        side = at.z // 2
        self.mine, self.theirs = pl.ds(2 * side, 2), pl.ds(2 - 2 * side, 2)

    def sent(self, j):
        own, two = self.buf.at[j, 0], self.buf.at[j, pl.ds(0, 2)]
        wait_dma(own, self.s_a.at[j])

        @when(self.at.hub)
        def _():
            wait_dma(two, self.s_b.at[j])
            wait_dma(two, self.s_c.at[j])

    def emit(self, j, value):
        at = self.at
        self.buf[j, at.z] = value
        own = self.buf.at[j, at.z]

        @when(at.leaf)
        def _():
            send(own, own, self.s_a.at[j], self.r_a.at[j], at.my_hub)

        @when(at.hub)
        def _():
            send(own, own, self.s_a.at[j], self.r_a.at[j], at.my_leaf)

    def serve_first(self, j):
        wait_dma(self.buf.at[j, 0], self.r_a.at[j])
        two = self.buf.at[j, self.mine]
        send(two, two, self.s_b.at[j], self.r_b.at[j], self.at.other_hub)

    def serve_second(self, j):
        two = self.buf.at[j, self.theirs]
        wait_dma(two, self.r_b.at[j])
        send(two, two, self.s_c.at[j], self.r_b.at[j], self.at.my_leaf)

    def get(self, j):
        @when(self.at.leaf)
        def _():
            wait_dma(self.buf.at[j, 0], self.r_a.at[j])
            wait_dma(self.buf.at[j, self.theirs], self.r_b.at[j])

        return jnp.concatenate([self.buf[j, k] for k in range(4)], axis=1)


def head_stack(v):
    first = lax.broadcasted_iota(jnp.int32, v.shape, 1) < W // 2
    zero = jnp.zeros_like(v)
    return jnp.concatenate([jnp.where(first, v, zero), jnp.where(first, zero, v)], axis=0)


def head_merge(v):
    n = v.shape[0] // 2
    first = lax.broadcasted_iota(jnp.int32, (n, W), 1) < W // 2
    return jnp.where(first, v[:n], v[n:])


def as_row(v):
    return jnp.broadcast_to(v, (v.shape[0], W)).T[:8]


def fold(v, op):
    out = v[:, :W]
    for k in range(1, v.shape[1] // W):
        out = op(out, v[:, k * W:(k + 1) * W])
    return out


def decoder_kernel(x_in, dy, wq, wo, w1, w2, ws,
                   h_out, g_in, o_w1, o_w2, o_q, o_o, o_sm,
                   wsv, wqv, w1v, w2v, wov, kv, xs, xm, qs, os_, lses, scores, acc, lsum,
                   gcur, gm, dkv, pk, h1s, dqkvs, gms, h2p, dprep, ap, dq_acc, xm_far, g_far, g_half,
                   a_w1, a_w2, a_q, a_o, d_w1, d_w2, d_q, d_o, y_w1, y_w2, y_q, y_o, sm, rsm,
                   part, lbuf, hbuf, fin, s1, s2, r_l, r_h, r_f, og, gs_a, gs_b, gs_c, gr_a, gr_b,
                   x_sem, wz_s, wz_r, w_local, w_send, w_recv, w_fwd, kv_s, kv_r, ho_s, ho_r,
                   dy_sem, dk_s, dk_r, gi_s, gi_r, d_s, d_r, y_s, y_r, o_sem, sm_s, sm_r, xf_s, xf_r, gf_s, gf_r, gh_r, gx):
    at = Place()
    gather = LineGather(at, og, gs_a, gs_b, gs_c, gr_a, gr_b)
    line = LineSum(at, gather, part, lbuf, hbuf, fin, s1, s2, r_l, r_h, r_f)
    y, c, p = at.y, at.c, at.p
    w_hbm = (ws, wq, w1, w2)
    w_vm = (wsv, wqv, w1v, w2v, wov)
    every = range(len(w_vm))
    at_once, group_a, group_m, out_proj = every[:4], every[:2], every[2:], every[4:]
    wo_mine = wov.at[p, chunk(at.z)]

    for j in range(NJ):
        local(x_in.at[y, at.rows_of(j)], xs.at[0, chunk(j)], x_sem.at[j])
    for k in at_once:
        local(w_hbm[k], w_vm[k].at[p], w_local.at[k])
    local(wo, wo_mine, w_local.at[4])

    at.enter()

    def spread(group, way, dev):
        for k in group:
            src = w_hbm[k] if k < 4 else wov.at[p]
            send(src, w_vm[k].at[p], w_send.at[way, k], w_recv.at[p, k], dev)

    @when(c == 0)
    def _():
        spread(at_once, 1, at.across)

    spread(at_once, 0, at.mate)
    for k in range(1, 4):
        send(wo, wo_mine, wz_s.at[k], wz_r.at[at.z], {"tp": (at.z + k) % 4})

    def spread_out_proj():
        wait_dma(wo_mine, w_local.at[4])
        for k in range(1, 4):
            wait_dma(wo_mine, wz_r.at[(at.z + k) % 4])
            wait_dma(wo_mine, wz_s.at[k])
        spread(out_proj, 0, at.mate)

        @when(c == 0)
        def _():
            spread(out_proj, 1, at.across)
    for j in range(NJ):
        local(dy.at[y, at.rows_of(j)], gcur.at[chunk(j)], dy_sem.at[j])

    def weights_on(s, group):
        @when((y != s // 2) & (c == s % 2))
        def _():
            for k in group:
                wait_dma(w_vm[k].at[s], w_recv.at[s, k])
                send(w_vm[k].at[s], w_vm[k].at[s], w_fwd.at[k], w_recv.at[s, k], at.mate)

    def weights_ready(s, group):
        @when(p == s)
        def _():
            for k in group:
                if k < 4:
                    wait_dma(w_vm[k].at[p], w_local.at[k])

        @when((p != s) & ((y == s // 2) | (c != s % 2)))
        def _():
            for k in group:
                wait_dma(w_vm[k].at[s], w_recv.at[s, k])

    def send_home(l, src, dst, ssem, rsem):
        @when(p == l)
        def _():
            local(src, dst, ssem)

        @when(p != l)
        def _():
            send(src, dst, ssem, rsem.at[p], {"pp": l})

    weights_on(0, group_a)
    weights_ready(0, group_a)

    def finish_y(l, j):
        rows = chunk(j)
        total = line.get(NJ + j)
        out = (xm[l, rows, :].astype(F32) + total + row(wsv[l].astype(F32), BFC2)).astype(BF)

        @when(l > 0)
        def _():
            wait_dma(gcur.at[rows], ho_s.at[j])

        xs[l + 1, rows, :] = out
        send_home(l, xs.at[l + 1, rows], h_out.at[y, at.rows_of(j)], ho_s.at[j], ho_r)

    def query_places(shape, axis, odd):
        return lax.broadcasted_iota(jnp.int32, shape, axis) % CH + (KB * odd + CH * ((c + odd) % 2))

    def tail_keys(jj, odd):
        return pl.ds(pl.multiple_of(jj * WIDE, WIDE), KB * (1 + odd))

    def attn_pair(l, jj):
        rows = pair(jj)
        both = (2 * jj, 2 * jj + 1)

        @when(l == 0)
        def _():
            for j in both:
                wait_dma(xs.at[0, chunk(j)], x_sem.at[j])

        @when(l > 0)
        def _():
            for j in both:
                finish_y(l - 1, j)

        small = wsv[l].astype(F32)
        xhat, _ = ln_stats(xs[l, rows, :].astype(F32))
        h1 = (xhat * row(small, GAIN1) + row(small, SHIFT1)).astype(BF)
        qkv = (nt(h1, wqv[l]) + row(small, BQKV)[:, :QKV]).astype(BF)
        for k, j in enumerate(both):
            kv[l, at.rows_of(j), :] = qkv[k * CH:(k + 1) * CH, W:]
        for j in both:
            mine = kv.at[l, at.rows_of(j)]
            send(mine, mine, kv_s.at[j], kv_r.at[j], at.mate)
        qs[l, rows, :] = qkv[:, :W]
        for odd in range(2):
            attend(l, jj, odd)

    def attend(l, jj, odd):
        j = 2 * jj + odd
        rows = chunk(j)
        q2 = head_stack(qs[l, rows, :] * jnp.asarray(0.125, BF))
        lsum[...] = jnp.full_like(lsum, MASKED)

        def pass_one(kb):
            s = nt(q2, kv[l, blk(kb, WIDE), 0:W])
            scores[kb] = s
            lsum[...] = jnp.maximum(lsum[...], fold(s, jnp.maximum))

        loop(jj, pass_one)
        wait_dma(kv.at[l, at.rows_of(j)], kv_r.at[j])
        tail = tail_keys(jj, odd)
        s = nt(q2, kv[l, tail, 0:W])
        s = jnp.where(query_places(s.shape, 0, odd) >= lax.broadcasted_iota(jnp.int32, s.shape, 1), s, MASKED)
        top = jnp.max(jnp.maximum(lsum[...], fold(s, jnp.maximum)), axis=-1, keepdims=True)

        def weigh(s, keys):
            e = jnp.exp(s - top)
            return fold(e, jnp.add), nn(e.astype(BF), kv[l, keys, W:])

        lsum[...], acc[...] = weigh(s, tail)

        def pass_two(kb):
            more, part_o = weigh(scores[kb], blk(kb, WIDE))
            lsum[...] += more
            acc[...] += part_o

        loop(jj, pass_two)
        den = jnp.sum(lsum[...], axis=-1, keepdims=True)
        o = head_merge(acc[...] / den).astype(BF)
        os_[l, rows, :] = o
        lses[l, blk(j, 8), :] = as_row(top + jnp.log(den))
        gather.emit(j, o)
        line.serve(SLOTS * l + j)

    def mlp_op(l, j):
        rows = chunk(j)
        small = wsv[l].astype(F32)
        mid = (xs[l, rows, :].astype(F32) + nn(gather.get(j), wov[l]) + row(small, BOUT)).astype(BF)
        xm[l, rows, :] = mid

        @when((l == 0) & (y == 1))
        def _():
            send(xm.at[0, rows], xm_far.at[rows], xf_s.at[j], xf_r.at[j], at.across)

        xhat, _ = ln_stats(mid.astype(F32))
        h2 = (xhat * row(small, GAIN2) + row(small, SHIFT2)).astype(BF)
        u = nn(h2, w1v[l]) + row(small, BFC1)
        a = 0.5 * u * (1.0 + jnp.tanh(GELU_C * (u + GELU_A * u * u * u)))
        gather.sent(j)
        line.emit(SLOTS * l + NJ + j, nn(a.astype(BF), w2v[l]))

    def forward_layer(l):
        def attn_step(jj):
            with jax.named_scope("attn"):
                attn_pair(l, jj)

            @when((l == 0) & (jj == 1))
            def _():
                spread_out_proj()

            @when((l < 2) & (jj == 2))
            def _():
                weights_on(l, group_m)


        loop(PAIRS, attn_step)

        @when((l == 0) & (c == 1))
        def _():
            spread(every, 1, at.across)

        @when(l < 2)
        def _():
            weights_ready(l, group_m)

        def mlp_step(j):
            with jax.named_scope("mlp"):
                mlp_op(l, j)

            for when_j, step in ((3, weights_on), (NJ - 2, weights_ready)):
                @when((j == when_j) & (l < LAYERS - 1))
                def _():
                    step(l + 1, group_a)

                @when((j == when_j) & (l > 0) & (l < LAYERS - 1))
                def _():
                    step(l + 1, group_m)

        loop(NJ, mlp_step)
        loop(NJ, lambda j: wait_dma(kv.at[0, chunk(0)], kv_s.at[j]))

    for l in range(LAYERS):
        sm[l] = jnp.zeros((SMALL, D), F32)
    loop(LAYERS, forward_layer)

    groups = (((a_w1, d_w1, y_w1, o_w1), (a_w2, d_w2, y_w2, o_w2)), ((a_q, d_q, y_q, o_q), (a_o, d_o, y_o, o_o)))

    def add_into(dst, src):
        def body(i):
            rows = blk(i, 64)
            dst[rows, :] += src[rows, :]

        loop(dst.shape[0] // 64, body)

    def grad_to_mate(l, g):
        @when(c != l % 2)
        def _():
            for k, (own, mid, _, _) in enumerate(groups[g]):
                send(own, mid, d_s.at[g, k], d_r.at[g, k], at.mate)

    def grad_across(l, g, whole=True):
        @when(c != l % 2)
        def _():
            for k, (own, _, _, _) in enumerate(groups[g]):
                wait_dma(own, d_s.at[g, k])

        @when(c == l % 2)
        def _():
            for k, (own, mid, far, _) in enumerate(groups[g]):
                wait_dma(mid, d_r.at[g, k])
                add_into(mid, own)

                @when((y != l // 2) & whole)
                def _():
                    send(mid, far, y_s.at[g, k], y_r.at[g, k], at.across)

    def grad_home(l, g):
        @when((c == l % 2) & (y != l // 2))
        def _():
            for k, (_, mid, _, _) in enumerate(groups[g]):
                wait_dma(mid, y_s.at[g, k])

        @when(p == l)
        def _():
            for k, (_, mid, far, out) in enumerate(groups[g]):
                wait_dma(far, y_r.at[g, k])
                add_into(far, mid)
                local(far, out, o_sem.at[g, k])

    def add_small(l, r, value):
        sm[l, r:r + 1, :] += value

    def finish_layer(l, j):
        rows = chunk(j)
        dh1 = line.get(SLOTS - 1 - j)
        xhat, rstd = ln_stats(xs[l, rows, :].astype(F32))
        add_small(l, GAIN1, colsum(dh1 * xhat))
        add_small(l, SHIFT1, colsum(dh1))
        out = (gm[rows, :] + ln_back(dh1, xhat, rstd, row(wsv[l].astype(F32), GAIN1))).astype(BF)

        @when(l < LAYERS - 1)
        def _():
            wait_dma(gcur.at[rows], gi_s.at[j])

        gcur[rows, :] = out

        @when((l == 1) & (y == 1))
        def _():
            send(gcur.at[rows], g_far.at[rows], gi_s.at[j], gf_r.at[j], at.across)

        @when((l == 0) & (y == 1))
        def _():
            half = blk(2 * j + at.z % 2, CH // 2)
            send(gcur.at[half], g_half.at[c, j], gi_s.at[j], gh_r.at[c, j], {"pp": 0})

        @when((l > 1) | (y == 0))
        def _():
            send_home(l, gcur.at[rows], g_in.at[y, at.rows_of(j)], gi_s.at[j], gi_r)

    def mlp_back(l, i):
        j = NJ - 1 - i
        rows = chunk(j)

        @when(l == LAYERS - 1)
        def _():
            wait_dma(gcur.at[rows], dy_sem.at[j])
            finish_y(l, i)

        @when(l < LAYERS - 1)
        def _():
            finish_layer(l + 1, j)

        g = gcur[rows, :]
        dpre = mlp_grads(l, j, xm[l, rows, :], g)
        add_small(l, BFC2, colsum(g.astype(F32)))
        add_small(l, BFC1, colsum(dpre))
        line.emit(FWD + SLOTS * (LAYERS - 1 - l) + i, nt(dpre.astype(BF), w1v[l]))

        @when((l > 0) | (y == 0))
        def _():
            mlp_weight_grads(i, gcur)

    def mlp_grads(l, j, mid, g):
        small = wsv[l].astype(F32)
        xhat, _ = ln_stats(mid.astype(F32))
        h2 = (xhat * row(small, GAIN2) + row(small, SHIFT2)).astype(BF)
        u = nn(h2, w1v[l]) + row(small, BFC1)
        t = jnp.tanh(GELU_C * (u + GELU_A * u * u * u))
        half = 0.5 * (1.0 + t)
        slope = half + 0.5 * u * (1.0 - t * t) * (GELU_C * (1.0 + 3.0 * GELU_A * u * u))
        dpre = nt(g, w2v[l]) * slope
        spot = chunk(j % 2)
        h2p[spot, :] = h2
        dprep[spot, :] = dpre.astype(BF)
        ap[spot, :] = (u * half).astype(BF)
        return dpre

    def mlp_weight_grads(i, g_ref):
        grads = blk((NJ - 1 - i) // 2, KB)

        @when(i == 1)
        def _():
            a_w1[...] = tn(h2p[...], dprep[...])
            a_w2[...] = tn(ap[...], g_ref[grads, :])

        @when((i > 1) & (i % 2 == 1))
        def _():
            a_w1[...] += tn(h2p[...], dprep[...])
            a_w2[...] += tn(ap[...], g_ref[grads, :])

    def far_mlp_weight_grads():
        def body(i):
            j = NJ - 1 - i
            rows = chunk(j)
            wait_dma(xm_far.at[rows], xf_r.at[j])
            wait_dma(g_far.at[rows], gf_r.at[j])
            dst = g_in.at[1, at.rows_of(j)]

            @when(c == 1)
            def _():
                local(g_far.at[rows], dst, gi_r.at[3])

            @when(c == 0)
            def _():
                send(g_far.at[rows], dst, gf_s.at[j], gi_r.at[2], at.mate)

            @when(c == 0)
            def _():
                for core in range(2):
                    piece = g_half.at[core, j]
                    wait_dma(piece, gh_r.at[core, j])
                    out = g_in.at[1, blk(4 * j + 2 * ((core + j) % 2) + at.z % 2, CH // 2)]
                    local(piece, out, gx.at[0])
                    send(piece, out, gx.at[1], gx.at[2], {"tp": at.z + 1 - 2 * (at.z % 2)})

            mlp_grads(0, j, xm_far[rows, :], g_far[rows, :])

            @when(i % 2 == 1)
            def _():
                a_w1[...] += tn(h2p[...], dprep[...])
                a_w2[...] += tn(ap[...], g_far[blk(j // 2, KB), :])

        loop(NJ, body)

        @when(c == 1)
        def _():
            for k, (own, mid, _, _) in enumerate(groups[0]):
                send(own, mid, d_s.at[0, k], d_r.at[0, k], at.mate)
            for k, (own, _, _, _) in enumerate(groups[0]):
                wait_dma(own, d_s.at[0, k])

        @when(c == 0)
        def _():
            for k, (own, mid, _, out) in enumerate(groups[0]):
                wait_dma(mid, d_r.at[0, k])
                add_into(mid, own)
                local(mid, out, o_sem.at[0, k])
            loop(NJ, lambda j: wait_dma(g_far.at[chunk(j)], gf_s.at[j]))
            for k in range(3):
                wait_dma(g_half, gx.at[k])

    def attn_weight_grads(l):
        a_q[...] = tn(dqkvs[...], h1s[...])
        a_o[...] = tn(os_[l], gms[...])
        grad_to_mate(l, 1)

    def attn_back(l, jj, odd):
        j = 2 * jj + odd
        rows = chunk(j)
        small = wsv[l].astype(F32)
        dh2 = line.get(NJ - 1 - j)
        xhat, rstd = ln_stats(xm[l, rows, :].astype(F32))
        add_small(l, GAIN2, colsum(dh2 * xhat))
        add_small(l, SHIFT2, colsum(dh2))
        wide = gcur[rows, :].astype(F32) + ln_back(dh2, xhat, rstd, row(small, GAIN2))
        gm[rows, :] = wide
        add_small(l, BOUT, colsum(wide))
        gmid = wide.astype(BF)
        gms[rows, :] = gmid
        do = nt(gmid, wov[l, chunk(at.z), :]).astype(BF)
        delta = jnp.sum(head_stack(do.astype(F32) * os_[l, rows, :].astype(F32)), axis=-1, keepdims=True)
        delta = as_row(delta)[0:1]
        lse = lses[l, blk(j, 8), :][0:1]
        q2 = head_stack(qs[l, rows, :] * jnp.asarray(0.125, BF))
        do2 = head_stack(do)

        def block(keys, masked):
            k = kv[l, keys, 0:W]
            st = nt(k, q2)
            if masked:
                st = jnp.where(query_places(st.shape, 1, odd) >= lax.broadcasted_iota(jnp.int32, st.shape, 0), st, MASKED)
            pt = jnp.exp(st - lse)
            dst = (pt * (nt(kv[l, keys, W:], do2) - delta)).astype(BF)
            dk = nn(dst, q2)
            dv = nn(pt.astype(BF), do2)
            dq = tn(dst, k)
            dkv[keys, 0:W] += dk
            dkv[keys, W:] += dv
            return dq

        dq_acc[...] = block(tail_keys(jj, odd), True)
        send(dkv.at[at.mate_rows(j)], pk.at[j], dk_s.at[j], dk_r.at[j], at.mate)

        def full(kb):
            dq_acc[...] += block(blk(kb, WIDE), False)

        loop(jj, full)
        dqkvs[rows, 0:W] = (head_merge(dq_acc[...]) * 0.125).astype(BF)

    def qkv_back(l, j):
        rows = chunk(j)
        small = wsv[l].astype(F32)
        xhat, _ = ln_stats(xs[l, rows, :].astype(F32))
        h1s[rows, :] = (xhat * row(small, GAIN1) + row(small, SHIFT1)).astype(BF)
        wait_dma(pk.at[j], dk_r.at[j])
        dkv_own = (dkv[at.rows_of(j), :] + pk[j]).astype(BF)
        dqkvs[rows, W:] = dkv_own
        dqkv = jnp.concatenate([dqkvs[rows, 0:W], dkv_own], axis=1)
        sm[l, BQKV:BQKV + 1, 0:QKV] += colsum(dqkv.astype(F32))
        line.emit(FWD + SLOTS * (LAYERS - l) - 1 - j, nn(dqkv, wqv[l]))

    def backward_layer(n):
        l = LAYERS - 1 - n

        def first_half(i):
            @when((i == 0) & (l < LAYERS - 1))
            def _():
                attn_weight_grads(l + 1)

            @when(i == 2)
            def _():
                @when(l < LAYERS - 2)
                def _():
                    grad_home(l + 2, 1)

                @when(l < LAYERS - 1)
                def _():
                    grad_across(l + 1, 1)

            with jax.named_scope("B1"):
                mlp_back(l, i)

        loop(NJ, first_half)

        @when(l > 0)
        def _():
            grad_to_mate(l, 0)

        def clear(i):
            dkv[blk(i, 64), :] = jnp.zeros((64, KB), F32)

        loop(SEQ // 64, clear)

        def second_half(ii):
            jj = PAIRS - 1 - ii

            @when((ii == 1) & (l < LAYERS - 1))
            def _():
                grad_home(l + 1, 0)

            with jax.named_scope("B2"):
                attn_back(l, jj, 1)

            @when((ii == 0) & (l > 0))
            def _():
                grad_across(l, 0)

            with jax.named_scope("B3"):
                qkv_back(l, 2 * jj + 1)
            with jax.named_scope("B2"):
                attn_back(l, jj, 0)
            with jax.named_scope("B3"):
                qkv_back(l, 2 * jj)

        loop(PAIRS, second_half)
        loop(NJ, lambda j: wait_dma(pk.at[j], dk_s.at[j]))

    loop(LAYERS, backward_layer)
    attn_weight_grads(0)
    last = FWD + LAYERS * SLOTS - 1

    def finish_last(i):
        @when((i == 1) | (i == 2))
        def _():
            line.serve_first(last - 2 + i)

        @when(i > 3)
        def _():
            line.serve_second(last - NJ + 1 + i)

        finish_layer(0, NJ - 1 - i)

        @when(i == 2)
        def _():
            grad_across(0, 1, False)

        @when((i > 1) & (p == 2))
        def _():
            rows = blk(i - 2, 64)
            send(d_q.at[rows], y_q.at[rows], y_s.at[1, 0], y_r.at[1, 0], at.across)

    loop(NJ, finish_last)

    @when(p == 2)
    def _():
        send(d_o, y_o, y_s.at[1, 1], y_r.at[1, 1], at.across)

    for s in range(LAYERS):
        @when(p != s)
        def _():
            send(sm.at[s], rsm.at[p], sm_s.at[s], sm_r.at[p], {"pp": s})

    @when(y == 0)
    def _():
        far_mlp_weight_grads()

    @when(y == 1)
    def _():
        loop(NJ, lambda j: wait_dma(xm.at[0, chunk(j)], xf_s.at[j]))

    grad_home(1, 1)
    grad_home(0, 1)
    for s in range(LAYERS):
        @when(p != s)
        def _():
            wait_dma(sm.at[s], sm_s.at[s])
            wait_dma(rsm.at[s], sm_r.at[s])
    rsm[p] = sm[p]
    o_sm[...] = (rsm[0] + rsm[1]) + (rsm[2] + rsm[3])

    def sent(j):
        wait_dma(gcur.at[chunk(0)], ho_s.at[j])

        @when(y == 0)
        def _():
            wait_dma(gcur.at[chunk(0)], gi_s.at[j])

        @when(y == 1)
        def _():
            wait_dma(g_half.at[0, 0], gi_s.at[j])

    loop(NJ, sent)
    for s in range(LAYERS):
        @when(p != s)
        def _():
            wait_dma(h_out.at[0, pl.ds(0, ROWS)], ho_r.at[s])

        @when((p != s) & ((p > 0) | (s == 1)))
        def _():
            wait_dma(g_in.at[0, pl.ds(0, ROWS)], gi_r.at[s])

    for g, items in enumerate(groups):
        for k, (_, _, far, _) in enumerate(items):
            wait_dma(far, o_sem.at[g, k])
    for k in every:
        wait_dma(w_vm[k].at[0], w_send.at[0, k])
        wait_dma(w_vm[k].at[0], w_send.at[1, k])
        wait_dma(w_vm[k].at[0], w_fwd.at[k])
    line.close()


def run_layers(*args):
    hbm = pl.BlockSpec(memory_space=pl.ANY)
    dma = pltpu.SemaphoreType.DMA
    slots = pltpu.VMEM((SLOTS, CH, D), BF)
    slot_sem = dma((SLOTS,))
    chunk_sem = dma((NJ,))
    stage_sem = dma((LAYERS,))
    pair_sem = dma((2, 2))

    def bf(*shape):
        return pltpu.VMEM(shape, BF)

    def f32(*shape):
        return pltpu.VMEM(shape, F32)

    grad_shapes = ((D, D), (D, D), (QKV, D), (W, D))
    grads = [f32(*shape) for shape in grad_shapes]
    acts = jax.ShapeDtypeStruct((2, SEQ, D), BF)
    return pl.pallas_call(
        decoder_kernel,
        out_shape=[acts, acts, *(jax.ShapeDtypeStruct(shape, F32) for shape in (*grad_shapes, (SMALL, D)))],
        in_specs=[hbm] * len(args),
        out_specs=[hbm] * 6 + [pl.BlockSpec(memory_space=pltpu.VMEM)],
        scratch_shapes=[
            bf(LAYERS, SMALL, D), bf(LAYERS, QKV, D), *[bf(LAYERS, D, D)] * 3,
            bf(LAYERS, SEQ, KB), bf(LAYERS + 1, ROWS, D), bf(LAYERS, ROWS, D), bf(LAYERS, ROWS, W), bf(LAYERS, ROWS, W),
            f32(LAYERS, NJ * 8, KB), f32(PAIRS, KB, WIDE), f32(KB, W), f32(KB, W),
            bf(ROWS, D), f32(ROWS, D), f32(SEQ, KB), f32(NJ, CH, KB), bf(ROWS, D), bf(ROWS, QKV), bf(ROWS, D), *[bf(KB, D)] * 3, f32(KB, W), bf(ROWS, D), bf(ROWS, D), bf(2, NJ, CH // 2, D),
            *grads, *grads, *grads, f32(LAYERS, SMALL, D), f32(LAYERS, SMALL, D),
            *[slots] * 4, *[slot_sem] * 5, bf(NJ, 4, CH, W), *[chunk_sem] * 5,
            chunk_sem, stage_sem, stage_sem, dma((len(args) - 2,)), dma((2, len(args) - 2)), dma((LAYERS, len(args) - 2)), dma((len(args) - 2,)),
            chunk_sem, chunk_sem, chunk_sem, stage_sem,
            chunk_sem, chunk_sem, chunk_sem, chunk_sem, stage_sem, *[pair_sem] * 5, stage_sem, stage_sem, *[chunk_sem] * 4, dma((2, NJ)), dma((3,)),
        ],
        compiler_params=pltpu.CompilerParams(collective_id=0, has_side_effects=True, vmem_limit_bytes=67043328),
        name="decoder_layers",
    )(*args)


def collect_kernel(*refs):
    count = 6
    srcs, small, outs = refs[:count], refs[count], refs[count + 1:2 * count + 1]
    ln, bout, bfc1, bfc2, bqkv = refs[2 * count + 1:2 * count + 6]
    bufs, (sem_in, sem_out) = refs[2 * count + 6:3 * count + 6], refs[3 * count + 6:]
    parts = []
    for k, src in enumerate(srcs):
        n = src.shape[0] // 4 if k < 2 else src.shape[0]
        parts += [(k, pl.ds(i * n, n)) for i in range(src.shape[0] // n)]
    for i, (k, rows) in enumerate(parts):
        local(srcs[k].at[rows], bufs[k].at[rows], sem_in.at[i])
    ln[...] = small[0:BOUT, :]
    for r, out in ((BOUT, bout), (BFC1, bfc1), (BFC2, bfc2)):
        out[...] = small[r:r + 1, :]
    for i in range(6):
        bqkv[i // 2, i % 2:i % 2 + 1, :] = small[BQKV:BQKV + 1, i * 64:(i + 1) * 64]
    for i, (k, rows) in enumerate(parts):
        wait_dma(bufs[k].at[rows], sem_in.at[i])
        local(bufs[k].at[rows], outs[k].at[rows], sem_out.at[i])
    for i, (k, rows) in enumerate(parts):
        wait_dma(bufs[k].at[rows], sem_out.at[i])


def collect(*args):
    hbm, vmem = pl.BlockSpec(memory_space=pl.ANY), pl.BlockSpec(memory_space=pltpu.VMEM)
    big = args[:-1]
    shapes = [(GAIN1 + 4, D), (1, D), (1, D), (1, D), (3, 2, 64)]
    return pl.pallas_call(
        collect_kernel,
        out_shape=[*(jax.ShapeDtypeStruct(a.shape, a.dtype) for a in big), *(jax.ShapeDtypeStruct(shape, F32) for shape in shapes)],
        in_specs=[hbm] * len(big) + [vmem],
        out_specs=[hbm] * len(big) + [vmem] * len(shapes),
        scratch_shapes=[*(pltpu.VMEM(a.shape, a.dtype) for a in big), *[pltpu.SemaphoreType.DMA((2 * len(big),))] * 2],
        compiler_params=pltpu.CompilerParams(vmem_limit_bytes=67043328),
        name="collect",
    )(*args)


def solution(mesh):
    def program(x_in, dy_out, w_qkv, b_qkv, w_out, b_out, ln_par, w_fc1, b_fc1, w_fc2, b_fc2):
        layers, parts, _, heads, width = w_qkv.shape
        wq = w_qkv.transpose(0, 1, 3, 4, 2).reshape(QKV, D)
        bq = jnp.pad(b_qkv.reshape(1, QKV), ((0, 0), (0, D - QKV)))
        ws = jnp.concatenate([ln_par.reshape(4, D), b_out, b_fc2, b_fc1, bq, jnp.zeros((8, D), BF)], axis=0)
        h_out, g_in, *rest = run_layers(
            x_in.reshape(2, SEQ, D), dy_out.reshape(2, SEQ, D), wq, w_out.reshape(W, D), w_fc1.reshape(D, D), w_fc2.reshape(D, D), ws)
        h_out, g_in, d_w1, d_w2, d_q, d_o, ln, bout, bfc1, bfc2, bqkv = collect(h_out.reshape(-1, D), g_in.reshape(-1, D), *rest)
        acts = (layers, *x_in.shape)
        return (h_out.reshape(acts), g_in.reshape(acts),
                d_q.reshape(layers, parts, heads, width, D).transpose(0, 1, 4, 2, 3), bqkv.reshape(b_qkv.shape),
                d_o.reshape(w_out.shape), bout, ln.reshape(ln_par.shape),
                d_w1.reshape(w_fc1.shape), bfc1, d_w2.reshape(w_fc2.shape), bfc2)

    act_spec = P(NO, "dp", NO, NO)
    arg_specs = (act_spec, act_spec,
                 P("pp", NO, NO, "tp", NO), P("pp", NO, "tp", NO), P("pp", "tp", NO, NO),
                 P("pp", NO), P("pp", NO, NO), P("pp", NO, "tp"), P("pp", "tp"),
                 P("pp", "tp", NO), P("pp", NO))
    stage_spec = P("pp", NO, "dp", NO, NO)
    grad_axes = ("dp", "pp")
    result_specs = (stage_spec, stage_spec,
                    P(grad_axes, NO, NO, "tp", NO), P(grad_axes, NO, "tp", NO), P(grad_axes, "tp", NO, NO),
                    P(grad_axes, NO), P(grad_axes, NO, NO), P(grad_axes, NO, "tp"), P(grad_axes, "tp"),
                    P(grad_axes, "tp", NO), P(grad_axes, NO))
    return jax.shard_map(program, mesh=mesh, in_specs=arg_specs, out_specs=result_specs, check_vma=False)
```

```python
import jax
import jax.numpy as jnp
from jax import lax
from jax.experimental import pallas as pl
from jax.experimental.pallas import tpu as pltpu
from jax.sharding import PartitionSpec as P

LN_EPS = 1e-5
BF = jnp.bfloat16
F32 = jnp.float32
MESH = pl.DeviceIdType.MESH

LAYERS = 4
SEQ = 2048
D = 512
CH = 128
NJ = 8
PAIRS = NJ // 2
ROWS = CH * NJ
SLOTS = 2 * NJ
FWD = LAYERS * SLOTS
W = 128
QKV = 3 * W
KB = 256
WIDE = 2 * KB
SMALL = 16
GELU_C = 0.7978845608028654
GELU_A = 0.044715
MASKED = -1e30
NO = None
GAIN1, SHIFT1, GAIN2, SHIFT2, BOUT, BFC2, BFC1, BQKV = range(8)


def nn(a, b):
    return lax.dot_general(a, b, (((1,), (0,)), ((), ())), preferred_element_type=F32)


def nt(a, b):
    return lax.dot_general(a, b, (((1,), (1,)), ((), ())), preferred_element_type=F32)


def tn(a, b):
    return lax.dot_general(a, b, (((0,), (0,)), ((), ())), preferred_element_type=F32)


def ln_stats(x_wide):
    mean = jnp.mean(x_wide, axis=-1, keepdims=True)
    cent = x_wide - mean
    var = jnp.mean(cent * cent, axis=-1, keepdims=True)
    rstd = lax.rsqrt(var + LN_EPS)
    return cent * rstd, rstd


def ln_back(dy, xhat, rstd, gain):
    dxhat = dy * gain
    m1 = jnp.mean(dxhat, axis=-1, keepdims=True)
    m2 = jnp.mean(dxhat * xhat, axis=-1, keepdims=True)
    return rstd * (dxhat - m1 - xhat * m2)


def colsum(v):
    return jnp.sum(v, axis=0, keepdims=True)


def row(small, r):
    return small[r:r + 1]


def blk(i, n):
    return pl.ds(pl.multiple_of(i * n, n), n)


def chunk(j):
    return blk(j, CH)


def pair(jj):
    return blk(jj, KB)


def loop(n, body):
    def step(i, carry):
        body(i)
        return carry

    lax.fori_loop(0, n, step, 0)


when = pl.when


def wait_dma(ref, sem):
    pltpu.make_async_copy(ref, ref, sem).wait()


def local(src, dst, sem):
    pltpu.make_async_copy(src, dst, sem).start()


def send(src, dst, ssem, rsem, dev):
    pltpu.make_async_remote_copy(src, dst, ssem, rsem, device_id=dev, device_id_type=MESH).start()


class Place:
    def __init__(self):
        self.z = lax.axis_index("tp")
        self.p = lax.axis_index("pp")
        self.y = self.p // 2
        self.c = self.p % 2
        self.hub = (self.z == 1) | (self.z == 2)
        self.leaf = jnp.logical_not(self.hub)
        self.my_hub = {"tp": jnp.where(self.z == 0, 1, 2)}
        self.my_leaf = {"tp": jnp.where(self.z == 1, 0, 3)}
        self.other_hub = {"tp": 3 - self.z}
        self.mate = {"pp": self.p + 1 - 2 * self.c}
        self.across = {"pp": 2 * (1 - self.y) + self.c}

    def rows_of(self, j):
        return chunk(2 * j + (self.c + j) % 2)

    def mate_rows(self, j):
        return chunk(2 * j + (self.c + j + 1) % 2)

    def enter(self):
        bar = pltpu.get_barrier_semaphore()

        def greet(dev):
            pl.semaphore_signal(bar, inc=1, device_id=dev, device_id_type=MESH)

        for k in range(1, 4):
            greet({"pp": (self.p + k) % 4})
            greet({"tp": (self.z + k) % 4})

        pl.semaphore_wait(bar, 6)


def is_gather(e):
    return (e < FWD) & (e % SLOTS < NJ)


class LineSum:
    def __init__(self, at, gather, part, lbuf, hbuf, fin, s1, s2, r_l, r_h, r_f):
        self.gather = gather
        self.at, self.part, self.lbuf, self.hbuf, self.fin = at, part, lbuf, hbuf, fin
        self.s1, self.s2, self.r_l, self.r_h, self.r_f = s1, s2, r_l, r_h, r_f

    def emit(self, e, value):
        slot = e % SLOTS

        @when((e >= SLOTS) & jnp.logical_not(is_gather(e - SLOTS)))
        def _():
            wait_dma(self.part.at[slot], self.s1.at[slot])

        self.part[slot] = value.astype(BF)

        @when(self.at.leaf)
        def _():
            send(self.part.at[slot], self.lbuf.at[slot], self.s1.at[slot], self.r_l.at[slot], self.at.my_hub)

        self.serve(e)

    def serve(self, e):
        for back, mine, other in ((2, self.serve_first, self.gather.serve_first), (4, self.serve_second, self.gather.serve_second)):
            mine(e - back)

            @when(self.at.hub & (e >= back) & is_gather(e - back))
            def _():
                other((e - back + SLOTS) % SLOTS)

    def serve_first(self, e):
        slot = (e + SLOTS) % SLOTS

        @when(self.at.hub & (e >= 0) & jnp.logical_not(is_gather(e)))
        def _():
            wait_dma(self.lbuf.at[slot], self.r_l.at[slot])
            self.part[slot] = (self.part[slot].astype(F32) + self.lbuf[slot].astype(F32)).astype(BF)
            send(self.part.at[slot], self.hbuf.at[slot], self.s1.at[slot], self.r_h.at[slot], self.at.other_hub)

    def serve_second(self, e):
        slot = (e + SLOTS) % SLOTS

        @when(self.at.hub & (e >= 0) & jnp.logical_not(is_gather(e)))
        def _():
            wait_dma(self.hbuf.at[slot], self.r_h.at[slot])

            @when((e >= SLOTS) & jnp.logical_not(is_gather(e - SLOTS)))
            def _():
                wait_dma(self.fin.at[slot], self.s2.at[slot])

            self.fin[slot] = (self.part[slot].astype(F32) + self.hbuf[slot].astype(F32)).astype(BF)
            send(self.fin.at[slot], self.fin.at[slot], self.s2.at[slot], self.r_f.at[slot], self.at.my_leaf)

    def get(self, slot):
        @when(self.at.leaf)
        def _():
            wait_dma(self.fin.at[slot], self.r_f.at[slot])

        return self.fin[slot].astype(F32)

    def close(self):
        def body(slot):
            wait_dma(self.part.at[slot], self.s1.at[slot])

            @when(self.at.hub)
            def _():
                wait_dma(self.fin.at[slot], self.s2.at[slot])

        loop(SLOTS, body)


class LineGather:
    def __init__(self, at, buf, s_a, s_b, s_c, r_a, r_b):
        self.at, self.buf, self.s_a, self.s_b, self.s_c, self.r_a, self.r_b = at, buf, s_a, s_b, s_c, r_a, r_b
        side = at.z // 2
        self.mine, self.theirs = pl.ds(2 * side, 2), pl.ds(2 - 2 * side, 2)

    def sent(self, j):
        own, two = self.buf.at[j, 0], self.buf.at[j, pl.ds(0, 2)]
        wait_dma(own, self.s_a.at[j])

        @when(self.at.hub)
        def _():
            wait_dma(two, self.s_b.at[j])
            wait_dma(two, self.s_c.at[j])

    def emit(self, j, value):
        at = self.at
        self.buf[j, at.z] = value
        own = self.buf.at[j, at.z]

        @when(at.leaf)
        def _():
            send(own, own, self.s_a.at[j], self.r_a.at[j], at.my_hub)

        @when(at.hub)
        def _():
            send(own, own, self.s_a.at[j], self.r_a.at[j], at.my_leaf)

    def serve_first(self, j):
        wait_dma(self.buf.at[j, 0], self.r_a.at[j])
        two = self.buf.at[j, self.mine]
        send(two, two, self.s_b.at[j], self.r_b.at[j], self.at.other_hub)

    def serve_second(self, j):
        two = self.buf.at[j, self.theirs]
        wait_dma(two, self.r_b.at[j])
        send(two, two, self.s_c.at[j], self.r_b.at[j], self.at.my_leaf)

    def get(self, j):
        @when(self.at.leaf)
        def _():
            wait_dma(self.buf.at[j, 0], self.r_a.at[j])
            wait_dma(self.buf.at[j, self.theirs], self.r_b.at[j])

        return jnp.concatenate([self.buf[j, k] for k in range(4)], axis=1)


def head_stack(v):
    first = lax.broadcasted_iota(jnp.int32, v.shape, 1) < W // 2
    zero = jnp.zeros_like(v)
    return jnp.concatenate([jnp.where(first, v, zero), jnp.where(first, zero, v)], axis=0)


def head_merge(v):
    n = v.shape[0] // 2
    first = lax.broadcasted_iota(jnp.int32, (n, W), 1) < W // 2
    return jnp.where(first, v[:n], v[n:])


def as_row(v):
    return jnp.broadcast_to(v, (v.shape[0], W)).T[:8]


def fold(v, op):
    out = v[:, :W]
    for k in range(1, v.shape[1] // W):
        out = op(out, v[:, k * W:(k + 1) * W])
    return out


def decoder_kernel(x_in, dy, wq, wo, w1, w2, ws,
                   h_out, g_in, o_w1, o_w2, o_q, o_o, o_sm,
                   wsv, wqv, w1v, w2v, wov, kv, xs, xm, qs, os_, lses, scores, acc, lsum,
                   gcur, gm, dkv, pk, h1s, dqkvs, gms, h2p, dprep, ap, dq_acc, xm_far, g_far, g_half,
                   a_w1, a_w2, a_q, a_o, d_w1, d_w2, d_q, d_o, y_w1, y_w2, y_q, y_o, sm, rsm,
                   part, lbuf, hbuf, fin, s1, s2, r_l, r_h, r_f, og, gs_a, gs_b, gs_c, gr_a, gr_b,
                   x_sem, wz_s, wz_r, w_local, w_send, w_recv, w_fwd, kv_s, kv_r, ho_s, ho_r,
                   dy_sem, dk_s, dk_r, gi_s, gi_r, d_s, d_r, y_s, y_r, o_sem, sm_s, sm_r, xf_s, xf_r, gf_s, gf_r, gh_r, gx):
    at = Place()
    gather = LineGather(at, og, gs_a, gs_b, gs_c, gr_a, gr_b)
    line = LineSum(at, gather, part, lbuf, hbuf, fin, s1, s2, r_l, r_h, r_f)
    y, c, p = at.y, at.c, at.p
    w_hbm = (ws, wq, w1, w2)
    w_vm = (wsv, wqv, w1v, w2v, wov)
    every = range(len(w_vm))
    at_once, group_a, mlp_w, group_m, out_proj = every[:4], every[:2], every[2:4], every[2:], every[4:]
    wo_mine = wov.at[p, chunk(at.z)]

    for j in range(NJ):
        local(x_in.at[y, at.rows_of(j)], xs.at[0, chunk(j)], x_sem.at[j])
    for k in at_once:
        local(w_hbm[k], w_vm[k].at[p], w_local.at[k])
    local(wo, wo_mine, w_local.at[4])

    at.enter()

    for k in group_a:
        wait_dma(w_vm[k].at[p], w_local.at[k])

    def spread(group, way, dev):
        for k in group:
            src = w_hbm[k] if k in mlp_w else w_vm[k].at[p]
            send(src, w_vm[k].at[p], w_send.at[way, k], w_recv.at[p, k], dev)

    def gather_out_proj():
        for k in range(1, 4):
            send(wo, wo_mine, wz_s.at[k], wz_r.at[at.z], {"tp": (at.z + k) % 4})

    def spread_out_proj():
        wait_dma(wo_mine, w_local.at[4])
        for k in range(1, 4):
            wait_dma(wo_mine, wz_r.at[(at.z + k) % 4])
            wait_dma(wo_mine, wz_s.at[k])
        spread(out_proj, 0, at.mate)

    @when(c == 0)
    def _():
        spread(every[:3], 1, at.across)

    @when(p != 1)
    def _():
        gather_out_proj()

    spread(at_once, 0, at.mate)
    for j in range(NJ):
        local(dy.at[y, at.rows_of(j)], gcur.at[chunk(j)], dy_sem.at[j])

    def weights_on(s, group):
        @when((y != s // 2) & (c == s % 2))
        def _():
            for k in group:
                wait_dma(w_vm[k].at[s], w_recv.at[s, k])
                send(w_vm[k].at[s], w_vm[k].at[s], w_fwd.at[k], w_recv.at[s, k], at.mate)

    def weights_ready(s, group):
        @when(p == s)
        def _():
            for k in group:
                if k in mlp_w:
                    wait_dma(w_vm[k].at[p], w_local.at[k])

        @when((p != s) & ((y == s // 2) | (c != s % 2)))
        def _():
            for k in group:
                wait_dma(w_vm[k].at[s], w_recv.at[s, k])

    def send_home(l, src, dst, ssem, rsem):
        @when(p == l)
        def _():
            local(src, dst, ssem)

        @when(p != l)
        def _():
            send(src, dst, ssem, rsem.at[p], {"pp": l})

    weights_on(0, group_a)
    weights_ready(0, group_a)

    def finish_y(l, j):
        rows = chunk(j)
        total = line.get(NJ + j)
        out = (xm[l, rows, :].astype(F32) + total + row(wsv[l].astype(F32), BFC2)).astype(BF)

        @when(l > 0)
        def _():
            wait_dma(gcur.at[rows], ho_s.at[j])

        xs[l + 1, rows, :] = out
        send_home(l, xs.at[l + 1, rows], h_out.at[y, at.rows_of(j)], ho_s.at[j], ho_r)

    def query_places(shape, axis, odd):
        return lax.broadcasted_iota(jnp.int32, shape, axis) % CH + (KB * odd + CH * ((c + odd) % 2))

    def tail_keys(jj, odd):
        return pl.ds(pl.multiple_of(jj * WIDE, WIDE), KB * (1 + odd))

    def attn_pair(l, jj):
        rows = pair(jj)
        both = (2 * jj, 2 * jj + 1)

        @when(l == 0)
        def _():
            for j in both:
                wait_dma(xs.at[0, chunk(j)], x_sem.at[j])

        @when(l > 0)
        def _():
            for j in both:
                finish_y(l - 1, j)

        small = wsv[l].astype(F32)
        xhat, _ = ln_stats(xs[l, rows, :].astype(F32))
        h1 = (xhat * row(small, GAIN1) + row(small, SHIFT1)).astype(BF)
        qkv = (nt(h1, wqv[l]) + row(small, BQKV)[:, :QKV]).astype(BF)
        for k, j in enumerate(both):
            kv[l, at.rows_of(j), :] = qkv[k * CH:(k + 1) * CH, W:]
        for j in both:
            mine = kv.at[l, at.rows_of(j)]
            send(mine, mine, kv_s.at[j], kv_r.at[j], at.mate)
        q = qkv[:, :W]
        qs[l, rows, :] = q
        q4 = head_stack(q * jnp.asarray(0.125, BF))
        lsum[...] = jnp.full_like(lsum, MASKED)

        def pass_one(kb):
            s = nt(q4, kv[l, blk(kb, WIDE), 0:W])
            scores[kb] = s
            lsum[...] = jnp.maximum(lsum[...], fold(s, jnp.maximum))

        loop(jj, pass_one)
        for j in both:
            wait_dma(kv.at[l, at.rows_of(j)], kv_r.at[j])
        s = nt(q4, kv[l, blk(jj, WIDE), 0:W])
        r = lax.broadcasted_iota(jnp.int32, (WIDE, WIDE), 0) % KB
        seen = r % CH + jnp.where(r < CH, CH * c, KB + CH * (1 - c)) >= lax.broadcasted_iota(jnp.int32, (WIDE, WIDE), 1)
        s = jnp.where(seen, s, MASKED)
        top = jnp.max(jnp.maximum(lsum[...], fold(s, jnp.maximum)), axis=-1, keepdims=True)

        def weigh(s, keys):
            e = jnp.exp(s - top)
            return fold(e, jnp.add), nn(e.astype(BF), kv[l, keys, W:])

        lsum[...], acc[...] = weigh(s, blk(jj, WIDE))

        def pass_two(kb):
            more, part_o = weigh(scores[kb], blk(kb, WIDE))
            lsum[...] += more
            acc[...] += part_o

        loop(jj, pass_two)
        den = jnp.sum(lsum[...], axis=-1, keepdims=True)
        o = head_merge(acc[...] / den).astype(BF)
        os_[l, rows, :] = o
        stat = as_row(top + jnp.log(den))
        for k, j in enumerate(both):
            lses[l, blk(j, 8), :] = jnp.concatenate([stat[:, k * CH:(k + 1) * CH], stat[:, KB + k * CH:KB + (k + 1) * CH]], axis=1)
        for k, j in enumerate(both):
            gather.emit(j, o[k * CH:(k + 1) * CH])
            line.serve(SLOTS * l + j)

    def mlp_op(l, j):
        rows = chunk(j)
        small = wsv[l].astype(F32)
        mid = (xs[l, rows, :].astype(F32) + nn(gather.get(j), wov[l]) + row(small, BOUT)).astype(BF)
        xm[l, rows, :] = mid

        @when((l == 0) & (y == 1))
        def _():
            send(xm.at[0, rows], xm_far.at[rows], xf_s.at[j], xf_r.at[j], at.across)

        xhat, _ = ln_stats(mid.astype(F32))
        h2 = (xhat * row(small, GAIN2) + row(small, SHIFT2)).astype(BF)
        u = nn(h2, w1v[l]) + row(small, BFC1)
        a = 0.5 * u * (1.0 + jnp.tanh(GELU_C * (u + GELU_A * u * u * u)))
        gather.sent(j)
        line.emit(SLOTS * l + NJ + j, nn(a.astype(BF), w2v[l]))

    def forward_layer(l):
        def attn_step(jj):
            with jax.named_scope("attn"):
                attn_pair(l, jj)

            @when((l == 0) & (jj == 0) & (c == 0))
            def _():
                spread_out_proj()
                spread(out_proj, 1, at.across)
                spread(mlp_w[1:], 1, at.across)

            @when((l == 0) & (jj == 1))
            def _():
                weights_on(0, mlp_w[:1])

                @when(p == 1)
                def _():
                    gather_out_proj()

            @when((l == 0) & (jj == 2))
            def _():
                weights_on(0, out_proj)

            @when((l == 1) & (jj == 2))
            def _():
                weights_on(1, group_m)

        loop(PAIRS, attn_step)

        @when(l == 0)
        def _():
            weights_on(0, mlp_w[1:])

            @when(c == 1)
            def _():
                spread_out_proj()
                spread(every, 1, at.across)

        @when(l < 2)
        def _():
            weights_ready(l, group_m)

        def mlp_step(j):
            with jax.named_scope("mlp"):
                mlp_op(l, j)

            for when_j, step in ((3, weights_on), (NJ - 2, weights_ready)):
                @when((j == when_j) & (l < LAYERS - 1))
                def _():
                    step(l + 1, group_a)

                @when((j == when_j) & (l > 0) & (l < LAYERS - 1))
                def _():
                    step(l + 1, group_m)

        loop(NJ, mlp_step)
        loop(NJ, lambda j: wait_dma(kv.at[0, chunk(0)], kv_s.at[j]))

    for l in range(LAYERS):
        sm[l] = jnp.zeros((SMALL, D), F32)
    loop(LAYERS, forward_layer)

    groups = (((a_w1, d_w1, y_w1, o_w1), (a_w2, d_w2, y_w2, o_w2)), ((a_q, d_q, y_q, o_q), (a_o, d_o, y_o, o_o)))

    def add_into(dst, src):
        def body(i):
            rows = blk(i, 64)
            dst[rows, :] += src[rows, :]

        loop(dst.shape[0] // 64, body)

    def grad_to_mate(l, g):
        @when(c != l % 2)
        def _():
            for k, (own, mid, _, _) in enumerate(groups[g]):
                send(own, mid, d_s.at[g, k], d_r.at[g, k], at.mate)

    def grad_across(l, g, whole=True):
        @when(c != l % 2)
        def _():
            for k, (own, _, _, _) in enumerate(groups[g]):
                wait_dma(own, d_s.at[g, k])

        @when(c == l % 2)
        def _():
            for k, (own, mid, far, _) in enumerate(groups[g]):
                wait_dma(mid, d_r.at[g, k])
                add_into(mid, own)

                @when((y != l // 2) & whole)
                def _():
                    send(mid, far, y_s.at[g, k], y_r.at[g, k], at.across)

    def grad_home(l, g):
        @when((c == l % 2) & (y != l // 2))
        def _():
            for k, (_, mid, _, _) in enumerate(groups[g]):
                wait_dma(mid, y_s.at[g, k])

        @when(p == l)
        def _():
            for k, (_, mid, far, out) in enumerate(groups[g]):
                wait_dma(far, y_r.at[g, k])
                add_into(far, mid)
                local(far, out, o_sem.at[g, k])

    def add_small(l, r, value):
        sm[l, r:r + 1, :] += value

    def finish_layer(l, j):
        rows = chunk(j)
        dh1 = line.get(SLOTS - 1 - j)
        xhat, rstd = ln_stats(xs[l, rows, :].astype(F32))
        add_small(l, GAIN1, colsum(dh1 * xhat))
        add_small(l, SHIFT1, colsum(dh1))
        out = (gm[rows, :] + ln_back(dh1, xhat, rstd, row(wsv[l].astype(F32), GAIN1))).astype(BF)

        @when(l < LAYERS - 1)
        def _():
            wait_dma(gcur.at[rows], gi_s.at[j])

        gcur[rows, :] = out

        @when((l == 1) & (y == 1))
        def _():
            send(gcur.at[rows], g_far.at[rows], gi_s.at[j], gf_r.at[j], at.across)

        @when((l == 0) & (y == 1))
        def _():
            half = blk(2 * j + at.z % 2, CH // 2)
            send(gcur.at[half], g_half.at[c, j], gi_s.at[j], gh_r.at[c, j], {"pp": 0})

        @when((l > 1) | (y == 0))
        def _():
            send_home(l, gcur.at[rows], g_in.at[y, at.rows_of(j)], gi_s.at[j], gi_r)

    def mlp_back(l, i):
        j = NJ - 1 - i
        rows = chunk(j)

        @when(l == LAYERS - 1)
        def _():
            wait_dma(gcur.at[rows], dy_sem.at[j])
            finish_y(l, i)

        @when(l < LAYERS - 1)
        def _():
            finish_layer(l + 1, j)

        g = gcur[rows, :]
        dpre = mlp_grads(l, j, xm[l, rows, :], g)
        add_small(l, BFC2, colsum(g.astype(F32)))
        add_small(l, BFC1, colsum(dpre))
        line.emit(FWD + SLOTS * (LAYERS - 1 - l) + i, nt(dpre.astype(BF), w1v[l]))

        @when((l > 0) | (y == 0))
        def _():
            mlp_weight_grads(i, gcur)

    def mlp_grads(l, j, mid, g):
        small = wsv[l].astype(F32)
        xhat, _ = ln_stats(mid.astype(F32))
        h2 = (xhat * row(small, GAIN2) + row(small, SHIFT2)).astype(BF)
        u = nn(h2, w1v[l]) + row(small, BFC1)
        t = jnp.tanh(GELU_C * (u + GELU_A * u * u * u))
        half = 0.5 * (1.0 + t)
        slope = half + 0.5 * u * (1.0 - t * t) * (GELU_C * (1.0 + 3.0 * GELU_A * u * u))
        dpre = nt(g, w2v[l]) * slope
        spot = chunk(j % 2)
        h2p[spot, :] = h2
        dprep[spot, :] = dpre.astype(BF)
        ap[spot, :] = (u * half).astype(BF)
        return dpre

    def mlp_weight_grads(i, g_ref):
        grads = blk((NJ - 1 - i) // 2, KB)

        @when(i == 1)
        def _():
            a_w1[...] = tn(h2p[...], dprep[...])
            a_w2[...] = tn(ap[...], g_ref[grads, :])

        @when((i > 1) & (i % 2 == 1))
        def _():
            a_w1[...] += tn(h2p[...], dprep[...])
            a_w2[...] += tn(ap[...], g_ref[grads, :])

    def far_mlp_weight_grads(i):
        j = NJ - 1 - i
        rows = chunk(j)
        wait_dma(xm_far.at[rows], xf_r.at[j])
        wait_dma(g_far.at[rows], gf_r.at[j])
        dst = g_in.at[1, at.rows_of(j)]

        @when(c == 1)
        def _():
            local(g_far.at[rows], dst, gi_r.at[3])

        @when(c == 0)
        def _():
            send(g_far.at[rows], dst, gf_s.at[j], gi_r.at[2], at.mate)

        mlp_grads(0, j, xm_far[rows, :], g_far[rows, :])

        @when(i % 2 == 1)
        def _():
            a_w1[...] += tn(h2p[...], dprep[...])
            a_w2[...] += tn(ap[...], g_far[blk(j // 2, KB), :])

    def swap_halves(i):
        j = NJ - 1 - i
        for core in range(2):
            piece = g_half.at[core, j]
            wait_dma(piece, gh_r.at[core, j])
            out = g_in.at[1, blk(4 * j + 2 * ((core + j) % 2) + at.z % 2, CH // 2)]
            local(piece, out, gx.at[0])
            send(piece, out, gx.at[1], gx.at[2], {"tp": at.z + 1 - 2 * (at.z % 2)})

    def far_sums():
        for k, (own, mid, _, out) in enumerate(groups[0]):
            wait_dma(mid, d_r.at[0, k])
            add_into(mid, own)
            local(mid, out, o_sem.at[0, k])

    def attn_weight_grads(l):
        a_q[...] = tn(dqkvs[...], h1s[...])
        a_o[...] = tn(os_[l], gms[...])
        grad_to_mate(l, 1)

    def attn_back(l, jj, odd):
        j = 2 * jj + odd
        rows = chunk(j)
        small = wsv[l].astype(F32)
        dh2 = line.get(NJ - 1 - j)
        xhat, rstd = ln_stats(xm[l, rows, :].astype(F32))
        add_small(l, GAIN2, colsum(dh2 * xhat))
        add_small(l, SHIFT2, colsum(dh2))
        wide = gcur[rows, :].astype(F32) + ln_back(dh2, xhat, rstd, row(small, GAIN2))
        gm[rows, :] = wide
        add_small(l, BOUT, colsum(wide))
        gmid = wide.astype(BF)
        gms[rows, :] = gmid
        do = nt(gmid, wov[l, chunk(at.z), :]).astype(BF)
        delta = jnp.sum(head_stack(do.astype(F32) * os_[l, rows, :].astype(F32)), axis=-1, keepdims=True)
        delta = as_row(delta)[0:1]
        lse = lses[l, blk(j, 8), :][0:1]
        q2 = head_stack(qs[l, rows, :] * jnp.asarray(0.125, BF))
        do2 = head_stack(do)

        def block(keys, masked):
            k = kv[l, keys, 0:W]
            st = nt(k, q2)
            if masked:
                st = jnp.where(query_places(st.shape, 1, odd) >= lax.broadcasted_iota(jnp.int32, st.shape, 0), st, MASKED)
            pt = jnp.exp(st - lse)
            dst = (pt * (nt(kv[l, keys, W:], do2) - delta)).astype(BF)
            dk = nn(dst, q2)
            dv = nn(pt.astype(BF), do2)
            dq = tn(dst, k)
            dkv[keys, 0:W] += dk
            dkv[keys, W:] += dv
            return dq

        dq_acc[...] = block(tail_keys(jj, odd), True)
        send(dkv.at[at.mate_rows(j)], pk.at[j], dk_s.at[j], dk_r.at[j], at.mate)

        def full(kb):
            dq_acc[...] += block(blk(kb, WIDE), False)

        loop(jj, full)
        dqkvs[rows, 0:W] = (head_merge(dq_acc[...]) * 0.125).astype(BF)

    def qkv_back(l, j):
        rows = chunk(j)
        small = wsv[l].astype(F32)
        xhat, _ = ln_stats(xs[l, rows, :].astype(F32))
        h1s[rows, :] = (xhat * row(small, GAIN1) + row(small, SHIFT1)).astype(BF)
        wait_dma(pk.at[j], dk_r.at[j])
        dkv_own = (dkv[at.rows_of(j), :] + pk[j]).astype(BF)
        dqkvs[rows, W:] = dkv_own
        dqkv = jnp.concatenate([dqkvs[rows, 0:W], dkv_own], axis=1)
        sm[l, BQKV:BQKV + 1, 0:QKV] += colsum(dqkv.astype(F32))
        line.emit(FWD + SLOTS * (LAYERS - l) - 1 - j, nn(dqkv, wqv[l]))

    def backward_layer(n):
        l = LAYERS - 1 - n

        def first_half(i):
            @when((i == 0) & (l < LAYERS - 1))
            def _():
                attn_weight_grads(l + 1)

            @when(i == 2)
            def _():
                @when(l < LAYERS - 2)
                def _():
                    grad_home(l + 2, 1)

                @when(l < LAYERS - 1)
                def _():
                    grad_across(l + 1, 1)

            with jax.named_scope("B1"):
                mlp_back(l, i)

        loop(NJ, first_half)

        @when(l > 0)
        def _():
            grad_to_mate(l, 0)

        def clear(i):
            dkv[blk(i, 64), :] = jnp.zeros((64, KB), F32)

        loop(SEQ // 64, clear)

        def second_half(ii):
            jj = PAIRS - 1 - ii

            @when((ii == 1) & (l < LAYERS - 1))
            def _():
                grad_home(l + 1, 0)

            with jax.named_scope("B2"):
                attn_back(l, jj, 1)

            @when((ii == 0) & (l > 0))
            def _():
                grad_across(l, 0)

            with jax.named_scope("B3"):
                qkv_back(l, 2 * jj + 1)
            with jax.named_scope("B2"):
                attn_back(l, jj, 0)
            with jax.named_scope("B3"):
                qkv_back(l, 2 * jj)

        loop(PAIRS, second_half)
        loop(NJ, lambda j: wait_dma(pk.at[j], dk_s.at[j]))

    loop(LAYERS, backward_layer)
    attn_weight_grads(0)
    last = FWD + LAYERS * SLOTS - 1

    def finish_last(i):
        @when((i == 1) | (i == 2))
        def _():
            line.serve_first(last - 2 + i)

        @when(i > 3)
        def _():
            line.serve_second(last - NJ + 1 + i)

        finish_layer(0, NJ - 1 - i)

        @when(y == 0)
        def _():
            far_mlp_weight_grads(i)

        @when((p == 0) & at.leaf & (i > 2))
        def _():
            swap_halves(i - 3)

        first = jnp.where(at.hub, 2, 0)

        @when(i == first)
        def _():
            grad_across(0, 1, False)

        @when((i >= first) & (i < first + 6) & (p == 2))
        def _():
            rows = blk(i - first, 64)
            send(d_q.at[rows], y_q.at[rows], y_s.at[1, 0], y_r.at[1, 0], at.across)

    loop(NJ, finish_last)

    @when(p == 1)
    def _():
        for k, (own, mid, _, _) in enumerate(groups[0]):
            send(own, mid, d_s.at[0, k], d_r.at[0, k], at.mate)

    @when(p == 2)
    def _():
        send(d_o, y_o, y_s.at[1, 1], y_r.at[1, 1], at.across)

    for s in range(LAYERS):
        @when(p != s)
        def _():
            send(sm.at[s], rsm.at[p], sm_s.at[s], sm_r.at[p], {"pp": s})

    @when((p == 0) & at.hub)
    def _():
        loop(NJ - 3, swap_halves)

    for k in every:
        wait_dma(w_vm[k].at[0], w_send.at[0, k])
        wait_dma(w_vm[k].at[0], w_send.at[1, k])
        wait_dma(w_vm[k].at[0], w_fwd.at[k])
    line.close()
    loop(NJ, lambda j: wait_dma(gcur.at[chunk(0)], ho_s.at[j]))

    @when(p == 1)
    def _():
        for k, (own, mid, _, _) in enumerate(groups[0]):
            wait_dma(own, d_s.at[0, k])

    @when(p == 0)
    def _():
        swap_halves(NJ - 3)
        swap_halves(NJ - 2)
        far_sums()
        swap_halves(NJ - 1)
        loop(NJ, lambda j: wait_dma(g_far.at[chunk(j)], gf_s.at[j]))
        for k in range(3):
            wait_dma(g_half, gx.at[k])

    @when(y == 1)
    def _():
        loop(NJ, lambda j: wait_dma(xm.at[0, chunk(j)], xf_s.at[j]))

    grad_home(1, 1)
    grad_home(0, 1)
    for s in range(LAYERS):
        @when(p != s)
        def _():
            wait_dma(sm.at[s], sm_s.at[s])
            wait_dma(rsm.at[s], sm_r.at[s])
    rsm[p] = sm[p]
    sm[0] = (rsm[0] + rsm[1]) + (rsm[2] + rsm[3])
    local(sm.at[0], o_sm, x_sem.at[0])

    def sent(j):
        @when(y == 0)
        def _():
            wait_dma(gcur.at[chunk(0)], gi_s.at[j])

        @when(y == 1)
        def _():
            wait_dma(g_half.at[0, 0], gi_s.at[j])

    loop(NJ, sent)
    for s in range(LAYERS):
        @when(p != s)
        def _():
            wait_dma(h_out.at[0, pl.ds(0, ROWS)], ho_r.at[s])

        @when((p != s) & ((p > 0) | (s == 1)))
        def _():
            wait_dma(g_in.at[0, pl.ds(0, ROWS)], gi_r.at[s])

    for g, items in enumerate(groups):
        for k, (_, _, far, _) in enumerate(items):
            wait_dma(far, o_sem.at[g, k])
    wait_dma(sm.at[0], x_sem.at[0])


def run_layers(*args):
    hbm = pl.BlockSpec(memory_space=pl.ANY)
    dma = pltpu.SemaphoreType.DMA
    slots = pltpu.VMEM((SLOTS, CH, D), BF)
    slot_sem = dma((SLOTS,))
    chunk_sem = dma((NJ,))
    stage_sem = dma((LAYERS,))
    pair_sem = dma((2, 2))

    def bf(*shape):
        return pltpu.VMEM(shape, BF)

    def f32(*shape):
        return pltpu.VMEM(shape, F32)

    grad_shapes = ((D, D), (D, D), (QKV, D), (W, D))
    grads = [f32(*shape) for shape in grad_shapes]
    acts = jax.ShapeDtypeStruct((2, SEQ, D), BF)
    return pl.pallas_call(
        decoder_kernel,
        out_shape=[acts, acts, *(jax.ShapeDtypeStruct(shape, F32) for shape in (*grad_shapes, (SMALL, D)))],
        in_specs=[hbm] * len(args),
        out_specs=[hbm] * 7,
        scratch_shapes=[
            bf(LAYERS, SMALL, D), bf(LAYERS, QKV, D), *[bf(LAYERS, D, D)] * 3,
            bf(LAYERS, SEQ, KB), bf(LAYERS + 1, ROWS, D), bf(LAYERS, ROWS, D), bf(LAYERS, ROWS, W), bf(LAYERS, ROWS, W),
            f32(LAYERS, NJ * 8, KB), f32(PAIRS, WIDE, WIDE), f32(WIDE, W), f32(WIDE, W),
            bf(ROWS, D), f32(ROWS, D), f32(SEQ, KB), f32(NJ, CH, KB), bf(ROWS, D), bf(ROWS, QKV), bf(ROWS, D), *[bf(KB, D)] * 3, f32(KB, W), bf(ROWS, D), bf(ROWS, D), bf(2, NJ, CH // 2, D),
            *grads, *grads, *grads, f32(LAYERS, SMALL, D), f32(LAYERS, SMALL, D),
            *[slots] * 4, *[slot_sem] * 5, bf(NJ, 4, CH, W), *[chunk_sem] * 5,
            chunk_sem, stage_sem, stage_sem, dma((len(args) - 2,)), dma((2, len(args) - 2)), dma((LAYERS, len(args) - 2)), dma((len(args) - 2,)),
            chunk_sem, chunk_sem, chunk_sem, stage_sem,
            chunk_sem, chunk_sem, chunk_sem, chunk_sem, stage_sem, *[pair_sem] * 5, stage_sem, stage_sem, *[chunk_sem] * 4, dma((2, NJ)), dma((3,)),
        ],
        compiler_params=pltpu.CompilerParams(collective_id=0, has_side_effects=True, vmem_limit_bytes=67043328),
        name="decoder_layers",
    )(*args)


def collect_kernel(*refs):
    count = 6
    srcs, small, outs = refs[:count], refs[count], refs[count + 1:2 * count + 1]
    ln, bout, bfc1, bfc2, bqkv = refs[2 * count + 1:2 * count + 6]
    bufs, (sem_in, sem_out) = refs[2 * count + 6:3 * count + 6], refs[3 * count + 6:]
    for k in range(count):
        local(srcs[k], bufs[k], sem_in.at[k])
    ln[...] = small[0:BOUT, :]
    for r, out in ((BOUT, bout), (BFC1, bfc1), (BFC2, bfc2)):
        out[...] = small[r:r + 1, :]
    for i in range(6):
        bqkv[i // 2, i % 2:i % 2 + 1, :] = small[BQKV:BQKV + 1, i * 64:(i + 1) * 64]
    for k in range(count):
        wait_dma(bufs[k], sem_in.at[k])
        local(bufs[k], outs[k], sem_out.at[k])
    for k in range(count):
        wait_dma(bufs[k], sem_out.at[k])


def collect(*args):
    hbm, vmem = pl.BlockSpec(memory_space=pl.ANY), pl.BlockSpec(memory_space=pltpu.VMEM)
    big = args[:-1]
    shapes = [(GAIN1 + 4, D), (1, D), (1, D), (1, D), (3, 2, 64)]
    return pl.pallas_call(
        collect_kernel,
        out_shape=[*(jax.ShapeDtypeStruct(a.shape, a.dtype) for a in big), *(jax.ShapeDtypeStruct(shape, F32) for shape in shapes)],
        in_specs=[hbm] * len(big) + [vmem],
        out_specs=[hbm] * len(big) + [vmem] * len(shapes),
        scratch_shapes=[*(pltpu.VMEM(a.shape, a.dtype) for a in big), *[pltpu.SemaphoreType.DMA((len(big),))] * 2],
        compiler_params=pltpu.CompilerParams(vmem_limit_bytes=67043328),
        name="collect",
    )(*args)


def solution(mesh):
    def program(x_in, dy_out, w_qkv, b_qkv, w_out, b_out, ln_par, w_fc1, b_fc1, w_fc2, b_fc2):
        layers, parts, _, heads, width = w_qkv.shape
        wq = w_qkv.transpose(0, 1, 3, 4, 2).reshape(QKV, D)
        bq = jnp.pad(b_qkv.reshape(1, QKV), ((0, 0), (0, D - QKV)))
        ws = jnp.concatenate([ln_par.reshape(4, D), b_out, b_fc2, b_fc1, bq, jnp.zeros((8, D), BF)], axis=0)
        h_out, g_in, *rest = run_layers(
            x_in.reshape(2, SEQ, D), dy_out.reshape(2, SEQ, D), wq, w_out.reshape(W, D), w_fc1.reshape(D, D), w_fc2.reshape(D, D), ws)
        h_out, g_in, d_w1, d_w2, d_q, d_o, ln, bout, bfc1, bfc2, bqkv = collect(h_out.reshape(-1, D), g_in.reshape(-1, D), *rest)
        acts = (layers, *x_in.shape)
        return (h_out.reshape(acts), g_in.reshape(acts),
                d_q.reshape(layers, parts, heads, width, D).transpose(0, 1, 4, 2, 3), bqkv.reshape(b_qkv.shape),
                d_o.reshape(w_out.shape), bout, ln.reshape(ln_par.shape),
                d_w1.reshape(w_fc1.shape), bfc1, d_w2.reshape(w_fc2.shape), bfc2)

    act_spec = P(NO, "dp", NO, NO)
    arg_specs = (act_spec, act_spec,
                 P("pp", NO, NO, "tp", NO), P("pp", NO, "tp", NO), P("pp", "tp", NO, NO),
                 P("pp", NO), P("pp", NO, NO), P("pp", NO, "tp"), P("pp", "tp"),
                 P("pp", "tp", NO), P("pp", NO))
    stage_spec = P("pp", NO, "dp", NO, NO)
    grad_axes = ("dp", "pp")
    result_specs = (stage_spec, stage_spec,
                    P(grad_axes, NO, NO, "tp", NO), P(grad_axes, NO, "tp", NO), P(grad_axes, "tp", NO, NO),
                    P(grad_axes, NO), P(grad_axes, NO, NO), P(grad_axes, NO, "tp"), P(grad_axes, "tp"),
                    P(grad_axes, "tp", NO), P(grad_axes, NO))
    return jax.shard_map(program, mesh=mesh, in_specs=arg_specs, out_specs=result_specs, check_vma=False)
```

```python
import jax
import jax.numpy as jnp
from jax import lax
from jax.experimental import pallas as pl
from jax.experimental.pallas import tpu as pltpu
from jax.sharding import PartitionSpec as P

LN_EPS = 1e-5
BF = jnp.bfloat16
F32 = jnp.float32
MESH = pl.DeviceIdType.MESH

LAYERS = 4
SEQ = 2048
D = 512
CH = 128
NJ = 8
PAIRS = NJ // 2
ROWS = CH * NJ
SLOTS = 2 * NJ
FWD = LAYERS * SLOTS
W = 128
QKV = 3 * W
KB = 256
WIDE = 2 * KB
SMALL = 16
GELU_C = 0.7978845608028654
GELU_A = 0.044715
MASKED = -1e30
NO = None
TP = 4
HALF = CH // 2
VMEM_LIMIT = 67043328
GAIN1, SHIFT1, GAIN2, SHIFT2, BOUT, BFC2, BFC1, BQKV = range(8)


def nn(a, b):
    return lax.dot_general(a, b, (((1,), (0,)), ((), ())), preferred_element_type=F32)


def nt(a, b):
    return lax.dot_general(a, b, (((1,), (1,)), ((), ())), preferred_element_type=F32)


def tn(a, b):
    return lax.dot_general(a, b, (((0,), (0,)), ((), ())), preferred_element_type=F32)


def ln_stats(x_wide):
    mean = jnp.mean(x_wide, axis=-1, keepdims=True)
    cent = x_wide - mean
    var = jnp.mean(cent * cent, axis=-1, keepdims=True)
    rstd = lax.rsqrt(var + LN_EPS)
    return cent * rstd, rstd


def ln_back(dy, xhat, rstd, gain):
    dxhat = dy * gain
    m1 = jnp.mean(dxhat, axis=-1, keepdims=True)
    m2 = jnp.mean(dxhat * xhat, axis=-1, keepdims=True)
    return rstd * (dxhat - m1 - xhat * m2)


def colsum(v):
    return jnp.sum(v, axis=0, keepdims=True)


def row(small, r):
    return small[r:r + 1]


def blk(i, n):
    return pl.ds(pl.multiple_of(i * n, n), n)


def chunk(j):
    return blk(j, CH)


def pair(jj):
    return blk(jj, KB)


def loop(n, body):
    def step(i, carry):
        body(i)
        return carry

    lax.fori_loop(0, n, step, 0)


when = pl.when


def wait_dma(ref, sem):
    pltpu.make_async_copy(ref, ref, sem).wait()


def local(src, dst, sem):
    pltpu.make_async_copy(src, dst, sem).start()


def send(src, dst, ssem, rsem, dev):
    pltpu.make_async_remote_copy(src, dst, ssem, rsem, device_id=dev, device_id_type=MESH).start()


class Place:
    def __init__(self):
        self.z = lax.axis_index("tp")
        self.p = lax.axis_index("pp")
        self.y = self.p // 2
        self.c = self.p % 2
        self.hub = (self.z == 1) | (self.z == 2)
        self.leaf = jnp.logical_not(self.hub)
        self.my_hub = {"tp": jnp.where(self.z == 0, 1, 2)}
        self.my_leaf = {"tp": jnp.where(self.z == 1, 0, 3)}
        self.other_hub = {"tp": 3 - self.z}
        self.mate = {"pp": self.p + 1 - 2 * self.c}
        self.across = {"pp": 2 * (1 - self.y) + self.c}

    def rows_of(self, j):
        return chunk(2 * j + (self.c + j) % 2)

    def mate_rows(self, j):
        return chunk(2 * j + (self.c + j + 1) % 2)

    def enter(self):
        bar = pltpu.get_barrier_semaphore()

        def greet(dev):
            pl.semaphore_signal(bar, inc=1, device_id=dev, device_id_type=MESH)

        for k in range(1, TP):
            greet({"pp": (self.p + k) % TP})
            greet({"tp": (self.z + k) % TP})

        pl.semaphore_wait(bar, 6)


def is_gather(e):
    return (e < FWD) & (e % SLOTS < NJ)


class LineSum:
    def __init__(self, at, gather, part, lbuf, hbuf, fin, s1, s2, r_l, r_h, r_f):
        self.gather = gather
        self.at, self.part, self.lbuf, self.hbuf, self.fin = at, part, lbuf, hbuf, fin
        self.s1, self.s2, self.r_l, self.r_h, self.r_f = s1, s2, r_l, r_h, r_f

    def emit(self, e, value):
        slot = e % SLOTS

        @when((e >= SLOTS) & jnp.logical_not(is_gather(e - SLOTS)))
        def _():
            wait_dma(self.part.at[slot], self.s1.at[slot])

        self.part[slot] = value.astype(BF)

        @when(self.at.leaf)
        def _():
            send(self.part.at[slot], self.lbuf.at[slot], self.s1.at[slot], self.r_l.at[slot], self.at.my_hub)

        self.serve(e)

    def serve(self, e):
        for back, mine, other in ((2, self.serve_first, self.gather.serve_first), (4, self.serve_second, self.gather.serve_second)):
            mine(e - back)

            @when(self.at.hub & (e >= back) & is_gather(e - back))
            def _():
                other((e - back + SLOTS) % SLOTS)

    def serve_first(self, e):
        slot = (e + SLOTS) % SLOTS

        @when(self.at.hub & (e >= 0) & jnp.logical_not(is_gather(e)))
        def _():
            wait_dma(self.lbuf.at[slot], self.r_l.at[slot])
            self.part[slot] = (self.part[slot].astype(F32) + self.lbuf[slot].astype(F32)).astype(BF)
            send(self.part.at[slot], self.hbuf.at[slot], self.s1.at[slot], self.r_h.at[slot], self.at.other_hub)

    def serve_second(self, e):
        slot = (e + SLOTS) % SLOTS

        @when(self.at.hub & (e >= 0) & jnp.logical_not(is_gather(e)))
        def _():
            wait_dma(self.hbuf.at[slot], self.r_h.at[slot])

            @when((e >= SLOTS) & jnp.logical_not(is_gather(e - SLOTS)))
            def _():
                wait_dma(self.fin.at[slot], self.s2.at[slot])

            self.fin[slot] = (self.part[slot].astype(F32) + self.hbuf[slot].astype(F32)).astype(BF)
            send(self.fin.at[slot], self.fin.at[slot], self.s2.at[slot], self.r_f.at[slot], self.at.my_leaf)

    def get(self, slot):
        @when(self.at.leaf)
        def _():
            wait_dma(self.fin.at[slot], self.r_f.at[slot])

        return self.fin[slot].astype(F32)

    def close(self):
        def body(slot):
            wait_dma(self.part.at[slot], self.s1.at[slot])

            @when(self.at.hub)
            def _():
                wait_dma(self.fin.at[slot], self.s2.at[slot])

        loop(SLOTS, body)


class LineGather:
    def __init__(self, at, buf, s_a, s_b, s_c, r_a, r_b):
        self.at, self.buf, self.s_a, self.s_b, self.s_c, self.r_a, self.r_b = at, buf, s_a, s_b, s_c, r_a, r_b
        side = at.z // 2
        self.mine, self.theirs = pl.ds(2 * side, 2), pl.ds(2 - 2 * side, 2)

    def sent(self, j):
        own, two = self.buf.at[j, 0], self.buf.at[j, pl.ds(0, 2)]
        wait_dma(own, self.s_a.at[j])

        @when(self.at.hub)
        def _():
            wait_dma(two, self.s_b.at[j])
            wait_dma(two, self.s_c.at[j])

    def emit(self, j, value):
        at = self.at
        self.buf[j, at.z] = value
        own = self.buf.at[j, at.z]

        @when(at.leaf)
        def _():
            send(own, own, self.s_a.at[j], self.r_a.at[j], at.my_hub)

        @when(at.hub)
        def _():
            send(own, own, self.s_a.at[j], self.r_a.at[j], at.my_leaf)

    def serve_first(self, j):
        wait_dma(self.buf.at[j, 0], self.r_a.at[j])
        two = self.buf.at[j, self.mine]
        send(two, two, self.s_b.at[j], self.r_b.at[j], self.at.other_hub)

    def serve_second(self, j):
        two = self.buf.at[j, self.theirs]
        wait_dma(two, self.r_b.at[j])
        send(two, two, self.s_c.at[j], self.r_b.at[j], self.at.my_leaf)

    def get(self, j):
        @when(self.at.leaf)
        def _():
            wait_dma(self.buf.at[j, 0], self.r_a.at[j])
            wait_dma(self.buf.at[j, self.theirs], self.r_b.at[j])

        return jnp.concatenate([self.buf[j, k] for k in range(TP)], axis=1)


def head_stack(v):
    first = lax.broadcasted_iota(jnp.int32, v.shape, 1) < W // 2
    zero = jnp.zeros_like(v)
    return jnp.concatenate([jnp.where(first, v, zero), jnp.where(first, zero, v)], axis=0)


def head_merge(v):
    n = v.shape[0] // 2
    first = lax.broadcasted_iota(jnp.int32, (n, W), 1) < W // 2
    return jnp.where(first, v[:n], v[n:])


def as_row(v):
    return jnp.broadcast_to(v, (v.shape[0], W)).T[:8]


def fold(v, op):
    out = v[:, :W]
    for k in range(1, v.shape[1] // W):
        out = op(out, v[:, k * W:(k + 1) * W])
    return out


def decoder_kernel(x_in, dy, wq, wo, w1, w2, ln_par, b_out, b_fc2, b_fc1, b_qkv,
                   h_out, g_in, o_w1, o_w2, o_q, o_o, o_sm,
                   wsv, wqv, w1v, w2v, wov, kv, xs, xm, qs, os_, lses, scores, acc, lsum,
                   gcur, gm, dkv, pk, h1s, dqkvs, gms, h2p, dprep, ap, dq_acc, xm_far, g_far, g_half,
                   a_w1, a_w2, a_q, a_o, d_w1, d_w2, d_q, d_o, y_w1, y_w2, y_q, y_o, sm, rsm,
                   part, lbuf, hbuf, fin, s1, s2, r_l, r_h, r_f, og, gs_a, gs_b, gs_c, gr_a, gr_b,
                   v_ln, v_bout, v_bfc2, v_bfc1, v_bqkv, v_sem,
                   x_sem, wz_s, wz_r, w_local, w_send, w_recv, w_fwd, kv_s, kv_r, ho_s, ho_r,
                   dy_sem, dk_s, dk_r, gi_s, gi_r, d_s, d_r, y_s, y_r, o_sem, sm_s, sm_r, xf_s, xf_r, gf_s, gf_r, gh_r, gx):
    at = Place()
    gather = LineGather(at, og, gs_a, gs_b, gs_c, gr_a, gr_b)
    line = LineSum(at, gather, part, lbuf, hbuf, fin, s1, s2, r_l, r_h, r_f)
    y, c, p = at.y, at.c, at.p
    w_hbm = (NO, wq, w1, w2)
    small_in = ((ln_par, v_ln), (b_out, v_bout), (b_fc2, v_bfc2), (b_fc1, v_bfc1), (b_qkv, v_bqkv))
    w_vm = (wsv, wqv, w1v, w2v, wov)
    every = range(len(w_vm))
    at_once, group_a, mlp_w, group_m, out_proj = every[:4], every[:2], every[2:4], every[2:], every[4:]
    wo_mine = wov.at[p, chunk(at.z)]

    for j in range(NJ):
        local(x_in.at[y, at.rows_of(j)], xs.at[0, chunk(j)], x_sem.at[j])
    for k in at_once[1:]:
        local(w_hbm[k], w_vm[k].at[p], w_local.at[k])
    for k, (src, dst) in enumerate(small_in):
        local(src, dst, v_sem.at[k])
    local(wo, wo_mine, w_local.at[4])

    at.enter()

    for k, (_, dst) in enumerate(small_in):
        wait_dma(dst, v_sem.at[k])
    pieces = [v_bqkv[i // 2, i % 2:i % 2 + 1, :].astype(F32) for i in range(6)]
    bias = jnp.concatenate([*pieces, jnp.zeros((1, D - QKV), F32)], axis=1)
    rows = [v[...].astype(F32) for v in (v_ln, v_bout, v_bfc2, v_bfc1)]
    wsv[p] = jnp.concatenate([*rows, bias, jnp.zeros((SMALL // 2, D), F32)], axis=0).astype(BF)
    wait_dma(wqv.at[p], w_local.at[1])

    def spread(group, way, dev):
        for k in group:
            src = w_hbm[k] if k in mlp_w else w_vm[k].at[p]
            send(src, w_vm[k].at[p], w_send.at[way, k], w_recv.at[p, k], dev)

    def gather_out_proj():
        for k in range(1, TP):
            send(wo, wo_mine, wz_s.at[k], wz_r.at[at.z], {"tp": (at.z + k) % TP})

    def spread_out_proj():
        wait_dma(wo_mine, w_local.at[4])
        for k in range(1, TP):
            wait_dma(wo_mine, wz_r.at[(at.z + k) % TP])
            wait_dma(wo_mine, wz_s.at[k])
        spread(out_proj, 0, at.mate)

    @when(c == 0)
    def _():
        spread(every[:3], 1, at.across)

    @when(p != 1)
    def _():
        gather_out_proj()

    spread(at_once, 0, at.mate)
    for j in range(NJ):
        local(dy.at[y, at.rows_of(j)], gcur.at[chunk(j)], dy_sem.at[j])

    def weights_on(s, group):
        @when((y != s // 2) & (c == s % 2))
        def _():
            for k in group:
                wait_dma(w_vm[k].at[s], w_recv.at[s, k])
                send(w_vm[k].at[s], w_vm[k].at[s], w_fwd.at[k], w_recv.at[s, k], at.mate)

    def weights_ready(s, group):
        @when(p == s)
        def _():
            for k in group:
                if k in mlp_w:
                    wait_dma(w_vm[k].at[p], w_local.at[k])

        @when((p != s) & ((y == s // 2) | (c != s % 2)))
        def _():
            for k in group:
                wait_dma(w_vm[k].at[s], w_recv.at[s, k])

    def send_home(l, src, dst, ssem, rsem):
        @when(p == l)
        def _():
            local(src, dst, ssem)

        @when(p != l)
        def _():
            send(src, dst, ssem, rsem.at[p], {"pp": l})

    weights_on(0, group_a)
    weights_ready(0, group_a)

    def finish_y(l, j):
        rows = chunk(j)
        total = line.get(NJ + j)
        out = (xm[l, rows, :].astype(F32) + total + row(wsv[l].astype(F32), BFC2)).astype(BF)

        @when(l > 0)
        def _():
            wait_dma(gcur.at[rows], ho_s.at[j])

        xs[l + 1, rows, :] = out
        send_home(l, xs.at[l + 1, rows], h_out.at[y, at.rows_of(j)], ho_s.at[j], ho_r)

    def query_places(shape, axis, odd):
        return lax.broadcasted_iota(jnp.int32, shape, axis) % CH + (KB * odd + CH * ((c + odd) % 2))

    def tail_keys(jj, odd):
        return pl.ds(pl.multiple_of(jj * WIDE, WIDE), KB * (1 + odd))

    def attn_pair(l, jj):
        rows = pair(jj)
        both = (2 * jj, 2 * jj + 1)

        @when(l == 0)
        def _():
            for j in both:
                wait_dma(xs.at[0, chunk(j)], x_sem.at[j])

        @when(l > 0)
        def _():
            for j in both:
                finish_y(l - 1, j)

        small = wsv[l].astype(F32)
        xhat, _ = ln_stats(xs[l, rows, :].astype(F32))
        h1 = (xhat * row(small, GAIN1) + row(small, SHIFT1)).astype(BF)
        qkv = (nt(h1, wqv[l]) + row(small, BQKV)[:, :QKV]).astype(BF)
        for k, j in enumerate(both):
            kv[l, at.rows_of(j), :] = qkv[k * CH:(k + 1) * CH, W:]
        for j in both:
            mine = kv.at[l, at.rows_of(j)]
            send(mine, mine, kv_s.at[j], kv_r.at[j], at.mate)
        q = qkv[:, :W]
        qs[l, rows, :] = q
        q4 = head_stack(q * jnp.asarray(0.125, BF))
        lsum[...] = jnp.full_like(lsum, MASKED)

        def pass_one(kb):
            s = nt(q4, kv[l, blk(kb, WIDE), 0:W])
            scores[kb] = s
            lsum[...] = jnp.maximum(lsum[...], fold(s, jnp.maximum))

        loop(jj, pass_one)
        for j in both:
            wait_dma(kv.at[l, at.rows_of(j)], kv_r.at[j])
        s = nt(q4, kv[l, blk(jj, WIDE), 0:W])
        r = lax.broadcasted_iota(jnp.int32, (WIDE, WIDE), 0) % KB
        seen = r % CH + jnp.where(r < CH, CH * c, KB + CH * (1 - c)) >= lax.broadcasted_iota(jnp.int32, (WIDE, WIDE), 1)
        s = jnp.where(seen, s, MASKED)
        top = jnp.max(jnp.maximum(lsum[...], fold(s, jnp.maximum)), axis=-1, keepdims=True)

        def weigh(s, keys):
            e = jnp.exp(s - top)
            return fold(e, jnp.add), nn(e.astype(BF), kv[l, keys, W:])

        lsum[...], acc[...] = weigh(s, blk(jj, WIDE))

        def pass_two(kb):
            more, part_o = weigh(scores[kb], blk(kb, WIDE))
            lsum[...] += more
            acc[...] += part_o

        loop(jj, pass_two)
        den = jnp.sum(lsum[...], axis=-1, keepdims=True)
        o = head_merge(acc[...] / den).astype(BF)
        os_[l, rows, :] = o
        stat = as_row(top + jnp.log(den))
        for k, j in enumerate(both):
            lses[l, blk(j, 8), :] = jnp.concatenate([stat[:, k * CH:(k + 1) * CH], stat[:, KB + k * CH:KB + (k + 1) * CH]], axis=1)
        for k, j in enumerate(both):
            gather.emit(j, o[k * CH:(k + 1) * CH])
            line.serve(SLOTS * l + j)

    def mlp_op(l, j):
        rows = chunk(j)
        small = wsv[l].astype(F32)
        mid = (xs[l, rows, :].astype(F32) + nn(gather.get(j), wov[l]) + row(small, BOUT)).astype(BF)
        xm[l, rows, :] = mid

        @when((l == 0) & (y == 1))
        def _():
            send(xm.at[0, rows], xm_far.at[rows], xf_s.at[j], xf_r.at[j], at.across)

        xhat, _ = ln_stats(mid.astype(F32))
        h2 = (xhat * row(small, GAIN2) + row(small, SHIFT2)).astype(BF)
        u = nn(h2, w1v[l]) + row(small, BFC1)
        a = 0.5 * u * (1.0 + jnp.tanh(GELU_C * (u + GELU_A * u * u * u)))
        gather.sent(j)
        line.emit(SLOTS * l + NJ + j, nn(a.astype(BF), w2v[l]))

    def forward_layer(l):
        def attn_step(jj):
            with jax.named_scope("attn"):
                attn_pair(l, jj)

            @when((l == 0) & (jj == 0) & (c == 0))
            def _():
                spread_out_proj()
                spread(out_proj, 1, at.across)
                spread(mlp_w[1:], 1, at.across)

            @when((l == 0) & (jj == 1))
            def _():
                weights_on(0, mlp_w[:1])

                @when(p == 1)
                def _():
                    gather_out_proj()

            @when((l == 0) & (jj == 2))
            def _():
                weights_on(0, out_proj)

            @when((l == 1) & (jj == 2))
            def _():
                weights_on(1, group_m)

        loop(PAIRS, attn_step)

        @when(l == 0)
        def _():
            weights_on(0, mlp_w[1:])

            @when(c == 1)
            def _():
                spread_out_proj()
                spread(every, 1, at.across)

        @when(l < 2)
        def _():
            weights_ready(l, group_m)

        def mlp_step(j):
            with jax.named_scope("mlp"):
                mlp_op(l, j)

            for when_j, step in ((3, weights_on), (NJ - 2, weights_ready)):
                @when((j == when_j) & (l < LAYERS - 1))
                def _():
                    step(l + 1, group_a)

                @when((j == when_j) & (l > 0) & (l < LAYERS - 1))
                def _():
                    step(l + 1, group_m)

        loop(NJ, mlp_step)
        loop(NJ, lambda j: wait_dma(kv.at[0, chunk(0)], kv_s.at[j]))

    for l in range(LAYERS):
        sm[l] = jnp.zeros((SMALL, D), F32)
    loop(LAYERS, forward_layer)

    groups = (((a_w1, d_w1, y_w1, o_w1), (a_w2, d_w2, y_w2, o_w2)), ((a_q, d_q, y_q, o_q), (a_o, d_o, y_o, o_o)))

    def add_into(dst, src):
        def body(i):
            rows = blk(i, HALF)
            dst[rows, :] += src[rows, :]

        loop(dst.shape[0] // HALF, body)

    def grad_to_mate(l, g):
        @when(c != l % 2)
        def _():
            for k, (own, mid, _, _) in enumerate(groups[g]):
                send(own, mid, d_s.at[g, k], d_r.at[g, k], at.mate)

    def grad_across(l, g, whole=True):
        @when(c != l % 2)
        def _():
            for k, (own, _, _, _) in enumerate(groups[g]):
                wait_dma(own, d_s.at[g, k])

        @when(c == l % 2)
        def _():
            for k, (own, mid, far, _) in enumerate(groups[g]):
                wait_dma(mid, d_r.at[g, k])
                add_into(mid, own)

                @when((y != l // 2) & whole)
                def _():
                    send(mid, far, y_s.at[g, k], y_r.at[g, k], at.across)

    def grad_home(l, g):
        @when((c == l % 2) & (y != l // 2))
        def _():
            for k, (_, mid, _, _) in enumerate(groups[g]):
                wait_dma(mid, y_s.at[g, k])

        @when(p == l)
        def _():
            for k, (_, mid, far, out) in enumerate(groups[g]):
                wait_dma(far, y_r.at[g, k])
                add_into(far, mid)
                local(far, out, o_sem.at[g, k])

    def add_small(l, r, value):
        sm[l, r:r + 1, :] += value

    def finish_layer(l, j):
        rows = chunk(j)
        dh1 = line.get(SLOTS - 1 - j)
        xhat, rstd = ln_stats(xs[l, rows, :].astype(F32))
        add_small(l, GAIN1, colsum(dh1 * xhat))
        add_small(l, SHIFT1, colsum(dh1))
        out = (gm[rows, :] + ln_back(dh1, xhat, rstd, row(wsv[l].astype(F32), GAIN1))).astype(BF)

        @when(l < LAYERS - 1)
        def _():
            wait_dma(gcur.at[rows], gi_s.at[j])

        gcur[rows, :] = out

        @when((l == 1) & (y == 1))
        def _():
            send(gcur.at[rows], g_far.at[rows], gi_s.at[j], gf_r.at[j], at.across)

        @when((l == 0) & (y == 1))
        def _():
            half = blk(2 * j + at.z % 2, HALF)
            send(gcur.at[half], g_half.at[c, j], gi_s.at[j], gh_r.at[c, j], {"pp": 0})

        @when((l > 1) | (y == 0))
        def _():
            send_home(l, gcur.at[rows], g_in.at[y, at.rows_of(j)], gi_s.at[j], gi_r)

    def mlp_back(l, i):
        j = NJ - 1 - i
        rows = chunk(j)

        @when(l == LAYERS - 1)
        def _():
            wait_dma(gcur.at[rows], dy_sem.at[j])
            finish_y(l, i)

        @when(l < LAYERS - 1)
        def _():
            finish_layer(l + 1, j)

        g = gcur[rows, :]
        dpre = mlp_grads(l, j, xm[l, rows, :], g)
        add_small(l, BFC2, colsum(g.astype(F32)))
        add_small(l, BFC1, colsum(dpre))
        line.emit(FWD + SLOTS * (LAYERS - 1 - l) + i, nt(dpre.astype(BF), w1v[l]))

        @when((l > 0) | (y == 0))
        def _():
            mlp_weight_grads(i, gcur)

    def mlp_grads(l, j, mid, g):
        small = wsv[l].astype(F32)
        xhat, _ = ln_stats(mid.astype(F32))
        h2 = (xhat * row(small, GAIN2) + row(small, SHIFT2)).astype(BF)
        u = nn(h2, w1v[l]) + row(small, BFC1)
        t = jnp.tanh(GELU_C * (u + GELU_A * u * u * u))
        half = 0.5 * (1.0 + t)
        slope = half + 0.5 * u * (1.0 - t * t) * (GELU_C * (1.0 + 3.0 * GELU_A * u * u))
        dpre = nt(g, w2v[l]) * slope
        spot = chunk(j % 2)
        h2p[spot, :] = h2
        dprep[spot, :] = dpre.astype(BF)
        ap[spot, :] = (u * half).astype(BF)
        return dpre

    def mlp_weight_grads(i, g_ref):
        grads = blk((NJ - 1 - i) // 2, KB)

        @when(i == 1)
        def _():
            a_w1[...] = tn(h2p[...], dprep[...])
            a_w2[...] = tn(ap[...], g_ref[grads, :])

        @when((i > 1) & (i % 2 == 1))
        def _():
            a_w1[...] += tn(h2p[...], dprep[...])
            a_w2[...] += tn(ap[...], g_ref[grads, :])

    def far_mlp_weight_grads(i):
        j = NJ - 1 - i
        rows = chunk(j)
        wait_dma(xm_far.at[rows], xf_r.at[j])
        wait_dma(g_far.at[rows], gf_r.at[j])
        dst = g_in.at[1, at.rows_of(j)]

        @when(c == 1)
        def _():
            local(g_far.at[rows], dst, gi_r.at[3])

        @when(c == 0)
        def _():
            send(g_far.at[rows], dst, gf_s.at[j], gi_r.at[2], at.mate)

        mlp_grads(0, j, xm_far[rows, :], g_far[rows, :])

        @when(i % 2 == 1)
        def _():
            a_w1[...] += tn(h2p[...], dprep[...])
            a_w2[...] += tn(ap[...], g_far[blk(j // 2, KB), :])

    def swap_halves(i):
        j = NJ - 1 - i
        for core in range(2):
            piece = g_half.at[core, j]
            wait_dma(piece, gh_r.at[core, j])
            out = g_in.at[1, blk(4 * j + 2 * ((core + j) % 2) + at.z % 2, HALF)]
            local(piece, out, gx.at[0])
            send(piece, out, gx.at[1], gx.at[2], {"tp": at.z + 1 - 2 * (at.z % 2)})

    def far_sums():
        for k, (own, mid, _, out) in enumerate(groups[0]):
            wait_dma(mid, d_r.at[0, k])
            add_into(mid, own)
            local(mid, out, o_sem.at[0, k])

    def attn_weight_grads(l):
        small = wsv[l].astype(F32)

        def normed(jj):
            xhat, _ = ln_stats(xs[l, pair(jj), :].astype(F32))
            h1s[pair(jj), :] = (xhat * row(small, GAIN1) + row(small, SHIFT1)).astype(BF)

        loop(PAIRS, normed)
        a_q[...] = tn(dqkvs[...], h1s[...])
        a_o[...] = tn(os_[l], gms[...])
        grad_to_mate(l, 1)

    def attn_back(l, jj, odd):
        j = 2 * jj + odd
        rows = chunk(j)
        small = wsv[l].astype(F32)
        dh2 = line.get(NJ - 1 - j)
        xhat, rstd = ln_stats(xm[l, rows, :].astype(F32))
        add_small(l, GAIN2, colsum(dh2 * xhat))
        add_small(l, SHIFT2, colsum(dh2))
        wide = gcur[rows, :].astype(F32) + ln_back(dh2, xhat, rstd, row(small, GAIN2))
        gm[rows, :] = wide
        add_small(l, BOUT, colsum(wide))
        gmid = wide.astype(BF)
        gms[rows, :] = gmid
        do = nt(gmid, wov[l, chunk(at.z), :]).astype(BF)
        delta = jnp.sum(head_stack(do.astype(F32) * os_[l, rows, :].astype(F32)), axis=-1, keepdims=True)
        delta = as_row(delta)[0:1]
        lse = lses[l, blk(j, 8), :][0:1]
        q2 = head_stack(qs[l, rows, :] * jnp.asarray(0.125, BF))
        do2 = head_stack(do)

        def block(keys, masked):
            k = kv[l, keys, 0:W]
            st = nt(k, q2)
            if masked:
                st = jnp.where(query_places(st.shape, 1, odd) >= lax.broadcasted_iota(jnp.int32, st.shape, 0), st, MASKED)
            pt = jnp.exp(st - lse)
            dst = (pt * (nt(kv[l, keys, W:], do2) - delta)).astype(BF)
            dk = nn(dst, q2)
            dv = nn(pt.astype(BF), do2)
            dq = tn(dst, k)
            dkv[keys, 0:W] += dk
            dkv[keys, W:] += dv
            return dq

        dq_acc[...] = block(tail_keys(jj, odd), True)
        send(dkv.at[at.mate_rows(j)], pk.at[j], dk_s.at[j], dk_r.at[j], at.mate)

        def full(kb):
            dq_acc[...] += block(blk(kb, WIDE), False)

        loop(jj, full)
        dqkvs[rows, 0:W] = (head_merge(dq_acc[...]) * 0.125).astype(BF)

    def qkv_back(l, j):
        rows = chunk(j)
        wait_dma(pk.at[j], dk_r.at[j])
        dkv_own = (dkv[at.rows_of(j), :] + pk[j]).astype(BF)
        dqkvs[rows, W:] = dkv_own
        dqkv = jnp.concatenate([dqkvs[rows, 0:W], dkv_own], axis=1)
        sm[l, BQKV:BQKV + 1, 0:QKV] += colsum(dqkv.astype(F32))
        line.emit(FWD + SLOTS * (LAYERS - l) - 1 - j, nn(dqkv, wqv[l]))

    def backward_layer(n):
        l = LAYERS - 1 - n

        def clear(i):
            dkv[blk(i, HALF), :] = jnp.zeros((HALF, KB), F32)

        def first_half(i):
            @when((i == 1) & (l < LAYERS - 1))
            def _():
                attn_weight_grads(l + 1)

            @when(i == 4)
            def _():
                @when(l < LAYERS - 2)
                def _():
                    grad_home(l + 2, 1)

                @when(l < LAYERS - 1)
                def _():
                    grad_across(l + 1, 1)

            @when(i == 3)
            def _():
                loop(SEQ // HALF, clear)

            with jax.named_scope("B1"):
                mlp_back(l, i)

        loop(NJ, first_half)

        @when(l > 0)
        def _():
            grad_to_mate(l, 0)

        def second_half(ii):
            jj = PAIRS - 1 - ii

            @when((ii == 1) & (l < LAYERS - 1))
            def _():
                grad_home(l + 1, 0)

            with jax.named_scope("B2"):
                attn_back(l, jj, 1)

            @when((ii == 0) & (l > 0))
            def _():
                grad_across(l, 0)

            with jax.named_scope("B3"):
                qkv_back(l, 2 * jj + 1)
            with jax.named_scope("B2"):
                attn_back(l, jj, 0)
            with jax.named_scope("B3"):
                qkv_back(l, 2 * jj)

        loop(PAIRS, second_half)
        loop(NJ, lambda j: wait_dma(pk.at[j], dk_s.at[j]))

    loop(LAYERS, backward_layer)
    attn_weight_grads(0)
    last = FWD + LAYERS * SLOTS - 1

    def finish_last(i):
        @when((i == 1) | (i == 2))
        def _():
            line.serve_first(last - 2 + i)

        @when(i > 3)
        def _():
            line.serve_second(last - NJ + 1 + i)

        finish_layer(0, NJ - 1 - i)

        @when(y == 0)
        def _():
            far_mlp_weight_grads(i)

        @when((p == 0) & at.leaf & (i > 2))
        def _():
            swap_halves(i - 3)

        first = jnp.where(at.hub, 2, 0)

        @when(i == first)
        def _():
            grad_across(0, 1, False)

        @when((i >= first) & (i < first + 6) & (p == 2))
        def _():
            rows = blk(i - first, HALF)
            send(d_q.at[rows], y_q.at[rows], y_s.at[1, 0], y_r.at[1, 0], at.across)

    loop(NJ, finish_last)

    @when(p == 1)
    def _():
        for k, (own, mid, _, _) in enumerate(groups[0]):
            send(own, mid, d_s.at[0, k], d_r.at[0, k], at.mate)

    @when(p == 2)
    def _():
        send(d_o, y_o, y_s.at[1, 1], y_r.at[1, 1], at.across)

    for s in range(LAYERS):
        @when(p != s)
        def _():
            send(sm.at[s], rsm.at[p], sm_s.at[s], sm_r.at[p], {"pp": s})

    @when((p == 0) & at.hub)
    def _():
        loop(NJ - 3, swap_halves)

    for k in every:
        wait_dma(w_vm[k].at[0], w_send.at[0, k])
        wait_dma(w_vm[k].at[0], w_send.at[1, k])
        wait_dma(w_vm[k].at[0], w_fwd.at[k])
    line.close()
    loop(NJ, lambda j: wait_dma(gcur.at[chunk(0)], ho_s.at[j]))

    @when(p == 1)
    def _():
        for k, (own, mid, _, _) in enumerate(groups[0]):
            wait_dma(own, d_s.at[0, k])

    @when(p == 0)
    def _():
        swap_halves(NJ - 3)
        swap_halves(NJ - 2)
        far_sums()
        swap_halves(NJ - 1)
        loop(NJ, lambda j: wait_dma(g_far.at[chunk(j)], gf_s.at[j]))
        for k in range(3):
            wait_dma(g_half, gx.at[k])

    @when(y == 1)
    def _():
        loop(NJ, lambda j: wait_dma(xm.at[0, chunk(j)], xf_s.at[j]))

    grad_home(1, 1)
    grad_home(0, 1)
    for s in range(LAYERS):
        @when(p != s)
        def _():
            wait_dma(sm.at[s], sm_s.at[s])
            wait_dma(rsm.at[s], sm_r.at[s])
    rsm[p] = sm[p]
    sm[0] = (rsm[0] + rsm[1]) + (rsm[2] + rsm[3])
    local(sm.at[0], o_sm, x_sem.at[0])

    def sent(j):
        @when(y == 0)
        def _():
            wait_dma(gcur.at[chunk(0)], gi_s.at[j])

        @when(y == 1)
        def _():
            wait_dma(g_half.at[0, 0], gi_s.at[j])

    loop(NJ, sent)
    for s in range(LAYERS):
        @when(p != s)
        def _():
            wait_dma(h_out.at[0, pl.ds(0, ROWS)], ho_r.at[s])

        @when((p != s) & ((p > 0) | (s == 1)))
        def _():
            wait_dma(g_in.at[0, pl.ds(0, ROWS)], gi_r.at[s])

    for g, items in enumerate(groups):
        for k, (_, _, far, _) in enumerate(items):
            wait_dma(far, o_sem.at[g, k])
    wait_dma(sm.at[0], x_sem.at[0])


def run_layers(*args):
    hbm = pl.BlockSpec(memory_space=pl.ANY)
    dma = pltpu.SemaphoreType.DMA
    slots = pltpu.VMEM((SLOTS, CH, D), BF)
    slot_sem = dma((SLOTS,))
    chunk_sem = dma((NJ,))
    stage_sem = dma((LAYERS,))
    pair_sem = dma((2, 2))

    def bf(*shape):
        return pltpu.VMEM(shape, BF)

    def f32(*shape):
        return pltpu.VMEM(shape, F32)

    grad_shapes = ((D, D), (D, D), (QKV, D), (W, D))
    grads = [f32(*shape) for shape in grad_shapes]
    acts = jax.ShapeDtypeStruct((2, SEQ, D), BF)
    return pl.pallas_call(
        decoder_kernel,
        out_shape=[acts, acts, *(jax.ShapeDtypeStruct(shape, F32) for shape in (*grad_shapes, (SMALL, D)))],
        in_specs=[hbm] * len(args),
        out_specs=[hbm] * 7,
        scratch_shapes=[
            bf(LAYERS, SMALL, D), bf(LAYERS, QKV, D), *[bf(LAYERS, D, D)] * 3,
            bf(LAYERS, SEQ, KB), bf(LAYERS + 1, ROWS, D), bf(LAYERS, ROWS, D), bf(LAYERS, ROWS, W), bf(LAYERS, ROWS, W),
            f32(LAYERS, NJ * 8, KB), f32(PAIRS, WIDE, WIDE), f32(WIDE, W), f32(WIDE, W),
            bf(ROWS, D), f32(ROWS, D), f32(SEQ, KB), f32(NJ, CH, KB), bf(ROWS, D), bf(ROWS, QKV), bf(ROWS, D), *[bf(KB, D)] * 3, f32(KB, W), bf(ROWS, D), bf(ROWS, D), bf(2, NJ, HALF, D),
            *grads, *grads, *grads, f32(LAYERS, SMALL, D), f32(LAYERS, SMALL, D),
            *[slots] * 4, *[slot_sem] * 5, bf(NJ, TP, CH, W), *[chunk_sem] * 5,
            *(pltpu.VMEM(a.shape, BF) for a in args[6:]), dma((len(args) - 6,)),
            chunk_sem, stage_sem, stage_sem, dma((5,)), dma((2, 5)), dma((LAYERS, 5)), dma((5,)),
            chunk_sem, chunk_sem, chunk_sem, stage_sem,
            chunk_sem, chunk_sem, chunk_sem, chunk_sem, stage_sem, *[pair_sem] * 5, stage_sem, stage_sem, *[chunk_sem] * 4, dma((2, NJ)), dma((3,)),
        ],
        compiler_params=pltpu.CompilerParams(collective_id=0, has_side_effects=True, vmem_limit_bytes=VMEM_LIMIT),
        name="decoder_layers",
    )(*args)


def collect_kernel(*refs):
    count = 6
    srcs, small, outs = refs[:count], refs[count], refs[count + 1:2 * count + 1]
    ln, bout, bfc1, bfc2, bqkv = refs[2 * count + 1:2 * count + 6]
    bufs, (sem_in, sem_out) = refs[2 * count + 6:3 * count + 6], refs[3 * count + 6:]
    for k in range(count):
        local(srcs[k], bufs[k], sem_in.at[k])
    ln[...] = small[0:BOUT, :]
    for r, out in ((BOUT, bout), (BFC1, bfc1), (BFC2, bfc2)):
        out[...] = small[r:r + 1, :]
    for i in range(6):
        bqkv[i // 2, i % 2:i % 2 + 1, :] = small[BQKV:BQKV + 1, i * HALF:(i + 1) * HALF]
    for k in range(count):
        wait_dma(bufs[k], sem_in.at[k])
        local(bufs[k], outs[k], sem_out.at[k])
    for k in range(count):
        wait_dma(bufs[k], sem_out.at[k])


def collect(*args):
    hbm, vmem = pl.BlockSpec(memory_space=pl.ANY), pl.BlockSpec(memory_space=pltpu.VMEM)
    big = args[:-1]
    shapes = [(GAIN1 + 4, D), (1, D), (1, D), (1, D), (3, 2, 64)]
    return pl.pallas_call(
        collect_kernel,
        out_shape=[*(jax.ShapeDtypeStruct(a.shape, a.dtype) for a in big), *(jax.ShapeDtypeStruct(shape, F32) for shape in shapes)],
        in_specs=[hbm] * len(big) + [vmem],
        out_specs=[hbm] * len(big) + [vmem] * len(shapes),
        scratch_shapes=[*(pltpu.VMEM(a.shape, a.dtype) for a in big), *[pltpu.SemaphoreType.DMA((len(big),))] * 2],
        compiler_params=pltpu.CompilerParams(vmem_limit_bytes=VMEM_LIMIT),
        name="collect",
    )(*args)


def solution(mesh):
    def program(x_in, dy_out, w_qkv, b_qkv, w_out, b_out, ln_par, w_fc1, b_fc1, w_fc2, b_fc2):
        layers, parts, _, heads, width = w_qkv.shape
        wq = w_qkv.transpose(0, 1, 3, 4, 2).reshape(QKV, D)
        h_out, g_in, *rest = run_layers(
            x_in.reshape(2, SEQ, D), dy_out.reshape(2, SEQ, D), wq, w_out.reshape(W, D), w_fc1.reshape(D, D), w_fc2.reshape(D, D),
            ln_par.reshape(-1, D), b_out, b_fc2, b_fc1, b_qkv.reshape(b_qkv.shape[1:]))
        h_out, g_in, d_w1, d_w2, d_q, d_o, ln, bout, bfc1, bfc2, bqkv = collect(h_out.reshape(-1, D), g_in.reshape(-1, D), *rest)
        acts = (layers, *x_in.shape)
        return (h_out.reshape(acts), g_in.reshape(acts),
                d_q.reshape(layers, parts, heads, width, D).transpose(0, 1, 4, 2, 3), bqkv.reshape(b_qkv.shape),
                d_o.reshape(w_out.shape), bout, ln.reshape(ln_par.shape),
                d_w1.reshape(w_fc1.shape), bfc1, d_w2.reshape(w_fc2.shape), bfc2)

    act_spec = P(NO, "dp", NO, NO)
    arg_specs = (act_spec, act_spec,
                 P("pp", NO, NO, "tp", NO), P("pp", NO, "tp", NO), P("pp", "tp", NO, NO),
                 P("pp", NO), P("pp", NO, NO), P("pp", NO, "tp"), P("pp", "tp"),
                 P("pp", "tp", NO), P("pp", NO))
    stage_spec = P("pp", NO, "dp", NO, NO)
    grad_axes = ("dp", "pp")
    result_specs = (stage_spec, stage_spec,
                    P(grad_axes, NO, NO, "tp", NO), P(grad_axes, NO, "tp", NO), P(grad_axes, "tp", NO, NO),
                    P(grad_axes, NO), P(grad_axes, NO, NO), P(grad_axes, NO, "tp"), P(grad_axes, "tp"),
                    P(grad_axes, "tp", NO), P(grad_axes, NO))
    return jax.shard_map(program, mesh=mesh, in_specs=arg_specs, out_specs=result_specs, check_vma=False)
```

```python
import jax
import jax.numpy as jnp
from jax import lax
from jax.experimental import pallas as pl
from jax.experimental.pallas import tpu as pltpu
from jax.sharding import PartitionSpec as P

LN_EPS = 1e-5
BF = jnp.bfloat16
F32 = jnp.float32
MESH = pl.DeviceIdType.MESH

LAYERS = 4
SEQ = 2048
D = 512
CH = 128
NJ = 8
PAIRS = NJ // 2
ROWS = CH * NJ
SLOTS = 2 * NJ
FWD = LAYERS * SLOTS
W = 128
QKV = 3 * W
KB = 256
WIDE = 2 * KB
SMALL = 16
GELU_C = 0.7978845608028654
GELU_A = 0.044715
MASKED = -1e30
NO = None
TP = 4
HALF = CH // 2
VMEM_LIMIT = 67043328
GAIN1, SHIFT1, GAIN2, SHIFT2, BOUT, BFC2, BFC1, BQKV = range(8)


def nn(a, b):
    return lax.dot_general(a, b, (((1,), (0,)), ((), ())), preferred_element_type=F32)


def nt(a, b):
    return lax.dot_general(a, b, (((1,), (1,)), ((), ())), preferred_element_type=F32)


def tn(a, b):
    return lax.dot_general(a, b, (((0,), (0,)), ((), ())), preferred_element_type=F32)


def ln_stats(x_wide):
    mean = jnp.mean(x_wide, axis=-1, keepdims=True)
    cent = x_wide - mean
    var = jnp.mean(cent * cent, axis=-1, keepdims=True)
    rstd = lax.rsqrt(var + LN_EPS)
    return cent * rstd, rstd


def ln_back(dy, xhat, rstd, gain):
    dxhat = dy * gain
    m1 = jnp.mean(dxhat, axis=-1, keepdims=True)
    m2 = jnp.mean(dxhat * xhat, axis=-1, keepdims=True)
    return rstd * (dxhat - m1 - xhat * m2)


def colsum(v):
    return jnp.sum(v, axis=0, keepdims=True)


def row(small, r):
    return small[r:r + 1]


def blk(i, n):
    return pl.ds(pl.multiple_of(i * n, n), n)


def chunk(j):
    return blk(j, CH)


def pair(jj):
    return blk(jj, KB)


def loop(n, body):
    def step(i, carry):
        body(i)
        return carry

    lax.fori_loop(0, n, step, 0)


when = pl.when


def wait_dma(ref, sem):
    pltpu.make_async_copy(ref, ref, sem).wait()


def local(src, dst, sem):
    pltpu.make_async_copy(src, dst, sem).start()


def send(src, dst, ssem, rsem, dev):
    pltpu.make_async_remote_copy(src, dst, ssem, rsem, device_id=dev, device_id_type=MESH).start()


class Place:
    def __init__(self):
        self.z = lax.axis_index("tp")
        self.p = lax.axis_index("pp")
        self.y = self.p // 2
        self.c = self.p % 2
        self.hub = (self.z == 1) | (self.z == 2)
        self.leaf = jnp.logical_not(self.hub)
        self.my_hub = {"tp": jnp.where(self.z == 0, 1, 2)}
        self.my_leaf = {"tp": jnp.where(self.z == 1, 0, 3)}
        self.other_hub = {"tp": 3 - self.z}
        self.mate = {"pp": self.p + 1 - 2 * self.c}
        self.across = {"pp": 2 * (1 - self.y) + self.c}

    def rows_of(self, j):
        return chunk(2 * j + (self.c + j) % 2)

    def mate_rows(self, j):
        return chunk(2 * j + (self.c + j + 1) % 2)

    def enter(self):
        bar = pltpu.get_barrier_semaphore()

        def greet(dev):
            pl.semaphore_signal(bar, inc=1, device_id=dev, device_id_type=MESH)

        for k in range(1, TP):
            greet({"pp": (self.p + k) % TP})
            greet({"tp": (self.z + k) % TP})

        pl.semaphore_wait(bar, 6)


def is_gather(e):
    return (e < FWD) & (e % SLOTS < NJ)


class LineSum:
    def __init__(self, at, gather, part, lbuf, hbuf, fin, s1, s2, r_l, r_h, r_f):
        self.gather = gather
        self.at, self.part, self.lbuf, self.hbuf, self.fin = at, part, lbuf, hbuf, fin
        self.s1, self.s2, self.r_l, self.r_h, self.r_f = s1, s2, r_l, r_h, r_f

    def emit(self, e, value):
        slot = e % SLOTS

        @when((e >= SLOTS) & jnp.logical_not(is_gather(e - SLOTS)))
        def _():
            wait_dma(self.part.at[slot], self.s1.at[slot])

        self.part[slot] = value.astype(BF)

        @when(self.at.leaf)
        def _():
            send(self.part.at[slot], self.lbuf.at[slot], self.s1.at[slot], self.r_l.at[slot], self.at.my_hub)

        self.serve(e)

    def serve(self, e):
        for back, mine, other in ((1, self.serve_first, self.gather.serve_first), (3, self.serve_second, self.gather.serve_second)):
            mine(e - back)

            @when(self.at.hub & (e >= back) & is_gather(e - back))
            def _():
                other((e - back + SLOTS) % SLOTS)

    def serve_first(self, e):
        slot = (e + SLOTS) % SLOTS

        @when(self.at.hub & (e >= 0) & jnp.logical_not(is_gather(e)))
        def _():
            wait_dma(self.lbuf.at[slot], self.r_l.at[slot])
            self.part[slot] = (self.part[slot].astype(F32) + self.lbuf[slot].astype(F32)).astype(BF)
            send(self.part.at[slot], self.hbuf.at[slot], self.s1.at[slot], self.r_h.at[slot], self.at.other_hub)

    def serve_second(self, e):
        slot = (e + SLOTS) % SLOTS

        @when(self.at.hub & (e >= 0) & jnp.logical_not(is_gather(e)))
        def _():
            wait_dma(self.hbuf.at[slot], self.r_h.at[slot])

            @when((e >= SLOTS) & jnp.logical_not(is_gather(e - SLOTS)))
            def _():
                wait_dma(self.fin.at[slot], self.s2.at[slot])

            self.fin[slot] = (self.part[slot].astype(F32) + self.hbuf[slot].astype(F32)).astype(BF)
            send(self.fin.at[slot], self.fin.at[slot], self.s2.at[slot], self.r_f.at[slot], self.at.my_leaf)

    def get(self, slot):
        @when(self.at.leaf)
        def _():
            wait_dma(self.fin.at[slot], self.r_f.at[slot])

        return self.fin[slot].astype(F32)

    def close(self):
        def body(slot):
            wait_dma(self.part.at[slot], self.s1.at[slot])

            @when(self.at.hub)
            def _():
                wait_dma(self.fin.at[slot], self.s2.at[slot])

        loop(SLOTS, body)


class LineGather:
    def __init__(self, at, buf, s_a, s_b, s_c, r_a, r_b):
        self.at, self.buf, self.s_a, self.s_b, self.s_c, self.r_a, self.r_b = at, buf, s_a, s_b, s_c, r_a, r_b
        side = at.z // 2
        self.mine, self.theirs = pl.ds(2 * side, 2), pl.ds(2 - 2 * side, 2)

    def sent(self, j):
        own, two = self.buf.at[j, 0], self.buf.at[j, pl.ds(0, 2)]
        wait_dma(own, self.s_a.at[j])

        @when(self.at.hub)
        def _():
            wait_dma(two, self.s_b.at[j])
            wait_dma(two, self.s_c.at[j])

    def emit(self, j, value):
        at = self.at
        self.buf[j, at.z] = value
        own = self.buf.at[j, at.z]

        @when(at.leaf)
        def _():
            send(own, own, self.s_a.at[j], self.r_a.at[j], at.my_hub)

        @when(at.hub)
        def _():
            send(own, own, self.s_a.at[j], self.r_a.at[j], at.my_leaf)

    def serve_first(self, j):
        wait_dma(self.buf.at[j, 0], self.r_a.at[j])
        two = self.buf.at[j, self.mine]
        send(two, two, self.s_b.at[j], self.r_b.at[j], self.at.other_hub)

    def serve_second(self, j):
        two = self.buf.at[j, self.theirs]
        wait_dma(two, self.r_b.at[j])
        send(two, two, self.s_c.at[j], self.r_b.at[j], self.at.my_leaf)

    def get(self, j):
        @when(self.at.leaf)
        def _():
            wait_dma(self.buf.at[j, 0], self.r_a.at[j])
            wait_dma(self.buf.at[j, self.theirs], self.r_b.at[j])

        return jnp.concatenate([self.buf[j, k] for k in range(TP)], axis=1)


def head_stack(v):
    first = lax.broadcasted_iota(jnp.int32, v.shape, 1) < W // 2
    zero = jnp.zeros_like(v)
    return jnp.concatenate([jnp.where(first, v, zero), jnp.where(first, zero, v)], axis=0)


def head_merge(v):
    n = v.shape[0] // 2
    first = lax.broadcasted_iota(jnp.int32, (n, W), 1) < W // 2
    return jnp.where(first, v[:n], v[n:])


def as_row(v):
    return jnp.broadcast_to(v, (v.shape[0], W)).T[:8]


def fold(v, op):
    out = v[:, :W]
    for k in range(1, v.shape[1] // W):
        out = op(out, v[:, k * W:(k + 1) * W])
    return out


def decoder_kernel(x_in, dy, wq, wo, w1, w2, ln_par, b_out, b_fc2, b_fc1, b_qkv,
                   h_out, g_in, o_w1, o_w2, o_q, o_o, o_sm,
                   wsv, wqv, w1v, w2v, wov, kv, xs, xm, qs, os_, lses, scores, acc, lsum,
                   gcur, gm, dkv, pk, h1s, dqkvs, gms, h2p, dprep, ap, dq_acc, xm_far, g_far, g_half,
                   a_w1, a_w2, a_q, a_o, d_w1, d_w2, d_q, d_o, y_w1, y_w2, y_q, y_o, sm, rsm,
                   part, lbuf, hbuf, fin, s1, s2, r_l, r_h, r_f, og, gs_a, gs_b, gs_c, gr_a, gr_b,
                   v_ln, v_bout, v_bfc2, v_bfc1, v_bqkv, v_sem,
                   x_sem, wz_s, wz_r, w_local, w_send, w_recv, w_fwd, kv_s, kv_r, ho_s, ho_r,
                   dy_sem, dk_s, dk_r, gi_s, gi_r, d_s, d_r, y_s, y_r, o_sem, sm_s, sm_r, xf_s, xf_r, gf_s, gf_r, gh_r, gx):
    at = Place()
    gather = LineGather(at, og, gs_a, gs_b, gs_c, gr_a, gr_b)
    line = LineSum(at, gather, part, lbuf, hbuf, fin, s1, s2, r_l, r_h, r_f)
    y, c, p = at.y, at.c, at.p
    w_hbm = (NO, wq, w1, w2)
    small_in = ((ln_par, v_ln), (b_out, v_bout), (b_fc2, v_bfc2), (b_fc1, v_bfc1), (b_qkv, v_bqkv))
    w_vm = (wsv, wqv, w1v, w2v, wov)
    every = range(len(w_vm))
    at_once, group_a, mlp_w, group_m, out_proj = every[:4], every[:2], every[2:4], every[2:], every[4:]
    wo_mine = wov.at[p, chunk(at.z)]

    for j in range(NJ):
        local(x_in.at[y, at.rows_of(j)], xs.at[0, chunk(j)], x_sem.at[j])
    for k in at_once[1:]:
        local(w_hbm[k], w_vm[k].at[p], w_local.at[k])
    for k, (src, dst) in enumerate(small_in):
        local(src, dst, v_sem.at[k])
    local(wo, wo_mine, w_local.at[4])

    at.enter()

    for k, (_, dst) in enumerate(small_in):
        wait_dma(dst, v_sem.at[k])
    pieces = [v_bqkv[i // 2, i % 2:i % 2 + 1, :].astype(F32) for i in range(6)]
    bias = jnp.concatenate([*pieces, jnp.zeros((1, D - QKV), F32)], axis=1)
    rows = [v[...].astype(F32) for v in (v_ln, v_bout, v_bfc2, v_bfc1)]
    wsv[p] = jnp.concatenate([*rows, bias, jnp.zeros((SMALL // 2, D), F32)], axis=0).astype(BF)
    wait_dma(wqv.at[p], w_local.at[1])

    def spread(group, way, dev):
        for k in group:
            src = w_hbm[k] if k in mlp_w else w_vm[k].at[p]
            send(src, w_vm[k].at[p], w_send.at[way, k], w_recv.at[p, k], dev)

    def gather_out_proj():
        for k in range(1, TP):
            send(wo, wo_mine, wz_s.at[k], wz_r.at[at.z], {"tp": (at.z + k) % TP})

    def spread_out_proj():
        wait_dma(wo_mine, w_local.at[4])
        for k in range(1, TP):
            wait_dma(wo_mine, wz_r.at[(at.z + k) % TP])
            wait_dma(wo_mine, wz_s.at[k])
        spread(out_proj, 0, at.mate)

    @when(c == 0)
    def _():
        spread(every[:3], 1, at.across)

    @when(p != 1)
    def _():
        gather_out_proj()

    spread(at_once, 0, at.mate)
    for j in range(NJ):
        local(dy.at[y, at.rows_of(j)], gcur.at[chunk(j)], dy_sem.at[j])

    def weights_on(s, group):
        @when((y != s // 2) & (c == s % 2))
        def _():
            for k in group:
                wait_dma(w_vm[k].at[s], w_recv.at[s, k])
                send(w_vm[k].at[s], w_vm[k].at[s], w_fwd.at[k], w_recv.at[s, k], at.mate)

    def weights_ready(s, group):
        @when(p == s)
        def _():
            for k in group:
                if k in mlp_w:
                    wait_dma(w_vm[k].at[p], w_local.at[k])

        @when((p != s) & ((y == s // 2) | (c != s % 2)))
        def _():
            for k in group:
                wait_dma(w_vm[k].at[s], w_recv.at[s, k])

    def send_home(l, src, dst, ssem, rsem):
        @when(p == l)
        def _():
            local(src, dst, ssem)

        @when(p != l)
        def _():
            send(src, dst, ssem, rsem.at[p], {"pp": l})

    weights_on(0, group_a)
    weights_ready(0, group_a)

    def finish_y(l, j):
        rows = chunk(j)
        total = line.get(NJ + j)
        out = (xm[l, rows, :].astype(F32) + total + row(wsv[l].astype(F32), BFC2)).astype(BF)

        @when(l > 0)
        def _():
            wait_dma(gcur.at[rows], ho_s.at[j])

        xs[l + 1, rows, :] = out
        send_home(l, xs.at[l + 1, rows], h_out.at[y, at.rows_of(j)], ho_s.at[j], ho_r)

    def query_places(shape, axis, odd):
        return lax.broadcasted_iota(jnp.int32, shape, axis) % CH + (KB * odd + CH * ((c + odd) % 2))

    def tail_keys(jj, odd):
        return pl.ds(pl.multiple_of(jj * WIDE, WIDE), KB * (1 + odd))

    def attn_pair(l, jj):
        rows = pair(jj)
        both = (2 * jj, 2 * jj + 1)

        @when(l == 0)
        def _():
            for j in both:
                wait_dma(xs.at[0, chunk(j)], x_sem.at[j])

        @when(l > 0)
        def _():
            for j in both:
                finish_y(l - 1, j)

        small = wsv[l].astype(F32)
        xhat, _ = ln_stats(xs[l, rows, :].astype(F32))
        h1 = (xhat * row(small, GAIN1) + row(small, SHIFT1)).astype(BF)
        qkv = (nt(h1, wqv[l]) + row(small, BQKV)[:, :QKV]).astype(BF)
        for k, j in enumerate(both):
            kv[l, at.rows_of(j), :] = qkv[k * CH:(k + 1) * CH, W:]
        for j in both:
            mine = kv.at[l, at.rows_of(j)]
            send(mine, mine, kv_s.at[j], kv_r.at[j], at.mate)
        q = qkv[:, :W]
        qs[l, rows, :] = q
        q4 = head_stack(q * jnp.asarray(0.125, BF))
        lsum[...] = jnp.full_like(lsum, MASKED)

        def pass_one(kb):
            s = nt(q4, kv[l, blk(kb, WIDE), 0:W])
            scores[kb] = s
            lsum[...] = jnp.maximum(lsum[...], fold(s, jnp.maximum))

        loop(jj, pass_one)
        for j in both:
            wait_dma(kv.at[l, at.rows_of(j)], kv_r.at[j])
        s = nt(q4, kv[l, blk(jj, WIDE), 0:W])
        r = lax.broadcasted_iota(jnp.int32, (WIDE, WIDE), 0) % KB
        seen = r % CH + jnp.where(r < CH, CH * c, KB + CH * (1 - c)) >= lax.broadcasted_iota(jnp.int32, (WIDE, WIDE), 1)
        s = jnp.where(seen, s, MASKED)
        top = jnp.max(jnp.maximum(lsum[...], fold(s, jnp.maximum)), axis=-1, keepdims=True)

        def weigh(s, keys):
            e = jnp.exp(s - top)
            return fold(e, jnp.add), nn(e.astype(BF), kv[l, keys, W:])

        lsum[...], acc[...] = weigh(s, blk(jj, WIDE))

        def pass_two(kb):
            more, part_o = weigh(scores[kb], blk(kb, WIDE))
            lsum[...] += more
            acc[...] += part_o

        loop(jj, pass_two)
        den = jnp.sum(lsum[...], axis=-1, keepdims=True)
        o = head_merge(acc[...] / den).astype(BF)
        os_[l, rows, :] = o
        stat = as_row(top + jnp.log(den))
        for k, j in enumerate(both):
            lses[l, blk(j, 8), :] = jnp.concatenate([stat[:, k * CH:(k + 1) * CH], stat[:, KB + k * CH:KB + (k + 1) * CH]], axis=1)
        for k, j in enumerate(both):
            gather.emit(j, o[k * CH:(k + 1) * CH])
            line.serve(SLOTS * l + j)

    def mlp_op(l, j):
        rows = chunk(j)
        small = wsv[l].astype(F32)
        mid = (xs[l, rows, :].astype(F32) + nn(gather.get(j), wov[l]) + row(small, BOUT)).astype(BF)
        xm[l, rows, :] = mid

        @when((l == 0) & (y == 1))
        def _():
            send(xm.at[0, rows], xm_far.at[rows], xf_s.at[j], xf_r.at[j], at.across)

        xhat, _ = ln_stats(mid.astype(F32))
        h2 = (xhat * row(small, GAIN2) + row(small, SHIFT2)).astype(BF)
        u = nn(h2, w1v[l]) + row(small, BFC1)
        a = 0.5 * u * (1.0 + jnp.tanh(GELU_C * (u + GELU_A * u * u * u)))
        gather.sent(j)
        line.emit(SLOTS * l + NJ + j, nn(a.astype(BF), w2v[l]))

    def forward_layer(l):
        def attn_step(jj):
            with jax.named_scope("attn"):
                attn_pair(l, jj)

            @when((l == 0) & (jj == 0) & (c == 0))
            def _():
                spread_out_proj()
                spread(out_proj, 1, at.across)
                spread(mlp_w[1:], 1, at.across)

            @when((l == 0) & (jj == 1))
            def _():
                weights_on(0, mlp_w[:1])

                @when(p == 1)
                def _():
                    gather_out_proj()

            @when((l == 0) & (jj == 2))
            def _():
                weights_on(0, out_proj)

            @when((l == 1) & (jj == 2))
            def _():
                weights_on(1, group_m)

        loop(PAIRS, attn_step)

        @when(l == 0)
        def _():
            weights_on(0, mlp_w[1:])

            @when(c == 1)
            def _():
                spread_out_proj()
                spread(every, 1, at.across)

        @when(l < 2)
        def _():
            weights_ready(l, group_m)

        def mlp_step(j):
            with jax.named_scope("mlp"):
                mlp_op(l, j)

            for when_j, step in ((3, weights_on), (NJ - 2, weights_ready)):
                @when((j == when_j) & (l < LAYERS - 1))
                def _():
                    step(l + 1, group_a)

                @when((j == when_j) & (l > 0) & (l < LAYERS - 1))
                def _():
                    step(l + 1, group_m)

        loop(NJ, mlp_step)
        loop(NJ, lambda j: wait_dma(kv.at[0, chunk(0)], kv_s.at[j]))

    for l in range(LAYERS):
        sm[l] = jnp.zeros((SMALL, D), F32)
    loop(LAYERS, forward_layer)

    groups = (((a_w1, d_w1, y_w1, o_w1), (a_w2, d_w2, y_w2, o_w2)), ((a_q, d_q, y_q, o_q), (a_o, d_o, y_o, o_o)))

    def add_into(dst, src):
        def body(i):
            rows = blk(i, HALF)
            dst[rows, :] += src[rows, :]

        loop(dst.shape[0] // HALF, body)

    def grad_to_mate(l, g):
        @when(c != l % 2)
        def _():
            for k, (own, mid, _, _) in enumerate(groups[g]):
                send(own, mid, d_s.at[g, k], d_r.at[g, k], at.mate)

    def grad_across(l, g, whole=True):
        @when(c != l % 2)
        def _():
            for k, (own, _, _, _) in enumerate(groups[g]):
                wait_dma(own, d_s.at[g, k])

        @when(c == l % 2)
        def _():
            for k, (own, mid, far, _) in enumerate(groups[g]):
                wait_dma(mid, d_r.at[g, k])
                add_into(mid, own)

                @when((y != l // 2) & whole)
                def _():
                    send(mid, far, y_s.at[g, k], y_r.at[g, k], at.across)

    def grad_home(l, g):
        @when((c == l % 2) & (y != l // 2))
        def _():
            for k, (_, mid, _, _) in enumerate(groups[g]):
                wait_dma(mid, y_s.at[g, k])

        @when(p == l)
        def _():
            for k, (_, mid, far, out) in enumerate(groups[g]):
                wait_dma(far, y_r.at[g, k])
                add_into(far, mid)
                local(far, out, o_sem.at[g, k])

    def add_small(l, r, value):
        sm[l, r:r + 1, :] += value

    def finish_layer(l, j):
        rows = chunk(j)
        dh1 = line.get(SLOTS - 1 - j)
        xhat, rstd = ln_stats(xs[l, rows, :].astype(F32))
        add_small(l, GAIN1, colsum(dh1 * xhat))
        add_small(l, SHIFT1, colsum(dh1))
        out = (gm[rows, :] + ln_back(dh1, xhat, rstd, row(wsv[l].astype(F32), GAIN1))).astype(BF)

        @when(l < LAYERS - 1)
        def _():
            wait_dma(gcur.at[rows], gi_s.at[j])

        gcur[rows, :] = out

        @when((l == 1) & (y == 1))
        def _():
            send(gcur.at[rows], g_far.at[rows], gi_s.at[j], gf_r.at[j], at.across)

        @when((l == 0) & (y == 1))
        def _():
            half = blk(2 * j + at.z % 2, HALF)
            send(gcur.at[half], g_half.at[c, j], gi_s.at[j], gh_r.at[c, j], {"pp": 0})

        @when((l > 1) | (y == 0))
        def _():
            send_home(l, gcur.at[rows], g_in.at[y, at.rows_of(j)], gi_s.at[j], gi_r)

    def mlp_back(l, i):
        j = NJ - 1 - i
        rows = chunk(j)

        @when(l == LAYERS - 1)
        def _():
            wait_dma(gcur.at[rows], dy_sem.at[j])
            finish_y(l, i)

        @when(l < LAYERS - 1)
        def _():
            finish_layer(l + 1, j)

        g = gcur[rows, :]
        dpre = mlp_grads(l, j, xm[l, rows, :], g)
        add_small(l, BFC2, colsum(g.astype(F32)))
        add_small(l, BFC1, colsum(dpre))
        line.emit(FWD + SLOTS * (LAYERS - 1 - l) + i, nt(dpre.astype(BF), w1v[l]))

        @when((l > 0) | (y == 0))
        def _():
            mlp_weight_grads(i, gcur)

    def mlp_grads(l, j, mid, g):
        small = wsv[l].astype(F32)
        xhat, _ = ln_stats(mid.astype(F32))
        h2 = (xhat * row(small, GAIN2) + row(small, SHIFT2)).astype(BF)
        u = nn(h2, w1v[l]) + row(small, BFC1)
        t = jnp.tanh(GELU_C * (u + GELU_A * u * u * u))
        half = 0.5 * (1.0 + t)
        slope = half + 0.5 * u * (1.0 - t * t) * (GELU_C * (1.0 + 3.0 * GELU_A * u * u))
        dpre = nt(g, w2v[l]) * slope
        spot = chunk(j % 2)
        h2p[spot, :] = h2
        dprep[spot, :] = dpre.astype(BF)
        ap[spot, :] = (u * half).astype(BF)
        return dpre

    def mlp_weight_grads(i, g_ref):
        grads = blk((NJ - 1 - i) // 2, KB)

        @when(i == 1)
        def _():
            a_w1[...] = tn(h2p[...], dprep[...])
            a_w2[...] = tn(ap[...], g_ref[grads, :])

        @when((i > 1) & (i % 2 == 1))
        def _():
            a_w1[...] += tn(h2p[...], dprep[...])
            a_w2[...] += tn(ap[...], g_ref[grads, :])

    def far_mlp_weight_grads(i):
        j = NJ - 1 - i
        rows = chunk(j)
        wait_dma(xm_far.at[rows], xf_r.at[j])
        wait_dma(g_far.at[rows], gf_r.at[j])
        dst = g_in.at[1, at.rows_of(j)]

        @when(c == 1)
        def _():
            local(g_far.at[rows], dst, gi_r.at[3])

        @when(c == 0)
        def _():
            send(g_far.at[rows], dst, gf_s.at[j], gi_r.at[2], at.mate)

        mlp_grads(0, j, xm_far[rows, :], g_far[rows, :])

        @when(i % 2 == 1)
        def _():
            a_w1[...] += tn(h2p[...], dprep[...])
            a_w2[...] += tn(ap[...], g_far[blk(j // 2, KB), :])

    def swap_halves(i):
        j = NJ - 1 - i
        for core in range(2):
            piece = g_half.at[core, j]
            wait_dma(piece, gh_r.at[core, j])
            out = g_in.at[1, blk(4 * j + 2 * ((core + j) % 2) + at.z % 2, HALF)]
            local(piece, out, gx.at[0])
            send(piece, out, gx.at[1], gx.at[2], {"tp": at.z + 1 - 2 * (at.z % 2)})

    def far_sums():
        for k, (own, mid, _, out) in enumerate(groups[0]):
            wait_dma(mid, d_r.at[0, k])
            add_into(mid, own)
            local(mid, out, o_sem.at[0, k])

    def attn_weight_grads(l):
        small = wsv[l].astype(F32)

        def normed(jj):
            xhat, _ = ln_stats(xs[l, pair(jj), :].astype(F32))
            h1s[pair(jj), :] = (xhat * row(small, GAIN1) + row(small, SHIFT1)).astype(BF)

        loop(PAIRS, normed)
        a_q[...] = tn(dqkvs[...], h1s[...])
        a_o[...] = tn(os_[l], gms[...])
        grad_to_mate(l, 1)

    def attn_back(l, jj, odd):
        j = 2 * jj + odd
        rows = chunk(j)
        small = wsv[l].astype(F32)
        dh2 = line.get(NJ - 1 - j)
        xhat, rstd = ln_stats(xm[l, rows, :].astype(F32))
        add_small(l, GAIN2, colsum(dh2 * xhat))
        add_small(l, SHIFT2, colsum(dh2))
        wide = gcur[rows, :].astype(F32) + ln_back(dh2, xhat, rstd, row(small, GAIN2))
        gm[rows, :] = wide
        add_small(l, BOUT, colsum(wide))
        gmid = wide.astype(BF)
        gms[rows, :] = gmid
        do = nt(gmid, wov[l, chunk(at.z), :]).astype(BF)
        delta = jnp.sum(head_stack(do.astype(F32) * os_[l, rows, :].astype(F32)), axis=-1, keepdims=True)
        delta = as_row(delta)[0:1]
        lse = lses[l, blk(j, 8), :][0:1]
        q2 = head_stack(qs[l, rows, :] * jnp.asarray(0.125, BF))
        do2 = head_stack(do)

        def block(keys, masked):
            k = kv[l, keys, 0:W]
            st = nt(k, q2)
            if masked:
                st = jnp.where(query_places(st.shape, 1, odd) >= lax.broadcasted_iota(jnp.int32, st.shape, 0), st, MASKED)
            pt = jnp.exp(st - lse)
            dst = (pt * (nt(kv[l, keys, W:], do2) - delta)).astype(BF)
            dk = nn(dst, q2)
            dv = nn(pt.astype(BF), do2)
            dq = tn(dst, k)
            dkv[keys, 0:W] += dk
            dkv[keys, W:] += dv
            return dq

        dq_acc[...] = block(tail_keys(jj, odd), True)
        send(dkv.at[at.mate_rows(j)], pk.at[j], dk_s.at[j], dk_r.at[j], at.mate)

        def full(kb):
            dq_acc[...] += block(blk(kb, WIDE), False)

        loop(jj, full)
        dqkvs[rows, 0:W] = (head_merge(dq_acc[...]) * 0.125).astype(BF)

    def qkv_back(l, j):
        rows = chunk(j)
        wait_dma(pk.at[j], dk_r.at[j])
        dkv_own = (dkv[at.rows_of(j), :] + pk[j]).astype(BF)
        dqkvs[rows, W:] = dkv_own
        dqkv = jnp.concatenate([dqkvs[rows, 0:W], dkv_own], axis=1)
        sm[l, BQKV:BQKV + 1, 0:QKV] += colsum(dqkv.astype(F32))
        line.emit(FWD + SLOTS * (LAYERS - l) - 1 - j, nn(dqkv, wqv[l]))

    def backward_layer(n):
        l = LAYERS - 1 - n

        def clear(i):
            dkv[blk(i, HALF), :] = jnp.zeros((HALF, KB), F32)

        def first_half(i):
            @when((i == 1) & (l < LAYERS - 1))
            def _():
                attn_weight_grads(l + 1)

            @when(i == 4)
            def _():
                @when(l < LAYERS - 2)
                def _():
                    grad_home(l + 2, 1)

                @when(l < LAYERS - 1)
                def _():
                    grad_across(l + 1, 1)

            @when(i == 3)
            def _():
                loop(SEQ // HALF, clear)

            with jax.named_scope("B1"):
                mlp_back(l, i)

        loop(NJ, first_half)

        @when(l > 0)
        def _():
            grad_to_mate(l, 0)

        def second_half(ii):
            jj = PAIRS - 1 - ii

            @when((ii == 1) & (l < LAYERS - 1))
            def _():
                grad_home(l + 1, 0)

            with jax.named_scope("B2"):
                attn_back(l, jj, 1)

            @when((ii == 0) & (l > 0))
            def _():
                grad_across(l, 0)

            with jax.named_scope("B3"):
                qkv_back(l, 2 * jj + 1)
            with jax.named_scope("B2"):
                attn_back(l, jj, 0)
            with jax.named_scope("B3"):
                qkv_back(l, 2 * jj)

        loop(PAIRS, second_half)
        loop(NJ, lambda j: wait_dma(pk.at[j], dk_s.at[j]))

    loop(LAYERS, backward_layer)
    attn_weight_grads(0)
    last = FWD + LAYERS * SLOTS - 1

    def finish_last(i):
        @when((i >= 1) & (i < 2))
        def _():
            line.serve_first(last - 1 + i)

        @when(i >= 5)
        def _():
            line.serve_second(last - 7 + i)

        finish_layer(0, NJ - 1 - i)

        @when(y == 0)
        def _():
            far_mlp_weight_grads(i)

        @when((p == 0) & at.leaf & (i > 2))
        def _():
            swap_halves(i - 3)

        first = jnp.where(at.hub, 2, 0)

        @when(i == first)
        def _():
            grad_across(0, 1, False)

        @when((i >= first) & (i < first + 6) & (p == 2))
        def _():
            rows = blk(i - first, HALF)
            send(d_q.at[rows], y_q.at[rows], y_s.at[1, 0], y_r.at[1, 0], at.across)

    loop(NJ, finish_last)

    @when(p == 1)
    def _():
        for k, (own, mid, _, _) in enumerate(groups[0]):
            send(own, mid, d_s.at[0, k], d_r.at[0, k], at.mate)

    @when(p == 2)
    def _():
        send(d_o, y_o, y_s.at[1, 1], y_r.at[1, 1], at.across)

    for s in range(LAYERS):
        @when(p != s)
        def _():
            send(sm.at[s], rsm.at[p], sm_s.at[s], sm_r.at[p], {"pp": s})

    @when((p == 0) & at.hub)
    def _():
        loop(NJ - 3, swap_halves)

    for k in every:
        wait_dma(w_vm[k].at[0], w_send.at[0, k])
        wait_dma(w_vm[k].at[0], w_send.at[1, k])
        wait_dma(w_vm[k].at[0], w_fwd.at[k])
    line.close()
    loop(NJ, lambda j: wait_dma(gcur.at[chunk(0)], ho_s.at[j]))

    @when(p == 1)
    def _():
        for k, (own, mid, _, _) in enumerate(groups[0]):
            wait_dma(own, d_s.at[0, k])

    @when(p == 0)
    def _():
        swap_halves(NJ - 3)
        swap_halves(NJ - 2)
        far_sums()
        swap_halves(NJ - 1)
        loop(NJ, lambda j: wait_dma(g_far.at[chunk(j)], gf_s.at[j]))
        for k in range(3):
            wait_dma(g_half, gx.at[k])

    @when(y == 1)
    def _():
        loop(NJ, lambda j: wait_dma(xm.at[0, chunk(j)], xf_s.at[j]))

    grad_home(1, 1)
    grad_home(0, 1)
    for s in range(LAYERS):
        @when(p != s)
        def _():
            wait_dma(sm.at[s], sm_s.at[s])
            wait_dma(rsm.at[s], sm_r.at[s])
    rsm[p] = sm[p]
    sm[0] = (rsm[0] + rsm[1]) + (rsm[2] + rsm[3])
    local(sm.at[0], o_sm, x_sem.at[0])

    def sent(j):
        @when(y == 0)
        def _():
            wait_dma(gcur.at[chunk(0)], gi_s.at[j])

        @when(y == 1)
        def _():
            wait_dma(g_half.at[0, 0], gi_s.at[j])

    loop(NJ, sent)
    for s in range(LAYERS):
        @when(p != s)
        def _():
            wait_dma(h_out.at[0, pl.ds(0, ROWS)], ho_r.at[s])

        @when((p != s) & ((p > 0) | (s == 1)))
        def _():
            wait_dma(g_in.at[0, pl.ds(0, ROWS)], gi_r.at[s])

    for g, items in enumerate(groups):
        for k, (_, _, far, _) in enumerate(items):
            wait_dma(far, o_sem.at[g, k])
    wait_dma(sm.at[0], x_sem.at[0])


def run_layers(*args):
    hbm = pl.BlockSpec(memory_space=pl.ANY)
    dma = pltpu.SemaphoreType.DMA
    slots = pltpu.VMEM((SLOTS, CH, D), BF)
    slot_sem = dma((SLOTS,))
    chunk_sem = dma((NJ,))
    stage_sem = dma((LAYERS,))
    pair_sem = dma((2, 2))

    def bf(*shape):
        return pltpu.VMEM(shape, BF)

    def f32(*shape):
        return pltpu.VMEM(shape, F32)

    grad_shapes = ((D, D), (D, D), (QKV, D), (W, D))
    grads = [f32(*shape) for shape in grad_shapes]
    acts = jax.ShapeDtypeStruct((2, SEQ, D), BF)
    return pl.pallas_call(
        decoder_kernel,
        out_shape=[acts, acts, *(jax.ShapeDtypeStruct(shape, F32) for shape in (*grad_shapes, (SMALL, D)))],
        in_specs=[hbm] * len(args),
        out_specs=[hbm] * 7,
        scratch_shapes=[
            bf(LAYERS, SMALL, D), bf(LAYERS, QKV, D), *[bf(LAYERS, D, D)] * 3,
            bf(LAYERS, SEQ, KB), bf(LAYERS + 1, ROWS, D), bf(LAYERS, ROWS, D), bf(LAYERS, ROWS, W), bf(LAYERS, ROWS, W),
            f32(LAYERS, NJ * 8, KB), f32(PAIRS, WIDE, WIDE), f32(WIDE, W), f32(WIDE, W),
            bf(ROWS, D), f32(ROWS, D), f32(SEQ, KB), f32(NJ, CH, KB), bf(ROWS, D), bf(ROWS, QKV), bf(ROWS, D), *[bf(KB, D)] * 3, f32(KB, W), bf(ROWS, D), bf(ROWS, D), bf(2, NJ, HALF, D),
            *grads, *grads, *grads, f32(LAYERS, SMALL, D), f32(LAYERS, SMALL, D),
            *[slots] * 4, *[slot_sem] * 5, bf(NJ, TP, CH, W), *[chunk_sem] * 5,
            *(pltpu.VMEM(a.shape, BF) for a in args[6:]), dma((len(args) - 6,)),
            chunk_sem, stage_sem, stage_sem, dma((5,)), dma((2, 5)), dma((LAYERS, 5)), dma((5,)),
            chunk_sem, chunk_sem, chunk_sem, stage_sem,
            chunk_sem, chunk_sem, chunk_sem, chunk_sem, stage_sem, *[pair_sem] * 5, stage_sem, stage_sem, *[chunk_sem] * 4, dma((2, NJ)), dma((3,)),
        ],
        compiler_params=pltpu.CompilerParams(collective_id=0, has_side_effects=True, vmem_limit_bytes=VMEM_LIMIT),
        name="decoder_layers",
    )(*args)


def collect_kernel(*refs):
    count = 6
    srcs, small, outs = refs[:count], refs[count], refs[count + 1:2 * count + 1]
    ln, bout, bfc1, bfc2, bqkv = refs[2 * count + 1:2 * count + 6]
    bufs, (sem_in, sem_out) = refs[2 * count + 6:3 * count + 6], refs[3 * count + 6:]
    for k in range(count):
        local(srcs[k], bufs[k], sem_in.at[k])
    ln[...] = small[0:BOUT, :]
    for r, out in ((BOUT, bout), (BFC1, bfc1), (BFC2, bfc2)):
        out[...] = small[r:r + 1, :]
    for i in range(6):
        bqkv[i // 2, i % 2:i % 2 + 1, :] = small[BQKV:BQKV + 1, i * HALF:(i + 1) * HALF]
    for k in range(count):
        wait_dma(bufs[k], sem_in.at[k])
        local(bufs[k], outs[k], sem_out.at[k])
    for k in range(count):
        wait_dma(bufs[k], sem_out.at[k])


def collect(*args):
    hbm, vmem = pl.BlockSpec(memory_space=pl.ANY), pl.BlockSpec(memory_space=pltpu.VMEM)
    big = args[:-1]
    shapes = [(GAIN1 + 4, D), (1, D), (1, D), (1, D), (3, 2, 64)]
    return pl.pallas_call(
        collect_kernel,
        out_shape=[*(jax.ShapeDtypeStruct(a.shape, a.dtype) for a in big), *(jax.ShapeDtypeStruct(shape, F32) for shape in shapes)],
        in_specs=[hbm] * len(big) + [vmem],
        out_specs=[hbm] * len(big) + [vmem] * len(shapes),
        scratch_shapes=[*(pltpu.VMEM(a.shape, a.dtype) for a in big), *[pltpu.SemaphoreType.DMA((len(big),))] * 2],
        compiler_params=pltpu.CompilerParams(vmem_limit_bytes=VMEM_LIMIT),
        name="collect",
    )(*args)


def solution(mesh):
    def program(x_in, dy_out, w_qkv, b_qkv, w_out, b_out, ln_par, w_fc1, b_fc1, w_fc2, b_fc2):
        layers, parts, _, heads, width = w_qkv.shape
        wq = w_qkv.transpose(0, 1, 3, 4, 2).reshape(QKV, D)
        h_out, g_in, *rest = run_layers(
            x_in.reshape(2, SEQ, D), dy_out.reshape(2, SEQ, D), wq, w_out.reshape(W, D), w_fc1.reshape(D, D), w_fc2.reshape(D, D),
            ln_par.reshape(-1, D), b_out, b_fc2, b_fc1, b_qkv.reshape(b_qkv.shape[1:]))
        h_out, g_in, d_w1, d_w2, d_q, d_o, ln, bout, bfc1, bfc2, bqkv = collect(h_out.reshape(-1, D), g_in.reshape(-1, D), *rest)
        acts = (layers, *x_in.shape)
        return (h_out.reshape(acts), g_in.reshape(acts),
                d_q.reshape(layers, parts, heads, width, D).transpose(0, 1, 4, 2, 3), bqkv.reshape(b_qkv.shape),
                d_o.reshape(w_out.shape), bout, ln.reshape(ln_par.shape),
                d_w1.reshape(w_fc1.shape), bfc1, d_w2.reshape(w_fc2.shape), bfc2)

    act_spec = P(NO, "dp", NO, NO)
    arg_specs = (act_spec, act_spec,
                 P("pp", NO, NO, "tp", NO), P("pp", NO, "tp", NO), P("pp", "tp", NO, NO),
                 P("pp", NO), P("pp", NO, NO), P("pp", NO, "tp"), P("pp", "tp"),
                 P("pp", "tp", NO), P("pp", NO))
    stage_spec = P("pp", NO, "dp", NO, NO)
    grad_axes = ("dp", "pp")
    result_specs = (stage_spec, stage_spec,
                    P(grad_axes, NO, NO, "tp", NO), P(grad_axes, NO, "tp", NO), P(grad_axes, "tp", NO, NO),
                    P(grad_axes, NO), P(grad_axes, NO, NO), P(grad_axes, NO, "tp"), P(grad_axes, "tp"),
                    P(grad_axes, "tp", NO), P(grad_axes, NO))
    return jax.shard_map(program, mesh=mesh, in_specs=arg_specs, out_specs=result_specs, check_vma=False)
```
